256 devices in a mesh: dp: 32 (over x, y, z_lo), seq: 8 (over z_hi, core).
Axes of the slice: x: 4, y: 4, z: 8 (z_hi: 4, z_lo: 2; z = z_hi * 2 + z_lo), core: 2. Of those that a mesh axis runs over, the one named last changes fastest.
Arguments:
- frames: bfloat16 [32, 4096, 512], P('dp', 'seq'), may hold values from -6 to 6
- cotangent: bfloat16 [32, 4096, 512], P('dp', 'seq'), may hold values from -6 to 6
- weight_in: bfloat16 [2, 512, 2176], replicated, may hold values from -0.25 to 0.25
- qk_scales: float32 [2, 2, 128], replicated, may hold values from 0.5 to 1.5
- weight_out: bfloat16 [2, 1024, 512], replicated, may hold values from -0.1875 to 0.1875
- gains: float32 [2, 512], replicated, may hold values from 0.5 to 1.5
Outputs:
- output: bfloat16 [32, 4096, 512], P('dp', 'seq')
- grad_frames: bfloat16 [32, 4096, 512], P('dp', 'seq')
- grad_in: float32 [2, 512, 2176], P(None, 'dp')
- grad_out: float32 [2, 1024, 512], P(None, 'dp')
- grad_gains: float32 [2, 512], replicated
- grad_scales: float32 [2, 2, 128], replicated
The draws below stay inside these ranges and needn't reach their ends.
All inputs are finite; a program needn't handle non-finite values.
Results may differ from the reference program's by a relative error of at most 0.028.
Values may be sent and summed in bfloat16 or wider, within the bound.
A program may use at most 192 MiB of HBM per device.

```python
from functools import partial
import jax
import jax.numpy as jnp
from jax import lax

D = 512
E = 1024
S = 128
BLOCK = 256
NCH = 16
SEQLEN = 4096
BATCH = 32


def steps_of(own_key, extent, cuts, low, top_value):
    factor_of, own = 1.0, jax.random.fold_in(own_key, 6)
    for axis_at, shards_of in cuts:
        draws = jnp.exp(jax.random.uniform(jax.random.fold_in(own, axis_at), (shards_of,), jnp.float32, low / len(cuts), top_value / len(cuts)))
        factor_of = factor_of * jnp.repeat(draws, extent[axis_at] // shards_of).reshape([-1 if axis == axis_at else 1 for axis in range(len(extent))])
    return factor_of


def bell_draw(key, extent, scale, limit, cuts=(), held_as=jnp.bfloat16):
    entries = scale * jax.random.normal(key, extent, jnp.float32)
    if cuts:
        entries = entries * steps_of(key, extent, cuts, -0.22, 0.18)
    return jnp.clip(entries, -limit, limit).astype(held_as)


def setup_inputs(seed: int = 0) -> dict:
    key_list = jax.random.split(jax.random.key(seed), 7)
    frames = bell_draw(key_list[0], (BATCH, SEQLEN, D), 1.0, 6.0, ((0, 32), (1, 8)))
    cotangent = bell_draw(key_list[1], (BATCH, SEQLEN, D), 1.0, 6.0, ((0, 32), (1, 8)))
    weight_in = bell_draw(key_list[2], (2, D, 2 * E + S), D ** -0.5, 0.25)
    qk_scales = jnp.clip(1.0 + 0.1 * jax.random.normal(key_list[3], (2, 2, S), jnp.float32), 0.5, 1.5)
    weight_out = bell_draw(key_list[4], (2, E, D), E ** -0.5, 0.1875)
    gains = jnp.clip(1.0 + 0.1 * jax.random.normal(key_list[5], (2, D), jnp.float32), 0.5, 1.5)
    return dict(frames=frames, cotangent=cotangent, weight_in=weight_in, qk_scales=qk_scales, weight_out=weight_out, gains=gains)


EPSILON = 1e-06

def normed(values, gain_row):
    scaling = lax.rsqrt(lax.optimization_barrier(jnp.mean(values * values, axis=-1, keepdims=True)) + EPSILON)
    return values * scaling * gain_row

def mixer(projected, scale_pair, attend_axis):
    width = (projected.shape[-1] - scale_pair.shape[-1]) // 2
    active = jax.nn.silu(projected)
    gate_part = active[..., :width]
    value_part = active[..., width:2 * width].astype(jnp.bfloat16)
    shared = active[..., 2 * width:]
    query = (shared * scale_pair[0]).astype(jnp.bfloat16)
    keyed = (shared * scale_pair[1]).astype(jnp.bfloat16)
    length = projected.shape[attend_axis]
    if attend_axis == 1:
        score_form = 'gls,gms->glm'
        mix_form = 'glm,gme->gle'
    else:
        score_form = 'lgs,mgs->glm'
        mix_form = 'glm,mge->lge'
    scores = jnp.einsum(score_form, query.astype(jnp.float32), keyed.astype(jnp.float32))
    scores = scores * scale_pair.shape[-1] ** (-0.5)
    weights = (jnp.square(jax.nn.relu(scores)) / length).astype(jnp.bfloat16)
    mixed = jnp.einsum(mix_form, weights.astype(jnp.float32), value_part.astype(jnp.float32))
    return (gate_part * mixed).astype(jnp.bfloat16)

def rows_product(left, right):
    left_rows = left.reshape(-1, left.shape[-1])
    right_rows = right.reshape(-1, right.shape[-1])
    return lax.dot_general(left_rows, right_rows, (((0,), (0,)), ((), ())), preferred_element_type=jnp.float32)

def against(values, weight):
    return lax.dot_general(values, weight, (((values.ndim - 1,), (1,)), ((), ())), preferred_element_type=jnp.float32)

def unit_forward(inputs_now, weight_in, scale_pair, weight_out, gain_row, attend_axis):
    hidden = normed(inputs_now.astype(jnp.float32), gain_row).astype(jnp.bfloat16)
    projected = jnp.dot(hidden, weight_in, preferred_element_type=jnp.float32)
    gated = mixer(projected, scale_pair, attend_axis)
    result = (inputs_now.astype(jnp.float32) + jnp.dot(gated, weight_out, preferred_element_type=jnp.float32)).astype(jnp.bfloat16)
    return (result, (hidden, projected, gated))

def unit_backward(inputs_now, upstream, weight_in, scale_pair, weight_out, gain_row, saved, attend_axis):
    hidden, projected, gated = saved
    grad_out = rows_product(gated, upstream)
    grad_gated = against(upstream, weight_out).astype(jnp.bfloat16)
    pulled = jax.vjp(partial(mixer, attend_axis=attend_axis), projected, scale_pair)[1]
    grad_proj, grad_scale = pulled(grad_gated)
    grad_proj = grad_proj.astype(jnp.bfloat16)
    grad_in = rows_product(hidden, grad_proj)
    grad_hidden = against(grad_proj, weight_in)
    norm_pull = jax.vjp(normed, inputs_now.astype(jnp.float32), gain_row)[1]
    grad_inputs, grad_gain = norm_pull(grad_hidden)
    grad_inputs = (upstream.astype(jnp.float32) + grad_inputs).astype(jnp.bfloat16)
    return (grad_inputs, grad_in, grad_out, grad_gain, grad_scale)

def reference(frames, cotangent, weight_in, qk_scales, weight_out, gains):
    scaling = (BATCH * SEQLEN) ** (-0.5)

    def one_sequence(carry, pair):
        seq_frames, seq_cot = pair
        blocked = seq_frames.reshape(NCH, BLOCK, D)
        upstream = seq_cot.reshape(NCH, BLOCK, D)
        first, saved_first = unit_forward(blocked, weight_in[0], qk_scales[0], weight_out[0], gains[0], 1)
        second, saved_second = unit_forward(first, weight_in[1], qk_scales[1], weight_out[1], gains[1], 0)
        back_first, in_late, out_late, gain_late, scale_late = unit_backward(first, upstream, weight_in[1], qk_scales[1], weight_out[1], gains[1], saved_second, 0)
        back_frames, in_early, out_early, gain_early, scale_early = unit_backward(blocked, back_first, weight_in[0], qk_scales[0], weight_out[0], gains[0], saved_first, 1)
        carry = (carry[0] + jnp.stack([in_early, in_late]), carry[1] + jnp.stack([out_early, out_late]), carry[2] + jnp.stack([gain_early, gain_late]), carry[3] + jnp.stack([scale_early, scale_late]))
        return (carry, (second.reshape(SEQLEN, D), back_frames.reshape(SEQLEN, D)))
    start = (jnp.zeros((2, D, 2 * E + S), jnp.float32), jnp.zeros((2, E, D), jnp.float32), jnp.zeros((2, D), jnp.float32), jnp.zeros((2, 2, S), jnp.float32))
    totals, outs_pair = lax.scan(one_sequence, start, (frames, cotangent))
    return (outs_pair[0], outs_pair[1], totals[0] * scaling, totals[1] * scaling, totals[2] * scaling, totals[3] * scaling)
```

```python
from functools import partial
import functools

import jax
import jax.numpy as jnp
from jax import lax
from jax.experimental import pallas as pl
from jax.experimental.pallas import tpu as pltpu
from jax.sharding import Mesh
from jax.sharding import PartitionSpec as P

BLOCK = 256
DP = ("dp_0", "dp_1", "dp_2")
SEQ = ("seq_0", "seq_1")
DP_SEQ = ("dp_0", "dp_1", "dp_2", "seq_0", "seq_1")


EPSILON = 1e-06


def in_order(parts, dim):
    parts = jnp.moveaxis(parts, 0, dim)
    shape = parts.shape
    return parts.reshape(*shape[:dim], shape[dim] * shape[dim + 1], *shape[dim + 2 :])


def one_gather(arrays, axis, dims):
    ravelled = jnp.concatenate([a.reshape(-1) for a in arrays])
    lines, at, gathered = (lax.all_gather(ravelled, axis), 0, [])
    for a, dim in zip(arrays, dims):
        parts = lines[:, at : at + a.size].reshape(-1, *a.shape)
        gathered.append(in_order(parts, dim))
        at += a.size
    return tuple(gathered)


def over_axes(x, axes):
    return functools.reduce(lax.psum, axes, x)


def normed(values, gain_row):
    scaling = lax.rsqrt(jnp.mean(values * values, axis=-1, keepdims=True) + EPSILON)
    return values * scaling * gain_row


def mixer(projected, scale_pair, attend_axis):
    width = (projected.shape[-1] - scale_pair.shape[-1]) // 2
    active = jax.nn.silu(projected)
    gate_part = active[..., :width]
    value_part = active[..., width : 2 * width].astype(jnp.bfloat16)
    shared = active[..., 2 * width :]
    query = (shared * scale_pair[0]).astype(jnp.bfloat16)
    keyed = (shared * scale_pair[1]).astype(jnp.bfloat16)
    length = projected.shape[attend_axis]
    if attend_axis == 1:
        score_form = "gls,gms->glm"
        mix_form = "glm,gme->gle"
    else:
        score_form = "lgs,mgs->glm"
        mix_form = "glm,mge->lge"
    scores = jnp.einsum(score_form, query, keyed, preferred_element_type=jnp.float32)
    scores = scores * scale_pair.shape[-1] ** (-0.5)
    weights = (jnp.square(jax.nn.relu(scores)) / length).astype(jnp.bfloat16)
    mixed = jnp.einsum(mix_form, weights, value_part, preferred_element_type=jnp.float32)
    return (gate_part * mixed).astype(jnp.bfloat16)


def rows_product(left, right):
    left_rows = left.reshape(-1, left.shape[-1])
    right_rows = right.reshape(-1, right.shape[-1])
    return lax.dot_general(
        left_rows, right_rows, (((0,), (0,)), ((), ())), preferred_element_type=jnp.float32
    )


def against(values, weight):
    return lax.dot_general(
        values, weight, (((values.ndim - 1,), (1,)), ((), ())), preferred_element_type=jnp.float32
    )


MESH = pl.DeviceIdType.MESH
NT = 25
HALVES = ((0, 13), (13, 12))


class Links:
    def __init__(self, send, recv):
        self.send, self.recv, self.used, self.open = send, recv, 0, []
        self.x, self.y, self.zl = (lax.axis_index(a) for a in DP)
        self.zh, self.c = (lax.axis_index(a) for a in SEQ)

    def take(self, count=1):
        at = self.used
        self.used += count
        return at

    def at(self, x=None, y=None, zl=None, zh=None, c=None):
        return (
            self.x if x is None else x,
            self.y if y is None else y,
            self.zl if zl is None else zl,
            self.zh if zh is None else zh,
            self.c if c is None else c,
        )

    def copy(self, src, dst, target, sem, recv_sem=None):
        return pltpu.make_async_remote_copy(
            src_ref=src,
            dst_ref=dst,
            send_sem=self.send.at[sem],
            recv_sem=self.recv.at[sem if recv_sem is None else recv_sem],
            device_id=target,
            device_id_type=MESH,
        )

    def start(self, src, dst, target, sem):
        op = self.copy(src, dst, target, sem)
        op.start()
        self.open.append(op)
        return op

    def drain(self):
        for op in self.open:
            if callable(op):
                op()
            else:
                op.wait_send()
        self.open = []


def mod4(v):
    return lax.rem(v + 4, 4)


def barrier(k):
    sem = pltpu.get_barrier_semaphore()
    targets = [k.at(x=mod4(k.x + d)) for d in (1, 2, 3)]
    targets += [k.at(y=mod4(k.y + d)) for d in (1, 2, 3)]
    for dl in (0, 1):
        for dh in range(4):
            for dc in (0, 1):
                if dl or dh or dc:
                    targets.append(
                        k.at(zl=lax.rem(k.zl + dl, 2), zh=mod4(k.zh + dh), c=lax.rem(k.c + dc, 2))
                    )
    for target in targets:
        pl.semaphore_signal(sem, inc=1, device_id=target, device_id_type=MESH)
    pl.semaphore_wait(sem, len(targets))


def small_sum(k, buf, value_ref, out_ref):
    f32_pair, f32_x, f32_y, f32_z = 0, 1, 5, 9
    sems = {}

    def pair():
        sems["p"] = k.take()
        k.start(value_ref, buf.at[f32_pair], k.at(c=1 - k.c), sems["p"])

    def x():
        k.copy(value_ref, buf.at[f32_pair], k.at(c=1 - k.c), sems["p"]).wait_recv()
        buf[f32_x + k.x] = value_ref[...] + buf[f32_pair]
        sems["x"] = k.take(3)
        for d in (1, 2, 3):
            src = buf.at[f32_x + k.x]
            k.start(src, src, k.at(x=mod4(k.x + d)), sems["x"] + d - 1)

    def y():
        for d in (1, 2, 3):
            slot = buf.at[f32_x + mod4(k.x - d)]
            k.copy(slot, slot, k.at(x=mod4(k.x - d)), sems["x"] + d - 1).wait_recv()
        buf[f32_y + k.y] = (buf[f32_x] + buf[f32_x + 1]) + (buf[f32_x + 2] + buf[f32_x + 3])
        sems["y"] = k.take(3)
        for d in (1, 2, 3):
            src = buf.at[f32_y + k.y]
            k.start(src, src, k.at(y=mod4(k.y + d)), sems["y"] + d - 1)

    def z():
        for d in (1, 2, 3):
            slot = buf.at[f32_y + mod4(k.y - d)]
            k.copy(slot, slot, k.at(y=mod4(k.y - d)), sems["y"] + d - 1).wait_recv()
        me = 2 * k.zh + k.zl
        buf[f32_z + me] = (buf[f32_y] + buf[f32_y + 1]) + (buf[f32_y + 2] + buf[f32_y + 3])
        sems["z"] = k.take(7)
        for d in range(1, 8):
            to = lax.rem(me + d, 8)
            src = buf.at[f32_z + me]
            k.start(src, src, k.at(zh=to // 2, zl=lax.rem(to, 2)), sems["z"] + d - 1)

    def end():
        me = 2 * k.zh + k.zl
        for d in range(1, 8):
            frm = lax.rem(me + 8 - d, 8)
            slot = buf.at[f32_z + frm]
            k.copy(slot, slot, k.at(zh=frm // 2, zl=lax.rem(frm, 2)), sems["z"] + d - 1).wait_recv()
        parts = [buf[f32_z + i] for i in range(8)]
        while len(parts) > 1:
            parts = [a + b for a, b in zip(parts[::2], parts[1::2])]
        out_ref[...] = parts[0]

    return [pair, x, y, z, end]


def sum_stages(k, grads, paired, first_in, second_in, z_in, gathered):
    sems = {}
    me = (k.x, k.y)

    def to_axis(half, step, delta):
        along = (half + step) % 2
        return k.at(x=mod4(k.x + delta)) if along == 0 else k.at(y=mod4(k.y + delta))

    def view(half, step, delta, part):
        t0, n = HALVES[half]
        along = (half + step) % 2
        dest = mod4(me[along] + delta)
        if step == 0:
            sub = pl.ds(0, 4) if part is None else pl.ds(2 * part, 2)
            return (
                paired.at[dest, sub, t0 : t0 + n]
                if along == 0
                else paired.at[sub, dest, t0 : t0 + n]
            )
        cut = (n + 1) // 2
        lo, hi = {None: (0, n), 0: (0, cut), 1: (cut, n)}[part]
        return (
            paired.at[dest, k.y, t0 + lo : t0 + hi]
            if along == 0
            else paired.at[k.x, dest, t0 + lo : t0 + hi]
        )

    def inbox(half, step, direction, part):
        n = HALVES[half][1]
        one = first_in[half] if step == 0 else second_in[half]
        box = one[2 + direction]
        if part is None:
            return box
        if step == 0:
            return box.at[2 * part : 2 * part + 2]
        cut = (n + 1) // 2
        return box.at[0:cut] if part == 0 else box.at[cut:n]

    def outset(half, step):
        one = first_in[half] if step == 0 else second_in[half]
        base = sems[half, step] = k.take(6)
        for direction, delta in ((0, 1), (1, -1)):
            k.start(
                view(half, step, 2, direction),
                one[direction],
                to_axis(half, step, delta),
                base + direction,
            )
        for direction, delta in ((0, 1), (1, -1)):
            part = 1 - direction
            k.start(
                view(half, step, delta, part),
                inbox(half, step, direction, part),
                to_axis(half, step, delta),
                base + 2 + direction,
            )

    def relay(half, step):
        one = first_in[half] if step == 0 else second_in[half]
        base = sems[half, step]
        for direction, delta in ((0, 1), (1, -1)):
            k.copy(
                one[direction], one[direction], to_axis(half, step, -delta), base + direction
            ).wait_recv()
            target = view(half, step, delta, direction)
            target[...] = target[...] + one[direction][...]
            k.start(
                target,
                inbox(half, step, direction, direction),
                to_axis(half, step, delta),
                base + 4 + direction,
            )

    def collect(half, step):
        base = sems[half, step]
        for direction, delta in ((0, 1), (1, -1)):
            for at, part in ((2, 1 - direction), (4, direction)):
                box = inbox(half, step, direction, part)
                k.copy(box, box, to_axis(half, step, -delta), base + at + direction).wait_recv()
        own = view(half, step, 0, None)
        f32 = jnp.float32
        own[...] = (
            own[...].astype(f32)
            + (inbox(half, step, 0, None)[...].astype(f32) + inbox(half, step, 1, None)[...].astype(f32))
        ).astype(jnp.bfloat16)

    def pair_out():
        sems["pair"] = k.take()
        k.start(grads.at[:, :, 1 - k.c], paired, k.at(c=1 - k.c), sems["pair"])

    def pair_in():
        k.copy(paired, paired, k.at(c=1 - k.c), sems["pair"]).wait_recv()

        @pl.loop(0, 4)
        def _(i):
            paired[i] = paired[i] + grads[i, :, k.c]

        for half in (0, 1):
            outset(half, 0)

    def relay_0():
        for half in (0, 1):
            relay(half, 0)

    def turn():
        for half in (0, 1):
            collect(half, 0)
            outset(half, 1)

    def relay_1():
        for half in (0, 1):
            relay(half, 1)

    def z_out():
        for half in (0, 1):
            collect(half, 1)
        base = sems["z"] = k.take(8)
        spot = 2 * k.zh + k.zl
        for q in range(4):
            for e in range(2):
                piece = 3 * (2 * q + e)
                source = paired.at[k.x, k.y, piece : piece + 4]
                mine = (k.zh == q) & (k.c == e) & (k.zl == k.c)
                op = pltpu.make_async_remote_copy(
                    src_ref=source,
                    dst_ref=z_in.at[spot],
                    send_sem=k.send.at[base + 2 * q + e],
                    recv_sem=k.recv.at[base + spot],
                    device_id=k.at(zl=k.c, zh=q, c=e),
                    device_id_type=MESH,
                )

                @pl.when(jnp.logical_not(mine))
                def _():
                    op.start()

                @pl.when(mine)
                def _():
                    z_in[spot] = source[...]

                def done(op=op, mine=mine):
                    @pl.when(jnp.logical_not(mine))
                    def _():
                        op.wait_send()

                k.open.append(done)

    def z_in_sum():
        base = sems["z"]
        spot = 2 * k.zh + k.zl
        for slot in range(8):
            mine = (spot == slot) & (k.zl == k.c)

            @pl.when(jnp.logical_not(mine))
            def _():
                box = z_in.at[slot]
                k.copy(box, box, k.at(zh=slot // 2, zl=slot % 2, c=k.zl), base + slot).wait_recv()

        parts = [z_in[i].astype(jnp.float32) for i in range(8)]
        while len(parts) > 1:
            parts = [a + b for a, b in zip(parts[::2], parts[1::2])]
        p = 2 * k.zh + k.c
        gathered[p] = parts[0].astype(jnp.bfloat16)
        base = sems["g"] = k.take(7)
        for d in range(1, 8):
            to = lax.rem(p + d, 8)
            box = gathered.at[p]
            k.start(box, box, k.at(zh=to // 2, c=lax.rem(to, 2)), base + d - 1)

    def gather():
        p = 2 * k.zh + k.c
        for d in range(1, 8):
            frm = lax.rem(p + 8 - d, 8)
            box = gathered.at[frm]
            k.copy(box, box, k.at(zh=frm // 2, c=lax.rem(frm, 2)), sems["g"] + d - 1).wait_recv()

    return [pair_out, pair_in, relay_0, turn, relay_1, z_out, z_in_sum, gather]


def write_shard(gathered, grad_in_ref, grad_out_ref, scaling):
    for tile in range(NT):
        p = min(tile // 3, 7)
        values = gathered[p, tile - 3 * p].astype(jnp.float32) * scaling
        if tile < 17:
            grad_in_ref[:, 128 * tile : 128 * tile + 128] = values
        else:
            column, half = (tile - 17) // 2, (tile - 17) % 2
            grad_out_ref[16 * half : 16 * half + 16, 128 * column : 128 * column + 128] = values


def sum_scratch():
    bf16 = jnp.bfloat16
    shapes = [pltpu.VMEM((4, 4, NT, 16, 128), bf16)]
    for _, n in HALVES:
        shapes += [pltpu.VMEM((2, n, 16, 128), bf16)] * 2 + [pltpu.VMEM((4, n, 16, 128), bf16)] * 2
    for _, n in HALVES:
        cut = (n + 1) // 2
        shapes += [pltpu.VMEM((cut, 16, 128), bf16), pltpu.VMEM((n - cut, 16, 128), bf16)]
        shapes += [pltpu.VMEM((n, 16, 128), bf16)] * 2
    shapes += [pltpu.VMEM((8, 4, 16, 128), bf16), pltpu.VMEM((8, 4, 16, 128), bf16)]
    shapes += [pltpu.VMEM((17, 8, 128), jnp.float32)]
    return shapes


def sum_refs(refs):
    paired, refs = refs[0], refs[1:]
    first = (refs[0:4], refs[4:8])
    second = (refs[8:12], refs[12:16])
    return (paired, first, second, refs[16], refs[17]), refs[18]


SEMS = 160


def reduce_kernel(scaling, g_ref, s_ref, in_ref, out_ref, small_ref, *scratch):
    send, recv = scratch[-2:]
    k = Links(send, recv)
    barrier(k)
    stages = []
    ends = []
    for unit in (1, 0):
        main, buf = sum_refs(scratch[20 * unit : 20 * unit + 20])
        stages.append(sum_stages(k, g_ref.at[unit], *main))
        stages.append(small_sum(k, buf, s_ref.at[unit], small_ref.at[unit]))
        ends.append((main[-1], unit))
    for step in range(8):
        for group in stages:
            if step < len(group):
                group[step]()
    for gathered, unit in ends:
        write_shard(gathered, in_ref.at[unit], out_ref.at[unit], scaling)
    small_ref[...] = small_ref[...] * scaling
    k.drain()


def reduced(grads, smalls, scaling):
    vmem = pl.BlockSpec(memory_space=pltpu.VMEM)
    return pl.pallas_call(
        functools.partial(reduce_kernel, scaling),
        out_shape=(
            jax.ShapeDtypeStruct((2, 16, 2176), jnp.float32),
            jax.ShapeDtypeStruct((2, 32, 512), jnp.float32),
            jax.ShapeDtypeStruct((2, 8, 128), jnp.float32),
        ),
        in_specs=[vmem, vmem],
        out_specs=(vmem, vmem, vmem),
        scratch_shapes=sum_scratch()
        + sum_scratch()
        + [pltpu.SemaphoreType.DMA((SEMS,)), pltpu.SemaphoreType.DMA((SEMS,))],
        compiler_params=pltpu.CompilerParams(
            collective_id=0, has_side_effects=True, vmem_limit_bytes=48 * 1024 * 1024
        ),
    )(grads, smalls)


def as_tiles(grad_in, grad_out):
    left = grad_in.astype(jnp.bfloat16).reshape(4, 4, 2, 16, 17, 128).transpose(0, 1, 2, 4, 3, 5)
    right = grad_out.astype(jnp.bfloat16).reshape(4, 4, 2, 2, 16, 4, 128).transpose(0, 1, 2, 5, 3, 4, 6)
    return jnp.concatenate([left, right.reshape(4, 4, 2, 8, 16, 128)], axis=3)


def small_tile(gain, scale):
    return jnp.concatenate([gain.reshape(4, 128), scale.reshape(2, 128), jnp.zeros((2, 128), jnp.float32)])


def unit_forward(inputs_now, weight_in, scale_pair, weight_out, gain_row, attend_axis):
    hidden = normed(inputs_now.astype(jnp.float32), gain_row).astype(jnp.bfloat16)
    projected = jnp.dot(hidden, weight_in, preferred_element_type=jnp.float32)
    gated = mixer(projected, scale_pair, attend_axis)
    result = (
        inputs_now.astype(jnp.float32)
        + jnp.dot(gated, weight_out, preferred_element_type=jnp.float32)
    ).astype(jnp.bfloat16)
    return (result, (hidden, projected, gated))


def unit_backward(
    inputs_now, upstream, weight_in, scale_pair, weight_out, gain_row, saved, attend_axis
):
    hidden, projected, gated = saved
    grad_out = rows_product(gated, upstream)
    grad_gated = against(upstream, weight_out).astype(jnp.bfloat16)
    pulled = jax.vjp(partial(mixer, attend_axis=attend_axis), projected, scale_pair)[1]
    grad_proj, grad_scale = pulled(grad_gated)
    grad_proj = grad_proj.astype(jnp.bfloat16)
    grad_in = rows_product(hidden, grad_proj)
    grad_hidden = against(grad_proj, weight_in)
    norm_pull = jax.vjp(normed, inputs_now.astype(jnp.float32), gain_row)[1]
    grad_inputs, grad_gain = norm_pull(grad_hidden)
    grad_inputs = (upstream.astype(jnp.float32) + grad_inputs).astype(jnp.bfloat16)
    return (grad_inputs, grad_in, grad_out, grad_gain, grad_scale)


def on_device(frames, cotangent, weight_in, qk_scales, weight_out, gains):
    block_count = frames.shape[1] // BLOCK
    width = frames.shape[2]
    tokens_all = frames.shape[0] * frames.shape[1] * lax.axis_size(DP) * lax.axis_size(SEQ)
    scaling = tokens_all ** (-0.5)
    blocked = frames.reshape(block_count, BLOCK, width)
    first, saved_first = unit_forward(
        blocked, weight_in[0], qk_scales[0], weight_out[0], gains[0], 1
    )
    first_pos = lax.all_to_all(first, SEQ, split_axis=1, concat_axis=0, tiled=True)
    second, saved_second = unit_forward(
        first_pos, weight_in[1], qk_scales[1], weight_out[1], gains[1], 0
    )
    result = lax.all_to_all(second, SEQ, split_axis=0, concat_axis=1, tiled=True)
    upstream = lax.all_to_all(
        cotangent.reshape(block_count, BLOCK, width), SEQ, split_axis=1, concat_axis=0, tiled=True
    )
    back_pos, in_late, out_late, gain_late, scale_late = unit_backward(
        first_pos, upstream, weight_in[1], qk_scales[1], weight_out[1], gains[1], saved_second, 0
    )
    back_first = lax.all_to_all(back_pos, SEQ, split_axis=0, concat_axis=1, tiled=True)
    back_frames, in_early, out_early, gain_early, scale_early = unit_backward(
        blocked, back_first, weight_in[0], qk_scales[0], weight_out[0], gains[0], saved_first, 1
    )
    grads = jnp.stack([as_tiles(in_early, out_early), as_tiles(in_late, out_late)])
    smalls = jnp.stack([small_tile(gain_early, scale_early), small_tile(gain_late, scale_late)])
    grad_in, grad_out, small = reduced(grads, smalls, scaling)
    return (
        result.reshape(frames.shape),
        back_frames.reshape(frames.shape),
        grad_in,
        grad_out,
        small[:, :4].reshape(2, 512),
        small[:, 4:6],
    )


def solution(mesh):
    split = Mesh(mesh.devices.reshape(4, 4, 2, 4, 2), ("dp_0", "dp_1", "dp_2", "seq_0", "seq_1"))
    placed = (P(DP, SEQ, None), P(DP, SEQ, None), P(), P(), P(), P())
    return jax.shard_map(
        on_device,
        mesh=split,
        in_specs=placed,
        out_specs=(
            P(DP, SEQ, None),
            P(DP, SEQ, None),
            P(None, DP, None),
            P(None, DP, None),
            P(),
            P(),
        ),
        check_vma=False,
    )
```

```python
import functools

import jax
import jax.numpy as jnp
from jax import lax
from jax.experimental import pallas as pl
from jax.experimental.pallas import tpu as pltpu
from jax.sharding import Mesh
from jax.sharding import PartitionSpec as P

DP = ("dp_0", "dp_1", "dp_2")
SEQ = ("seq_0", "seq_1")
D, E, S, BLOCK = 512, 1024, 128, 256
WIDE = 2 * E + S
EPSILON = 1e-06
F32, BF16 = jnp.float32, jnp.bfloat16
NT = 25
IN_TILES, OUT_TILES = (0, 17), (17, 8)
SEMS = 300


MESH = pl.DeviceIdType.MESH


def halves_of(n):
    return ((0, (n + 1) // 2), ((n + 1) // 2, n // 2))


def pieces_of(n):
    return n // 8, n - 7 * (n // 8)


class Links:
    def __init__(self, send, recv):
        self.send, self.recv, self.used, self.open = send, recv, 0, []
        self.x, self.y, self.zl = (lax.axis_index(a) for a in DP)
        self.zh, self.c = (lax.axis_index(a) for a in SEQ)

    def take(self, count=1):
        at = self.used
        self.used += count
        return at

    def at(self, x=None, y=None, zl=None, zh=None, c=None):
        return (
            self.x if x is None else x,
            self.y if y is None else y,
            self.zl if zl is None else zl,
            self.zh if zh is None else zh,
            self.c if c is None else c,
        )

    def copy(self, src, dst, target, sem, recv_sem=None):
        return pltpu.make_async_remote_copy(
            src_ref=src,
            dst_ref=dst,
            send_sem=self.send.at[sem],
            recv_sem=self.recv.at[sem if recv_sem is None else recv_sem],
            device_id=target,
            device_id_type=MESH,
        )

    def start(self, src, dst, target, sem):
        op = self.copy(src, dst, target, sem)
        op.start()
        self.open.append(op)
        return op

    def drain(self):
        for op in self.open:
            if callable(op):
                op()
            else:
                op.wait_send()
        self.open = []


def mod4(v):
    return lax.rem(v + 4, 4)


def barrier(k):
    sem = pltpu.get_barrier_semaphore()
    targets = [k.at(x=mod4(k.x + d)) for d in (1, 2, 3)]
    targets += [k.at(y=mod4(k.y + d)) for d in (1, 2, 3)]
    for dl in (0, 1):
        for dh in range(4):
            for dc in (0, 1):
                if dl or dh or dc:
                    targets.append(
                        k.at(zl=lax.rem(k.zl + dl, 2), zh=mod4(k.zh + dh), c=lax.rem(k.c + dc, 2))
                    )
    for target in targets:
        pl.semaphore_signal(sem, inc=1, device_id=target, device_id_type=MESH)
    pl.semaphore_wait(sem, len(targets))


def small_sum(k, buf, value_ref, out_ref):
    f32_pair, f32_x, f32_y, f32_z = 0, 1, 5, 9
    sems = {}

    def pair():
        sems["p"] = k.take()
        k.start(value_ref, buf.at[f32_pair], k.at(c=1 - k.c), sems["p"])

    def x():
        k.copy(value_ref, buf.at[f32_pair], k.at(c=1 - k.c), sems["p"]).wait_recv()
        buf[f32_x + k.x] = value_ref[...] + buf[f32_pair]
        sems["x"] = k.take(3)
        for d in (1, 2, 3):
            src = buf.at[f32_x + k.x]
            k.start(src, src, k.at(x=mod4(k.x + d)), sems["x"] + d - 1)

    def y():
        for d in (1, 2, 3):
            slot = buf.at[f32_x + mod4(k.x - d)]
            k.copy(slot, slot, k.at(x=mod4(k.x - d)), sems["x"] + d - 1).wait_recv()
        buf[f32_y + k.y] = (buf[f32_x] + buf[f32_x + 1]) + (buf[f32_x + 2] + buf[f32_x + 3])
        sems["y"] = k.take(3)
        for d in (1, 2, 3):
            src = buf.at[f32_y + k.y]
            k.start(src, src, k.at(y=mod4(k.y + d)), sems["y"] + d - 1)

    def z():
        for d in (1, 2, 3):
            slot = buf.at[f32_y + mod4(k.y - d)]
            k.copy(slot, slot, k.at(y=mod4(k.y - d)), sems["y"] + d - 1).wait_recv()
        me = 2 * k.zh + k.zl
        buf[f32_z + me] = (buf[f32_y] + buf[f32_y + 1]) + (buf[f32_y + 2] + buf[f32_y + 3])
        sems["z"] = k.take(7)
        for d in range(1, 8):
            to = lax.rem(me + d, 8)
            src = buf.at[f32_z + me]
            k.start(src, src, k.at(zh=to // 2, zl=lax.rem(to, 2)), sems["z"] + d - 1)

    def end():
        me = 2 * k.zh + k.zl
        for d in range(1, 8):
            frm = lax.rem(me + 8 - d, 8)
            slot = buf.at[f32_z + frm]
            k.copy(slot, slot, k.at(zh=frm // 2, zl=lax.rem(frm, 2)), sems["z"] + d - 1).wait_recv()
        parts = [buf[f32_z + i] for i in range(8)]
        while len(parts) > 1:
            parts = [a + b for a, b in zip(parts[::2], parts[1::2])]
        out_ref[...] = parts[0]

    return [pair, x, y, z, end]


def sum_stages(k, grads, t_base, n_tiles, paired, first_in, second_in, z_in, gathered):
    halves = halves_of(n_tiles)
    piece_step, piece_size = pieces_of(n_tiles)
    sems = {}
    me = (k.x, k.y)

    def to_axis(half, step, delta):
        along = (half + step) % 2
        return k.at(x=mod4(k.x + delta)) if along == 0 else k.at(y=mod4(k.y + delta))

    def view(half, step, delta, part):
        t0, n = halves[half]
        along = (half + step) % 2
        dest = mod4(me[along] + delta)
        if step == 0:
            sub = pl.ds(0, 4) if part is None else pl.ds(2 * part, 2)
            return (
                paired.at[dest, sub, t0 : t0 + n]
                if along == 0
                else paired.at[sub, dest, t0 : t0 + n]
            )
        cut = (n + 1) // 2
        lo, hi = {None: (0, n), 0: (0, cut), 1: (cut, n)}[part]
        return (
            paired.at[dest, k.y, t0 + lo : t0 + hi]
            if along == 0
            else paired.at[k.x, dest, t0 + lo : t0 + hi]
        )

    def inbox(half, step, direction, part):
        n = halves[half][1]
        one = first_in[half] if step == 0 else second_in[half]
        box = one[2 + direction]
        if part is None:
            return box
        if step == 0:
            return box.at[2 * part : 2 * part + 2]
        cut = (n + 1) // 2
        return box.at[0:cut] if part == 0 else box.at[cut:n]

    def outset(half, step):
        one = first_in[half] if step == 0 else second_in[half]
        base = sems[half, step] = k.take(6)
        for direction, delta in ((0, 1), (1, -1)):
            k.start(
                view(half, step, 2, direction),
                one[direction],
                to_axis(half, step, delta),
                base + direction,
            )
        for direction, delta in ((0, 1), (1, -1)):
            part = 1 - direction
            k.start(
                view(half, step, delta, part),
                inbox(half, step, direction, part),
                to_axis(half, step, delta),
                base + 2 + direction,
            )

    def relay(half, step):
        one = first_in[half] if step == 0 else second_in[half]
        base = sems[half, step]
        for direction, delta in ((0, 1), (1, -1)):
            k.copy(
                one[direction], one[direction], to_axis(half, step, -delta), base + direction
            ).wait_recv()
            target = view(half, step, delta, direction)
            target[...] = target[...] + one[direction][...]
            k.start(
                target,
                inbox(half, step, direction, direction),
                to_axis(half, step, delta),
                base + 4 + direction,
            )

    def collect(half, step):
        base = sems[half, step]
        for direction, delta in ((0, 1), (1, -1)):
            for at, part in ((2, 1 - direction), (4, direction)):
                box = inbox(half, step, direction, part)
                k.copy(box, box, to_axis(half, step, -delta), base + at + direction).wait_recv()
        own = view(half, step, 0, None)
        f32 = jnp.float32
        own[...] = (
            own[...].astype(f32)
            + (inbox(half, step, 0, None)[...].astype(f32) + inbox(half, step, 1, None)[...].astype(f32))
        ).astype(jnp.bfloat16)

    def pair_out():
        sems["pair"] = k.take()
        k.start(grads.at[:, :, 1 - k.c, t_base : t_base + n_tiles], paired, k.at(c=1 - k.c), sems["pair"])

    def pair_in():
        k.copy(paired, paired, k.at(c=1 - k.c), sems["pair"]).wait_recv()

        @pl.loop(0, 4)
        def _(i):
            paired[i] = paired[i] + grads[i, :, k.c, t_base : t_base + n_tiles]

        for half in (0, 1):
            outset(half, 0)

    def relay_0():
        for half in (0, 1):
            relay(half, 0)

    def turn():
        for half in (0, 1):
            collect(half, 0)
            outset(half, 1)

    def relay_1():
        for half in (0, 1):
            relay(half, 1)

    def z_out():
        for half in (0, 1):
            collect(half, 1)
        base = sems["z"] = k.take(8)
        spot = 2 * k.zh + k.zl
        for q in range(4):
            for e in range(2):
                piece = piece_step * (2 * q + e)
                source = paired.at[k.x, k.y, piece : piece + piece_size]
                mine = (k.zh == q) & (k.c == e) & (k.zl == k.c)
                op = pltpu.make_async_remote_copy(
                    src_ref=source,
                    dst_ref=z_in.at[spot],
                    send_sem=k.send.at[base + 2 * q + e],
                    recv_sem=k.recv.at[base + spot],
                    device_id=k.at(zl=k.c, zh=q, c=e),
                    device_id_type=MESH,
                )

                @pl.when(jnp.logical_not(mine))
                def _():
                    op.start()

                @pl.when(mine)
                def _():
                    z_in[spot] = source[...]

                def done(op=op, mine=mine):
                    @pl.when(jnp.logical_not(mine))
                    def _():
                        op.wait_send()

                k.open.append(done)

    def z_in_sum():
        base = sems["z"]
        spot = 2 * k.zh + k.zl
        for slot in range(8):
            mine = (spot == slot) & (k.zl == k.c)

            @pl.when(jnp.logical_not(mine))
            def _():
                box = z_in.at[slot]
                k.copy(box, box, k.at(zh=slot // 2, zl=slot % 2, c=k.zl), base + slot).wait_recv()

        parts = [z_in[i].astype(jnp.float32) for i in range(8)]
        while len(parts) > 1:
            parts = [a + b for a, b in zip(parts[::2], parts[1::2])]
        p = 2 * k.zh + k.c
        gathered[p] = parts[0].astype(jnp.bfloat16)
        base = sems["g"] = k.take(7)
        for d in range(1, 8):
            to = lax.rem(p + d, 8)
            box = gathered.at[p]
            k.start(box, box, k.at(zh=to // 2, c=lax.rem(to, 2)), base + d - 1)

    def gather():
        p = 2 * k.zh + k.c
        for d in range(1, 8):
            frm = lax.rem(p + 8 - d, 8)
            box = gathered.at[frm]
            k.copy(box, box, k.at(zh=frm // 2, c=lax.rem(frm, 2)), sems["g"] + d - 1).wait_recv()

    return [pair_out, pair_in, relay_0, turn, relay_1, z_out, z_in_sum, gather]


def write_shard(t_base, n_tiles, gathered, grad_in_ref, grad_out_ref, scaling):
    piece_step, _ = pieces_of(n_tiles)
    for at in range(n_tiles):
        p = min(at // piece_step, 7)
        values = gathered[p, at - piece_step * p].astype(jnp.float32) * scaling
        tile = t_base + at
        if tile < 17:
            grad_in_ref[:, 128 * tile : 128 * tile + 128] = values
        else:
            column, half = (tile - 17) // 2, (tile - 17) % 2
            grad_out_ref[16 * half : 16 * half + 16, 128 * column : 128 * column + 128] = values


def sum_scratch(n_tiles):
    def tiles(*lead):
        return pltpu.VMEM((*lead, 16, 128), jnp.bfloat16)

    shapes = [tiles(4, 4, n_tiles)]
    for _, n in halves_of(n_tiles):
        shapes += [tiles(2, n)] * 2 + [tiles(4, n)] * 2
    for _, n in halves_of(n_tiles):
        cut = (n + 1) // 2
        shapes += [tiles(cut), tiles(n - cut), tiles(n), tiles(n)]
    return shapes + [tiles(8, pieces_of(n_tiles)[1])] * 2


def sum_refs(refs):
    return refs[0], (refs[1:5], refs[5:9]), (refs[9:13], refs[13:17]), refs[17], refs[18]


NN = (((1,), (0,)), ((), ()))
NT_DIMS = (((1,), (1,)), ((), ()))
TN = (((0,), (0,)), ((), ()))


def dot(a, b, dims=NN):
    return lax.dot_general(a, b, dims, preferred_element_type=F32)


def sigmoid(p):
    return 0.5 * jnp.tanh(0.5 * p) + 0.5


def cols(at, width=512):
    return slice(at, at + width)


def group_mask(unit):
    if unit == 0:
        return None
    row = lax.broadcasted_iota(jnp.int32, (BLOCK, BLOCK), 0)
    column = lax.broadcasted_iota(jnp.int32, (BLOCK, BLOCK), 1)
    return lax.rem(row, 16) == lax.rem(column, 16)


def positive_scores(unit, query, keyed):
    r = jnp.maximum(dot(query, keyed, NT_DIMS) * S ** (-0.5), 0.0)
    mask = group_mask(unit)
    return r if mask is None else jnp.where(mask, r, 0.0)


def length_of(unit):
    return BLOCK if unit == 0 else 16


def forward_group(m, unit, g, x):
    xf = x.astype(F32)
    scaling = lax.rsqrt(jnp.mean(xf * xf, axis=-1, keepdims=True) + EPSILON)
    hidden = (xf * scaling * m.gains[unit : unit + 1, :]).astype(BF16)
    m.hidden[unit, g] = hidden
    p = dot(hidden, m.w_in[unit, :, 2 * E :])
    m.proj[unit, g, :, 2 * E :] = p
    z = p * sigmoid(p)
    query = (z * m.scales[unit, 0:1, :]).astype(BF16)
    keyed = (z * m.scales[unit, 1:2, :]).astype(BF16)
    m.query[unit, g] = query
    m.keyed[unit, g] = keyed
    r = positive_scores(unit, query, keyed)
    weights = (r * r * (1.0 / length_of(unit))).astype(BF16)
    m.weights[unit, g] = weights
    for at in range(0, E, 512):
        p = dot(hidden, m.w_in[unit, :, cols(E + at)])
        m.proj[unit, g, :, cols(E + at)] = p
        m.value[unit, g, :, cols(at)] = (p * sigmoid(p)).astype(BF16)
        p = dot(hidden, m.w_in[unit, :, cols(at)])
        m.proj[unit, g, :, cols(at)] = p
        mixed = dot(weights, m.value[unit, g, :, cols(at)])
        m.mixed[unit, g, :, cols(at)] = mixed
        m.gated[unit, g, :, cols(at)] = (p * sigmoid(p) * mixed).astype(BF16)
    return (x.astype(F32) + dot(m.gated[unit, g], m.w_out[unit])).astype(BF16)


def backward_group(m, unit, g, x, upstream):
    for at in range(0, E, 512):
        d_gated = dot(upstream, m.w_out[unit, cols(at), :], NT_DIMS).astype(BF16).astype(F32)
        p = m.proj[unit, g, :, cols(at)]
        sig = sigmoid(p)
        gate = p * sig
        m.d_mixed[:, cols(at)] = (d_gated * gate).astype(BF16)
        slope = sig + gate * (1.0 - sig)
        m.d_proj[g, :, cols(at)] = (d_gated * m.mixed[unit, g, :, cols(at)] * slope).astype(BF16)
    d_weights = dot(m.d_mixed[...], m.value[unit, g], NT_DIMS).astype(BF16).astype(F32)
    query, keyed = m.query[unit, g], m.keyed[unit, g]
    r = positive_scores(unit, query, keyed)
    d_scores = (d_weights * r * (2.0 / length_of(unit) * S ** (-0.5))).astype(BF16)
    d_query = dot(d_scores, keyed).astype(BF16).astype(F32)
    d_keyed = dot(d_scores, query, TN).astype(BF16).astype(F32)
    p = m.proj[unit, g, :, 2 * E :]
    sig = sigmoid(p)
    z = p * sig
    d_z = d_query * m.scales[unit, 0:1, :] + d_keyed * m.scales[unit, 1:2, :]
    m.d_proj[g, :, 2 * E :] = (d_z * (sig + z * (1.0 - sig))).astype(BF16)
    m.small[unit, 4:5, :] += jnp.sum(d_query * z, axis=0, keepdims=True)
    m.small[unit, 5:6, :] += jnp.sum(d_keyed * z, axis=0, keepdims=True)
    weights = m.weights[unit, g]
    for at in range(0, E, 512):
        d_value = dot(weights, m.d_mixed[:, cols(at)], TN).astype(BF16).astype(F32)
        p = m.proj[unit, g, :, cols(E + at)]
        sig = sigmoid(p)
        m.d_proj[g, :, cols(E + at)] = (d_value * (sig + p * sig * (1.0 - sig))).astype(BF16)
    d_hidden = dot(m.d_proj[g], m.w_in[unit], NT_DIMS)
    xf = x.astype(F32)
    scaling = lax.rsqrt(jnp.mean(xf * xf, axis=-1, keepdims=True) + EPSILON)
    xs = xf * scaling
    d_gain = jnp.sum(d_hidden * xs, axis=0, keepdims=True)
    for i in range(4):
        m.small[unit, i : i + 1, :] += d_gain[:, 128 * i : 128 * i + 128]
    d_xs = d_hidden * m.gains[unit : unit + 1, :]
    d_x = scaling * (d_xs - xs * jnp.mean(d_xs * xs, axis=-1, keepdims=True))
    return (upstream.astype(F32) + d_x).astype(BF16)


def turned(m, unit):
    for g in (0, 1):
        m.hidden_t[unit, :, cols(BLOCK * g, BLOCK)] = m.hidden[unit, g].T
        m.gated_t[unit, :, cols(BLOCK * g, BLOCK)] = m.gated[unit, g].T


def weight_out_grad(m, unit, upstream):
    for i in range(4):
        rows = dot(m.gated_t[unit, cols(256 * i, 256), :], upstream).astype(BF16)
        parts = rows.reshape(4, 2, 2, 16, 512)
        for column in range(4):
            at = 17 + 2 * column
            m.grads[unit, i, :, :, at : at + 2] = parts[..., 128 * column : 128 * column + 128]


def weight_in_grad(m, unit):
    for at, width in ((0, 512), (512, 512), (1024, 512), (1536, 512), (2048, 128)):
        right = m.d_proj[:, :, cols(at, width)].reshape(2 * BLOCK, width)
        for i in (0, 1):
            part = dot(m.hidden_t[unit, cols(256 * i, 256), :], right).astype(BF16)
            part = part.reshape(2, 4, 2, 16, width)
            for j in range(width // 128):
                m.grads[unit, 2 * i : 2 * i + 2, :, :, at // 128 + j] = part[
                    ..., 128 * j : 128 * j + 128
                ]


class Memory:
    pass


SCRATCH = dict(
    w_in=((2, D, WIDE), BF16),
    w_out=((2, E, D), BF16),
    frames=((2, BLOCK, D), BF16),
    cot=((2, 8, 2, 16, D), BF16),
    first=((2, 8, 2, 16, D), BF16),
    first_pos=((2, 16, 16, D), BF16),
    cot_pos=((2, 16, 16, D), BF16),
    out_pos=((2, 16, 16, D), BF16),
    out=((2, 8, 2, 16, D), BF16),
    back_pos=((2, 16, 16, D), BF16),
    back=((2, 8, 2, 16, D), BF16),
    back_frames=((2, BLOCK, D), BF16),
    hidden=((2, 2, BLOCK, D), BF16),
    hidden_t=((2, D, 2 * BLOCK), BF16),
    proj=((2, 2, BLOCK, WIDE), F32),
    value=((2, 2, BLOCK, E), BF16),
    query=((2, 2, BLOCK, S), BF16),
    keyed=((2, 2, BLOCK, S), BF16),
    weights=((2, 2, BLOCK, BLOCK), BF16),
    mixed=((2, 2, BLOCK, E), F32),
    gated=((2, 2, BLOCK, E), BF16),
    gated_t=((2, E, 2 * BLOCK), BF16),
    d_mixed=((BLOCK, E), BF16),
    d_proj=((2, BLOCK, WIDE), BF16),
    grads=((2, 4, 4, 2, NT, 16, 128), BF16),
    small=((2, 8, 128), F32),
)
GROUPS = ((1, 0, NT), (0,) + OUT_TILES, (0,) + IN_TILES)


def step_kernel(scaling, *refs):
    m = Memory()
    frames_hbm, cot_hbm, w_in_hbm, w_out_hbm, m.scales, m.gains = refs[:6]
    out_hbm, back_hbm, in_ref, wout_ref, small_ref = refs[6:11]
    refs = refs[11:]
    for name, ref in zip(SCRATCH, refs):
        setattr(m, name, ref)
    refs = refs[len(SCRATCH) :]
    sums = []
    for unit, t0, n in GROUPS:
        sums.append(refs[:19])
        refs = refs[19:]
    small_bufs = refs[0]
    local, send, recv = refs[1:4]
    k = Links(send, recv)
    p = 2 * k.zh + k.c

    def load(src, dst, sem):
        op = pltpu.make_async_copy(src, dst, local.at[sem])
        op.start()
        return op

    loads = dict(
        frames=load(frames_hbm, m.frames, 0),
        in_0=load(w_in_hbm.at[0], m.w_in.at[0], 1),
        cot=load(cot_hbm, m.cot, 2),
        out_0=load(w_out_hbm.at[0], m.w_out.at[0], 3),
        in_1=load(w_in_hbm.at[1], m.w_in.at[1], 4),
        out_1=load(w_out_hbm.at[1], m.w_out.at[1], 5),
    )
    barrier(k)
    m.small[...] = jnp.zeros((2, 8, 128), F32)

    def peer(d):
        j = lax.rem(p + d, 8)
        return j, k.at(zh=j // 2, c=lax.rem(j, 2))

    def from_peer(d):
        j = lax.rem(p + 8 - d, 8)
        return j, k.at(zh=j // 2, c=lax.rem(j, 2))

    first_sems, cot_sems, out_sems, back_sems = k.take(28), k.take(14), k.take(14), k.take(28)

    def first_copy(b, h, d, to):
        sem = first_sems + (b * 2 + h) * 7 + d - 1
        return k.copy(m.first.at[b, to[0], h], m.first_pos.at[h, 2 * p + b], to[1], sem)

    def cot_copy(h, d, to):
        return k.copy(
            m.cot.at[:, to[0], h], m.cot_pos.at[h, pl.ds(2 * p, 2)], to[1], cot_sems + h * 7 + d - 1
        )

    def out_copy(h, d, to):
        return k.copy(
            m.out_pos.at[h, pl.ds(2 * to[0], 2)], m.out.at[:, p, h], to[1], out_sems + h * 7 + d - 1
        )

    def back_copy(b, h, d, to):
        sem = back_sems + (b * 2 + h) * 7 + d - 1
        return k.copy(m.back_pos.at[h, 2 * to[0] + b], m.back.at[b, p, h], to[1], sem)

    def send_cot(h):
        for d in range(1, 8):
            cot_copy(h, d, peer(d)).start()
        m.cot_pos[h, pl.ds(2 * p, 2)] = m.cot[:, p, h]

    def send_out(h):
        for d in range(1, 8):
            out_copy(h, d, peer(d)).start()

    loads["cot"].wait()
    send_cot(0)
    loads["frames"].wait()
    loads["in_0"].wait()
    loads["out_0"].wait()

    @pl.loop(0, 2)
    def _(b):
        m.first[b] = forward_group(m, 0, b, m.frames[b]).reshape(8, 2, 16, D)
        for h in (0, 1):
            for d in range(1, 8):
                first_copy(b, h, d, peer(d)).start()
        m.first_pos[:, 2 * p + b] = m.first[b, p]

    send_cot(1)
    turned(m, 0)
    loads["in_1"].wait()
    loads["out_1"].wait()

    @pl.loop(0, 2)
    def _(h):
        for b in (0, 1):
            for d in range(1, 8):
                first_copy(b, h, d, from_peer(d)).wait_recv()
        x = m.first_pos[h].reshape(BLOCK, D)
        m.out_pos[h] = forward_group(m, 1, h, x).reshape(16, 16, D)

        @pl.when(h == 0)
        def _():
            send_out(0)

        m.out[:, p, h] = m.out_pos[h, pl.ds(2 * p, 2)]

    @pl.loop(0, 2)
    def _(h):
        for d in range(1, 8):
            cot_copy(h, d, from_peer(d)).wait_recv()
        x = m.first_pos[h].reshape(BLOCK, D)
        upstream = m.cot_pos[h].reshape(BLOCK, D)
        m.back_pos[h] = backward_group(m, 1, h, x, upstream).reshape(16, 16, D)
        for b in (0, 1):
            for d in range(1, 8):
                back_copy(b, h, d, peer(d)).start()
        m.back[:, p, h] = m.back_pos[h, pl.ds(2 * p, 2)]

    send_out(1)
    turned(m, 1)

    late, early_out, early_in = (
        sum_stages(k, m.grads.at[unit], t0, n, *sum_refs(s)) for (unit, t0, n), s in zip(GROUPS, sums)
    )
    late_small = small_sum(k, small_bufs.at[1], m.small.at[1], small_ref.at[1])
    early_small = small_sum(k, small_bufs.at[0], m.small.at[0], small_ref.at[0])

    def run(*groups):
        for group in groups:
            if group:
                group.pop(0)()

    weight_out_grad(m, 1, m.cot_pos[...].reshape(2 * BLOCK, D))
    weight_in_grad(m, 1)
    run(late, late_small)
    run(late, late_small)

    def wait_back(b):
        for h in (0, 1):
            for d in range(1, 8):
                back_copy(b, h, d, from_peer(d)).wait_recv()

    wait_back(0)
    m.back_frames[0] = backward_group(m, 0, 0, m.frames[0], m.back[0].reshape(BLOCK, D))
    run(late, late_small)
    wait_back(1)
    weight_out_grad(m, 0, m.back[...].reshape(2 * BLOCK, D))
    run(early_out)
    run(late, late_small)
    m.back_frames[1] = backward_group(m, 0, 1, m.frames[1], m.back[1].reshape(BLOCK, D))
    store_back = load(m.back_frames, back_hbm, 0)
    run(early_out, early_small)
    run(late, late_small)
    weight_in_grad(m, 0)
    run(early_in)
    run(early_out, late, early_small)
    for h in (0, 1):
        for d in range(1, 8):
            out_copy(h, d, from_peer(d)).wait_recv()
    store_out = load(m.out, out_hbm, 2)
    while early_in:
        run(early_in, early_out, late, early_small)
    for (unit, t0, n), s in zip(GROUPS, sums):
        write_shard(t0, n, s[18], in_ref.at[unit], wout_ref.at[unit], scaling)
    small_ref[...] = small_ref[...] * scaling
    k.drain()

    @pl.loop(0, 2)
    def _(h):
        for d in range(1, 8):
            to = peer(d)
            cot_copy(h, d, to).wait_send()
            out_copy(h, d, to).wait_send()
            for b in (0, 1):
                first_copy(b, h, d, to).wait_send()
                back_copy(b, h, d, to).wait_send()

    store_back.wait()
    store_out.wait()


def on_device(frames, cotangent, weight_in, qk_scales, weight_out, gains):
    tokens_all = frames.shape[0] * frames.shape[1] * lax.axis_size(DP) * lax.axis_size(SEQ)
    vmem = pl.BlockSpec(memory_space=pltpu.VMEM)
    hbm = pl.BlockSpec(memory_space=pl.ANY)
    scratch = [pltpu.VMEM(shape, dtype) for shape, dtype in SCRATCH.values()]
    for _, _, n in GROUPS:
        scratch += sum_scratch(n)
    scratch += [pltpu.VMEM((2, 17, 8, 128), F32)]
    dma = pltpu.SemaphoreType.DMA
    scratch += [dma((6,)), dma((SEMS,)), dma((SEMS,))]
    result, back, grad_in, grad_out, small = pl.pallas_call(
        functools.partial(step_kernel, tokens_all ** (-0.5)),
        out_shape=(
            jax.ShapeDtypeStruct((2, 8, 2, 16, D), BF16),
            jax.ShapeDtypeStruct((2, BLOCK, D), BF16),
            jax.ShapeDtypeStruct((2, 16, WIDE), F32),
            jax.ShapeDtypeStruct((2, 32, D), F32),
            jax.ShapeDtypeStruct((2, 8, 128), F32),
        ),
        in_specs=[hbm, hbm, hbm, hbm, vmem, vmem],
        out_specs=(hbm, hbm, vmem, vmem, vmem),
        scratch_shapes=scratch,
        compiler_params=pltpu.CompilerParams(
            collective_id=0, has_side_effects=True, vmem_limit_bytes=67_043_328
        ),
    )(
        frames.reshape(2, BLOCK, D),
        cotangent.reshape(2, 8, 2, 16, D),
        weight_in,
        weight_out,
        qk_scales,
        gains,
    )
    return (
        result.reshape(frames.shape),
        back.reshape(frames.shape),
        grad_in,
        grad_out,
        small[:, :4].reshape(2, D),
        small[:, 4:6],
    )


def solution(mesh):
    split = Mesh(mesh.devices.reshape(4, 4, 2, 4, 2), DP + SEQ)
    placed = (P(DP, SEQ, None), P(DP, SEQ, None), P(), P(), P(), P())
    return jax.shard_map(
        on_device,
        mesh=split,
        in_specs=placed,
        out_specs=(
            P(DP, SEQ, None),
            P(DP, SEQ, None),
            P(None, DP, None),
            P(None, DP, None),
            P(),
            P(),
        ),
        check_vma=False,
    )
```

```python
import functools

import jax
import jax.numpy as jnp
from jax import lax
from jax.experimental import pallas as pl
from jax.experimental.pallas import tpu as pltpu
from jax.sharding import Mesh
from jax.sharding import PartitionSpec as P

DP = ("dp_0", "dp_1", "dp_2")
SEQ = ("seq_0", "seq_1")
D, E, S, BLOCK = 512, 1024, 128, 256
WIDE = 2 * E + S
EPSILON = 1e-06
F32, BF16 = jnp.float32, jnp.bfloat16
NT = 25
SEMS = 300


MESH = pl.DeviceIdType.MESH


def halves_of(n):
    return ((0, (n + 1) // 2), ((n + 1) // 2, n // 2))


def pieces_of(n):
    return n // 8, n - 7 * (n // 8)


class Links:
    def __init__(self, send, recv):
        self.send, self.recv, self.used, self.open = send, recv, 0, []
        self.x, self.y, self.zl = (lax.axis_index(a) for a in DP)
        self.zh, self.c = (lax.axis_index(a) for a in SEQ)

    def take(self, count=1):
        at = self.used
        self.used += count
        return at

    def at(self, x=None, y=None, zl=None, zh=None, c=None):
        return (
            self.x if x is None else x,
            self.y if y is None else y,
            self.zl if zl is None else zl,
            self.zh if zh is None else zh,
            self.c if c is None else c,
        )

    def copy(self, src, dst, target, sem, recv_sem=None):
        return pltpu.make_async_remote_copy(
            src_ref=src,
            dst_ref=dst,
            send_sem=self.send.at[sem],
            recv_sem=self.recv.at[sem if recv_sem is None else recv_sem],
            device_id=target,
            device_id_type=MESH,
        )

    def start(self, src, dst, target, sem):
        op = self.copy(src, dst, target, sem)
        op.start()
        self.open.append(op)
        return op

    def drain(self):
        for op in self.open:
            if callable(op):
                op()
            else:
                op.wait_send()
        self.open = []


def mod4(v):
    return lax.rem(v + 4, 4)


def greet(k):
    sem = pltpu.get_barrier_semaphore()
    targets = [k.at(x=mod4(k.x + d)) for d in (1, 2, 3)]
    targets += [k.at(y=mod4(k.y + d)) for d in (1, 2, 3)]
    for dl in (0, 1):
        for dh in range(4):
            for dc in (0, 1):
                if dl or dh or dc:
                    targets.append(
                        k.at(zl=lax.rem(k.zl + dl, 2), zh=mod4(k.zh + dh), c=lax.rem(k.c + dc, 2))
                    )
    for target in targets:
        pl.semaphore_signal(sem, inc=1, device_id=target, device_id_type=MESH)
    return lambda: pl.semaphore_wait(sem, len(targets))


def small_sum(k, buf, value_ref, out_ref):
    f32_pair, f32_x, f32_y, f32_z = 0, 1, 5, 9
    sems = {}

    def pair():
        sems["p"] = k.take()
        k.start(value_ref, buf.at[f32_pair], k.at(c=1 - k.c), sems["p"])

    def x():
        k.copy(value_ref, buf.at[f32_pair], k.at(c=1 - k.c), sems["p"]).wait_recv()
        buf[f32_x + k.x] = value_ref[...] + buf[f32_pair]
        sems["x"] = k.take(3)
        for d in (1, 2, 3):
            src = buf.at[f32_x + k.x]
            k.start(src, src, k.at(x=mod4(k.x + d)), sems["x"] + d - 1)

    def y():
        for d in (1, 2, 3):
            slot = buf.at[f32_x + mod4(k.x - d)]
            k.copy(slot, slot, k.at(x=mod4(k.x - d)), sems["x"] + d - 1).wait_recv()
        buf[f32_y + k.y] = (buf[f32_x] + buf[f32_x + 1]) + (buf[f32_x + 2] + buf[f32_x + 3])
        sems["y"] = k.take(3)
        for d in (1, 2, 3):
            src = buf.at[f32_y + k.y]
            k.start(src, src, k.at(y=mod4(k.y + d)), sems["y"] + d - 1)

    def z():
        for d in (1, 2, 3):
            slot = buf.at[f32_y + mod4(k.y - d)]
            k.copy(slot, slot, k.at(y=mod4(k.y - d)), sems["y"] + d - 1).wait_recv()
        me = 2 * k.zh + k.zl
        buf[f32_z + me] = (buf[f32_y] + buf[f32_y + 1]) + (buf[f32_y + 2] + buf[f32_y + 3])
        sems["z"] = k.take(7)
        for d in range(1, 8):
            to = lax.rem(me + d, 8)
            src = buf.at[f32_z + me]
            k.start(src, src, k.at(zh=to // 2, zl=lax.rem(to, 2)), sems["z"] + d - 1)

    def end():
        me = 2 * k.zh + k.zl
        for d in range(1, 8):
            frm = lax.rem(me + 8 - d, 8)
            slot = buf.at[f32_z + frm]
            k.copy(slot, slot, k.at(zh=frm // 2, zl=lax.rem(frm, 2)), sems["z"] + d - 1).wait_recv()
        parts = [buf[f32_z + i] for i in range(8)]
        while len(parts) > 1:
            parts = [a + b for a, b in zip(parts[::2], parts[1::2])]
        out_ref[...] = parts[0]

    return [pair, x, y, z, end]


def sum_stages(k, grads, t_base, n_tiles, direct, paired, first_in, second_in, z_in, gathered):
    halves = halves_of(n_tiles)
    piece_step, piece_size = pieces_of(n_tiles)
    sems = {}
    me = (k.x, k.y)

    def to_axis(half, step, delta):
        along = (half + step) % 2
        return k.at(x=mod4(k.x + delta)) if along == 0 else k.at(y=mod4(k.y + delta))

    def view(half, step, delta, part):
        t0, n = halves[half]
        along = (half + step) % 2
        dest = mod4(me[along] + delta)
        if step == 0:
            sub = pl.ds(0, 4) if part is None else pl.ds(2 * part, 2)
            return (
                paired.at[dest, sub, t0 : t0 + n]
                if along == 0
                else paired.at[sub, dest, t0 : t0 + n]
            )
        cut = (n + 1) // 2
        lo, hi = {None: (0, n), 0: (0, cut), 1: (cut, n)}[part]
        return (
            paired.at[dest, k.y, t0 + lo : t0 + hi]
            if along == 0
            else paired.at[k.x, dest, t0 + lo : t0 + hi]
        )

    def inbox(half, step, direction, part):
        n = halves[half][1]
        one = first_in[half] if step == 0 else second_in[half]
        box = one[2 + direction]
        if part is None:
            return box
        if step == 0:
            return box.at[2 * part : 2 * part + 2]
        cut = (n + 1) // 2
        return box.at[0:cut] if part == 0 else box.at[cut:n]

    def outset(half, step):
        one = first_in[half] if step == 0 else second_in[half]
        base = sems[half, step] = k.take(6)
        for direction, delta in ((0, 1), (1, -1)):
            k.start(
                view(half, step, 2, direction),
                one[direction],
                to_axis(half, step, delta),
                base + direction,
            )
        for direction, delta in ((0, 1), (1, -1)):
            part = 1 - direction
            k.start(
                view(half, step, delta, part),
                inbox(half, step, direction, part),
                to_axis(half, step, delta),
                base + 2 + direction,
            )

    def relay(half, step):
        one = first_in[half] if step == 0 else second_in[half]
        base = sems[half, step]
        for direction, delta in ((0, 1), (1, -1)):
            k.copy(
                one[direction], one[direction], to_axis(half, step, -delta), base + direction
            ).wait_recv()
            target = view(half, step, delta, direction)
            target[...] = target[...] + one[direction][...]
            k.start(
                target,
                inbox(half, step, direction, direction),
                to_axis(half, step, delta),
                base + 4 + direction,
            )

    def collect(half, step):
        base = sems[half, step]
        for direction, delta in ((0, 1), (1, -1)):
            for at, part in ((2, 1 - direction), (4, direction)):
                box = inbox(half, step, direction, part)
                k.copy(box, box, to_axis(half, step, -delta), base + at + direction).wait_recv()
        own = view(half, step, 0, None)
        f32 = jnp.float32
        own[...] = (
            own[...].astype(f32)
            + (inbox(half, step, 0, None)[...].astype(f32) + inbox(half, step, 1, None)[...].astype(f32))
        ).astype(jnp.bfloat16)

    def pair_out():
        sems["pair"] = k.take()
        k.start(grads.at[:, :, 1 - k.c, t_base : t_base + n_tiles], paired, k.at(c=1 - k.c), sems["pair"])

    def pair_in():
        k.copy(paired, paired, k.at(c=1 - k.c), sems["pair"]).wait_recv()

        @pl.loop(0, 4)
        def _(i):
            paired[i] = paired[i] + grads[i, :, k.c, t_base : t_base + n_tiles]

        for half in (0, 1):
            outset(half, 0)

    def relay_0():
        for half in (0, 1):
            relay(half, 0)

    def turn():
        for half in (0, 1):
            collect(half, 0)
            outset(half, 1)

    def relay_1():
        for half in (0, 1):
            relay(half, 1)

    def z_out():
        for half in (0, 1):
            collect(half, 1)
        base = sems["z"] = k.take(8)
        spot = 2 * k.zh + k.zl
        for q in range(4):
            for e in range(2):
                piece = piece_step * (2 * q + e)
                source = paired.at[k.x, k.y, piece : piece + piece_size]
                mine = (k.zh == q) & (k.c == e) & (k.zl == k.c)
                op = pltpu.make_async_remote_copy(
                    src_ref=source,
                    dst_ref=z_in.at[spot],
                    send_sem=k.send.at[base + 2 * q + e],
                    recv_sem=k.recv.at[base + spot],
                    device_id=k.at(zl=k.c, zh=q, c=e),
                    device_id_type=MESH,
                )

                @pl.when(jnp.logical_not(mine))
                def _():
                    op.start()

                @pl.when(mine)
                def _():
                    z_in[spot] = source[...]

                def done(op=op, mine=mine):
                    @pl.when(jnp.logical_not(mine))
                    def _():
                        op.wait_send()

                k.open.append(done)

    def z_in_sum():
        base = sems["z"]
        spot = 2 * k.zh + k.zl
        for slot in range(8):
            mine = (spot == slot) & (k.zl == k.c)

            @pl.when(jnp.logical_not(mine))
            def _():
                box = z_in.at[slot]
                k.copy(box, box, k.at(zh=slot // 2, zl=slot % 2, c=k.zl), base + slot).wait_recv()

        parts = [z_in[i].astype(jnp.float32) for i in range(8)]
        while len(parts) > 1:
            parts = [a + b for a, b in zip(parts[::2], parts[1::2])]
        p = 2 * k.zh + k.c
        gathered[p] = parts[0].astype(jnp.bfloat16)
        base = sems["g"] = k.take(7)
        for d in range(1, 8):
            to = lax.rem(p + d, 8)
            box = gathered.at[p]
            k.start(box, box, k.at(zh=to // 2, c=lax.rem(to, 2)), base + d - 1)

    def gather():
        p = 2 * k.zh + k.c
        for d in range(1, 8):
            frm = lax.rem(p + 8 - d, 8)
            box = gathered.at[frm]
            k.copy(box, box, k.at(zh=frm // 2, c=lax.rem(frm, 2)), sems["g"] + d - 1).wait_recv()

    spot = 2 * k.zh + k.zl
    holds = k.zl == k.c

    def whole_copy(q):
        return pltpu.make_async_remote_copy(
            src_ref=paired.at[k.x, k.y],
            dst_ref=z_in.at[spot],
            send_sem=k.send.at[sems["z"] + q],
            recv_sem=k.recv.at[sems["z"] + spot],
            device_id=k.at(zl=k.c, zh=q),
            device_id_type=MESH,
        )

    def whole_out():
        for half in (0, 1):
            collect(half, 1)
        sems["z"] = k.take(8)
        for q in range(4):
            mine = holds & (k.zh == q)
            op = whole_copy(q)

            @pl.when(jnp.logical_not(mine))
            def _():
                op.start()

            def done(op=op, mine=mine):
                @pl.when(jnp.logical_not(mine))
                def _():
                    op.wait_send()

            k.open.append(done)

        @pl.when(holds)
        def _():
            z_in[spot] = paired[k.x, k.y]

    def whole_sum():
        sems["g"] = k.take()
        across = k.copy(gathered, gathered, k.at(c=1 - k.c), sems["g"])

        @pl.when(holds)
        def _():
            for slot in range(8):

                @pl.when(spot != slot)
                def _():
                    box = z_in.at[slot]
                    k.copy(
                        box, box, k.at(zh=slot // 2, zl=slot % 2), sems["z"] + slot
                    ).wait_recv()

            parts = [z_in[i].astype(jnp.float32) for i in range(8)]
            while len(parts) > 1:
                parts = [a + b for a, b in zip(parts[::2], parts[1::2])]
            gathered[0] = parts[0].astype(jnp.bfloat16)
            across.start()

        def done():
            @pl.when(holds)
            def _():
                across.wait_send()

        k.open.append(done)

    def whole_in():
        @pl.when(jnp.logical_not(holds))
        def _():
            k.copy(gathered, gathered, k.at(c=1 - k.c), sems["g"]).wait_recv()

    if direct:
        return [pair_out, pair_in, relay_0, turn, relay_1, whole_out, whole_sum, whole_in]
    return [pair_out, pair_in, relay_0, turn, relay_1, z_out, z_in_sum, gather]


def write_shard(t_base, n_tiles, direct, gathered, grad_in_ref, grad_out_ref, scaling):
    piece_step = n_tiles if direct else pieces_of(n_tiles)[0]
    for at in range(n_tiles):
        p = min(at // piece_step, 7)
        values = gathered[p, at - piece_step * p].astype(jnp.float32) * scaling
        tile = t_base + at
        if tile < 8:
            column, half = tile // 2, tile % 2
            grad_out_ref[16 * half : 16 * half + 16, 128 * column : 128 * column + 128] = values
        else:
            grad_in_ref[:, 128 * (tile - 8) : 128 * (tile - 7)] = values


def sum_scratch(n_tiles, direct):
    def tiles(*lead):
        return pltpu.VMEM((*lead, 16, 128), jnp.bfloat16)

    shapes = [tiles(4, 4, n_tiles)]
    for _, n in halves_of(n_tiles):
        shapes += [tiles(2, n)] * 2 + [tiles(4, n)] * 2
    for _, n in halves_of(n_tiles):
        cut = (n + 1) // 2
        shapes += [tiles(cut), tiles(n - cut), tiles(n), tiles(n)]
    if direct:
        return shapes + [tiles(8, n_tiles), tiles(1, n_tiles)]
    return shapes + [tiles(8, pieces_of(n_tiles)[1])] * 2


def sum_refs(refs):
    return refs[0], (refs[1:5], refs[5:9]), (refs[9:13], refs[13:17]), refs[17], refs[18]


NN = (((1,), (0,)), ((), ()))
NT_DIMS = (((1,), (1,)), ((), ()))
TN = (((0,), (0,)), ((), ()))


def dot(a, b, dims=NN):
    return lax.dot_general(a, b, dims, preferred_element_type=F32)


def sigmoid(p):
    return 0.5 * jnp.tanh(0.5 * p) + 0.5


def cols(at, width=512):
    return slice(at, at + width)


def group_mask(unit):
    if unit == 0:
        return None
    row = lax.broadcasted_iota(jnp.int32, (BLOCK, BLOCK), 0)
    column = lax.broadcasted_iota(jnp.int32, (BLOCK, BLOCK), 1)
    return lax.rem(row, 16) == lax.rem(column, 16)


def positive_scores(unit, query, keyed):
    r = jnp.maximum(dot(query, keyed, NT_DIMS) * S ** (-0.5), 0.0)
    mask = group_mask(unit)
    return r if mask is None else jnp.where(mask, r, 0.0)


def length_of(unit):
    return BLOCK if unit == 0 else 16


def forward_group(m, unit, g, x):
    xf = x.astype(F32)
    scaling = lax.rsqrt(jnp.mean(xf * xf, axis=-1, keepdims=True) + EPSILON)
    hidden = (xf * scaling * m.gains[unit : unit + 1, :]).astype(BF16)
    m.hidden[unit, g] = hidden
    p = dot(hidden, m.w_in[unit, :, 2 * E :])
    m.proj[unit, g, :, 2 * E :] = p
    z = p * sigmoid(p)
    query = (z * m.scales[unit, 0:1, :]).astype(BF16)
    keyed = (z * m.scales[unit, 1:2, :]).astype(BF16)
    m.query[unit, g] = query
    m.keyed[unit, g] = keyed
    r = positive_scores(unit, query, keyed)
    weights = (r * r * (1.0 / length_of(unit))).astype(BF16)
    m.weights[unit, g] = weights
    for at in range(0, E, 512):
        p = dot(hidden, m.w_in[unit, :, cols(E + at)])
        m.proj[unit, g, :, cols(E + at)] = p
        m.value[unit, g, :, cols(at)] = (p * sigmoid(p)).astype(BF16)
        p = dot(hidden, m.w_in[unit, :, cols(at)])
        m.proj[unit, g, :, cols(at)] = p
        mixed = dot(weights, m.value[unit, g, :, cols(at)])
        m.mixed[unit, g, :, cols(at)] = mixed
        m.gated[unit, g, :, cols(at)] = (p * sigmoid(p) * mixed).astype(BF16)
    return (x.astype(F32) + dot(m.gated[unit, g], m.w_out[unit])).astype(BF16)


def backward_gate(m, unit, g, upstream):
    for at in range(0, E, 512):
        d_gated = dot(upstream, m.w_out[unit, cols(at), :], NT_DIMS).astype(BF16).astype(F32)
        p = m.proj[unit, g, :, cols(at)]
        sig = sigmoid(p)
        gate = p * sig
        m.d_mixed[g, :, cols(at)] = (d_gated * gate).astype(BF16)
        slope = sig + gate * (1.0 - sig)
        m.d_proj[g, :, cols(at)] = (d_gated * m.mixed[unit, g, :, cols(at)] * slope).astype(BF16)


def backward_attention(m, unit, g):
    d_weights = dot(m.d_mixed[g], m.value[unit, g], NT_DIMS).astype(BF16).astype(F32)
    query, keyed = m.query[unit, g], m.keyed[unit, g]
    r = positive_scores(unit, query, keyed)
    d_scores = (d_weights * r * (2.0 / length_of(unit) * S ** (-0.5))).astype(BF16)
    d_query = dot(d_scores, keyed).astype(BF16).astype(F32)
    d_keyed = dot(d_scores, query, TN).astype(BF16).astype(F32)
    p = m.proj[unit, g, :, 2 * E :]
    sig = sigmoid(p)
    z = p * sig
    d_z = d_query * m.scales[unit, 0:1, :] + d_keyed * m.scales[unit, 1:2, :]
    m.d_proj[g, :, 2 * E :] = (d_z * (sig + z * (1.0 - sig))).astype(BF16)
    m.small[unit, 4:5, :] += jnp.sum(d_query * z, axis=0, keepdims=True)
    m.small[unit, 5:6, :] += jnp.sum(d_keyed * z, axis=0, keepdims=True)
    weights = m.weights[unit, g]
    for at in range(0, E, 512):
        d_value = dot(weights, m.d_mixed[g, :, cols(at)], TN).astype(BF16).astype(F32)
        p = m.proj[unit, g, :, cols(E + at)]
        sig = sigmoid(p)
        m.d_proj[g, :, cols(E + at)] = (d_value * (sig + p * sig * (1.0 - sig))).astype(BF16)


def backward_input(m, unit, g, x, upstream):
    d_hidden = dot(m.d_proj[g], m.w_in[unit], NT_DIMS)
    xf = x.astype(F32)
    scaling = lax.rsqrt(jnp.mean(xf * xf, axis=-1, keepdims=True) + EPSILON)
    xs = xf * scaling
    d_gain = jnp.sum(d_hidden * xs, axis=0, keepdims=True)
    for i in range(4):
        m.small[unit, i : i + 1, :] += d_gain[:, 128 * i : 128 * i + 128]
    d_xs = d_hidden * m.gains[unit : unit + 1, :]
    d_x = scaling * (d_xs - xs * jnp.mean(d_xs * xs, axis=-1, keepdims=True))
    return (upstream.astype(F32) + d_x).astype(BF16)


def turned(m, unit):
    for g in (0, 1):
        m.hidden_t[unit, :, cols(BLOCK * g, BLOCK)] = m.hidden[unit, g].T
        m.gated_t[unit, :, cols(BLOCK * g, BLOCK)] = m.gated[unit, g].T


def weight_out_grad(m, unit, upstream):
    for i in range(4):
        rows = dot(m.gated_t[unit, cols(256 * i, 256), :], upstream).astype(BF16)
        parts = rows.reshape(4, 2, 2, 16, 512)
        for column in range(4):
            at = 2 * column
            m.grads[unit, i, :, :, at : at + 2] = parts[..., 128 * column : 128 * column + 128]


GATE = ((0, 512), (512, 512))
OTHERS = ((1024, 512), (1536, 512), (2048, 128))


def weight_in_grad(m, unit, columns):
    for at, width in columns:
        right = m.d_proj[:, :, cols(at, width)].reshape(2 * BLOCK, width)
        for i in (0, 1):
            part = dot(m.hidden_t[unit, cols(256 * i, 256), :], right).astype(BF16)
            part = part.reshape(2, 4, 2, 16, width)
            for j in range(width // 128):
                m.grads[unit, 2 * i : 2 * i + 2, :, :, 8 + at // 128 + j] = part[
                    ..., 128 * j : 128 * j + 128
                ]


class Memory:
    pass


SCRATCH = dict(
    w_in=((2, D, WIDE), BF16),
    w_out=((2, E, D), BF16),
    frames=((2, BLOCK, D), BF16),
    cot=((2, 8, 2, 16, D), BF16),
    first=((2, 8, 2, 16, D), BF16),
    first_pos=((2, 16, 16, D), BF16),
    cot_pos=((2, 16, 16, D), BF16),
    out_pos=((2, 16, 16, D), BF16),
    out=((2, 8, 2, 16, D), BF16),
    back_pos=((2, 16, 16, D), BF16),
    back=((2, 8, 2, 16, D), BF16),
    back_frames=((2, BLOCK, D), BF16),
    hidden=((2, 2, BLOCK, D), BF16),
    hidden_t=((2, D, 2 * BLOCK), BF16),
    proj=((2, 2, BLOCK, WIDE), F32),
    value=((2, 2, BLOCK, E), BF16),
    query=((2, 2, BLOCK, S), BF16),
    keyed=((2, 2, BLOCK, S), BF16),
    weights=((2, 2, BLOCK, BLOCK), BF16),
    mixed=((2, 2, BLOCK, E), F32),
    gated=((2, 2, BLOCK, E), BF16),
    gated_t=((2, E, 2 * BLOCK), BF16),
    d_mixed=((2, BLOCK, E), BF16),
    d_proj=((2, BLOCK, WIDE), BF16),
    grads=((2, 4, 4, 2, NT, 16, 128), BF16),
    small=((2, 8, 128), F32),
)
GROUPS = ((1, 0, NT, False), (0, 0, 16, False), (0, 16, 9, True))


def step_kernel(scaling, *refs):
    m = Memory()
    frames_hbm, cot_hbm, w_in_hbm, w_out_hbm, m.scales, m.gains = refs[:6]
    out_hbm, back_hbm, in_ref, wout_ref, small_ref = refs[6:11]
    refs = refs[11:]
    for name, ref in zip(SCRATCH, refs):
        setattr(m, name, ref)
    refs = refs[len(SCRATCH) :]
    sums = []
    for _ in GROUPS:
        sums.append(refs[:19])
        refs = refs[19:]
    small_bufs = refs[0]
    local, send, recv = refs[1:4]
    k = Links(send, recv)
    p = 2 * k.zh + k.c

    def load(src, dst, sem):
        op = pltpu.make_async_copy(src, dst, local.at[sem])
        op.start()
        return op

    met = greet(k)
    loads = dict(
        frames=load(frames_hbm, m.frames, 0),
        in_0=load(w_in_hbm.at[0], m.w_in.at[0], 1),
        out_0=load(w_out_hbm.at[0], m.w_out.at[0], 3),
        cot=load(cot_hbm, m.cot, 2),
        in_1=load(w_in_hbm.at[1], m.w_in.at[1], 4),
        out_1=load(w_out_hbm.at[1], m.w_out.at[1], 5),
    )
    m.small[...] = jnp.zeros((2, 8, 128), F32)

    def peer(d):
        j = lax.rem(p + d, 8)
        return j, k.at(zh=j // 2, c=lax.rem(j, 2))

    def from_peer(d):
        j = lax.rem(p + 8 - d, 8)
        return j, k.at(zh=j // 2, c=lax.rem(j, 2))

    first_sems, cot_sems, out_sems, back_sems = (k.take(14) for _ in range(4))

    def first_copy(h, d, to):
        box = m.first_pos.at[h, pl.ds(2 * p, 2)]
        return k.copy(m.first.at[:, to[0], h], box, to[1], first_sems + h * 7 + d - 1)

    def cot_copy(h, d, to):
        box = m.cot_pos.at[h, pl.ds(2 * p, 2)]
        return k.copy(m.cot.at[:, to[0], h], box, to[1], cot_sems + h * 7 + d - 1)

    def out_copy(h, d, to):
        box = m.out.at[:, p, h]
        return k.copy(m.out_pos.at[h, pl.ds(2 * to[0], 2)], box, to[1], out_sems + h * 7 + d - 1)

    def back_copy(h, d, to):
        box = m.back.at[:, p, h]
        return k.copy(m.back_pos.at[h, pl.ds(2 * to[0], 2)], box, to[1], back_sems + h * 7 + d - 1)

    def send(copy, h):
        for d in range(1, 8):
            copy(h, d, peer(d)).start()

    def receive(copy, h):
        for d in range(1, 8):
            copy(h, d, from_peer(d)).wait_recv()

    loads["frames"].wait()
    loads["in_0"].wait()
    loads["out_0"].wait()
    with jax.named_scope("f0"):

        @pl.loop(0, 2)
        def _(b):
            m.first[b] = forward_group(m, 0, b, m.frames[b]).reshape(8, 2, 16, D)

    with jax.named_scope("barrier"):
        met()
    for h in (0, 1):
        send(first_copy, h)
        m.first_pos[h, pl.ds(2 * p, 2)] = m.first[:, p, h]
    loads["cot"].wait()
    for h in (0, 1):
        send(cot_copy, h)
        m.cot_pos[h, pl.ds(2 * p, 2)] = m.cot[:, p, h]
    with jax.named_scope("turn0"):
        turned(m, 0)
    loads["in_1"].wait()
    loads["out_1"].wait()

    @pl.loop(0, 2)
    def _(h):
        with jax.named_scope("w_first"):
            receive(first_copy, h)
        with jax.named_scope("f1"):
            x = m.first_pos[h].reshape(BLOCK, D)
            m.out_pos[h] = forward_group(m, 1, h, x).reshape(16, 16, D)

    m.out[:, p] = m.out_pos[:, pl.ds(2 * p, 2)].transpose(1, 0, 2, 3)
    with jax.named_scope("turn1"):
        turned(m, 1)

    @pl.loop(0, 2)
    def _(h):
        with jax.named_scope("w_cot"):
            receive(cot_copy, h)
        with jax.named_scope("b1"):
            x = m.first_pos[h].reshape(BLOCK, D)
            upstream = m.cot_pos[h].reshape(BLOCK, D)
            backward_gate(m, 1, h, upstream)
            backward_attention(m, 1, h)
            m.back_pos[h] = backward_input(m, 1, h, x, upstream).reshape(16, 16, D)
        send(back_copy, h)
        m.back[:, p, h] = m.back_pos[h, pl.ds(2 * p, 2)]

    late, early, last = (
        sum_stages(k, m.grads.at[unit], t0, n, direct, *sum_refs(s))
        for (unit, t0, n, direct), s in zip(GROUPS, sums)
    )
    late_small = small_sum(k, small_bufs.at[1], m.small.at[1], small_ref.at[1])
    early_small = small_sum(k, small_bufs.at[0], m.small.at[0], small_ref.at[0])
    names = dict(zip(map(id, (late, early, last)), ("late", "early", "last")))

    def run(*groups):
        for group in groups:
            if group:
                with jax.named_scope(f"{names.get(id(group), 'small')}{8 - len(group)}"):
                    group.pop(0)()

    with jax.named_scope("wg1"):
        weight_out_grad(m, 1, m.cot_pos[...].reshape(2 * BLOCK, D))
        weight_in_grad(m, 1, GATE + OTHERS)
    run(late, late_small)
    run(late, late_small)
    with jax.named_scope("w_back"):
        receive(back_copy, 0)
        receive(back_copy, 1)
    for h in (0, 1):
        send(out_copy, h)
    with jax.named_scope("gate0"):
        for g in (0, 1):
            backward_gate(m, 0, g, m.back[g].reshape(BLOCK, D))
    with jax.named_scope("wg0"):
        weight_out_grad(m, 0, m.back[...].reshape(2 * BLOCK, D))
        weight_in_grad(m, 0, GATE)
    run(early, late)
    with jax.named_scope("attn0"):
        for g in (0, 1):
            backward_attention(m, 0, g)
    run(early)
    with jax.named_scope("wg0b"):
        weight_in_grad(m, 0, OTHERS)
    run(last, late, late_small)
    with jax.named_scope("input0"):
        for g in (0, 1):
            m.back_frames[g] = backward_input(m, 0, g, m.frames[g], m.back[g].reshape(BLOCK, D))
    store_back = load(m.back_frames, back_hbm, 0)
    run(early_small, last, early, late, late_small)
    run(last, early_small, early, late, late_small)
    run(last, early_small, early, late, late_small)
    with jax.named_scope("w_out"):
        receive(out_copy, 0)
        receive(out_copy, 1)
    store_out = load(m.out, out_hbm, 2)
    while last or early or late or early_small or late_small:
        run(last, early_small, early, late, late_small)
    with jax.named_scope("write"):
        for (unit, t0, n, direct), s in zip(GROUPS, sums):
            write_shard(t0, n, direct, s[18], in_ref.at[unit], wout_ref.at[unit], scaling)
        small_ref[...] = small_ref[...] * scaling
    with jax.named_scope("drain"):
        k.drain()

        @pl.loop(0, 2)
        def _(h):
            for d in range(1, 8):
                to = peer(d)
                for copy in (first_copy, cot_copy, out_copy, back_copy):
                    copy(h, d, to).wait_send()

        store_back.wait()
        store_out.wait()


def write_kernel(result, back, grad_in, grad_out, small, o_result, o_back, o_in, o_out, o_gains, o_scales):
    o_result[...] = result[...].reshape(o_result.shape)
    o_back[...] = back[...].reshape(o_back.shape)
    o_in[...] = grad_in[...]
    o_out[...] = grad_out[...]
    for unit in (0, 1):
        for i in range(4):
            o_gains[unit : unit + 1, 128 * i : 128 * i + 128] = small[unit, i : i + 1, :]
        o_scales[unit] = small[unit, 4:6, :]


def on_device(frames, cotangent, weight_in, qk_scales, weight_out, gains):
    tokens_all = frames.shape[0] * frames.shape[1] * lax.axis_size(DP) * lax.axis_size(SEQ)
    vmem = pl.BlockSpec(memory_space=pltpu.VMEM)
    hbm = pl.BlockSpec(memory_space=pl.ANY)
    scratch = [pltpu.VMEM(shape, dtype) for shape, dtype in SCRATCH.values()]
    for _, _, n, direct in GROUPS:
        scratch += sum_scratch(n, direct)
    scratch += [pltpu.VMEM((2, 17, 8, 128), F32)]
    dma = pltpu.SemaphoreType.DMA
    scratch += [dma((6,)), dma((SEMS,)), dma((SEMS,))]
    parts = pl.pallas_call(
        functools.partial(step_kernel, tokens_all ** (-0.5)),
        out_shape=(
            jax.ShapeDtypeStruct((2, 8, 2, 16, D), BF16),
            jax.ShapeDtypeStruct((2, BLOCK, D), BF16),
            jax.ShapeDtypeStruct((2, 16, WIDE), F32),
            jax.ShapeDtypeStruct((2, 32, D), F32),
            jax.ShapeDtypeStruct((2, 8, 128), F32),
        ),
        in_specs=[hbm, hbm, hbm, hbm, vmem, vmem],
        out_specs=(hbm, hbm, vmem, vmem, vmem),
        scratch_shapes=scratch,
        compiler_params=pltpu.CompilerParams(
            collective_id=0, has_side_effects=True, vmem_limit_bytes=67_043_328
        ),
    )(
        frames.reshape(2, BLOCK, D),
        cotangent.reshape(2, 8, 2, 16, D),
        weight_in,
        weight_out,
        qk_scales,
        gains,
    )
    return pl.pallas_call(
        write_kernel,
        out_shape=(
            jax.ShapeDtypeStruct(frames.shape, BF16),
            jax.ShapeDtypeStruct(frames.shape, BF16),
            jax.ShapeDtypeStruct((2, 16, WIDE), F32),
            jax.ShapeDtypeStruct((2, 32, D), F32),
            jax.ShapeDtypeStruct((2, D), F32),
            jax.ShapeDtypeStruct((2, 2, S), F32),
        ),
        in_specs=[vmem] * 5,
        out_specs=(vmem,) * 6,
    )(*parts)


def solution(mesh):
    split = Mesh(mesh.devices.reshape(4, 4, 2, 4, 2), DP + SEQ)
    placed = (P(DP, SEQ, None), P(DP, SEQ, None), P(), P(), P(), P())
    return jax.shard_map(
        on_device,
        mesh=split,
        in_specs=placed,
        out_specs=(
            P(DP, SEQ, None),
            P(DP, SEQ, None),
            P(None, DP, None),
            P(None, DP, None),
            P(),
            P(),
        ),
        check_vma=False,
    )
```

```python
import functools

import jax
import jax.numpy as jnp
from jax import lax
from jax.experimental import pallas as pl
from jax.experimental.pallas import tpu as pltpu
from jax.sharding import Mesh
from jax.sharding import PartitionSpec as P

DP = ("dp_0", "dp_1", "dp_2")
SEQ = ("seq_0", "seq_1")
D, E, S, BLOCK = 512, 1024, 128, 256
WIDE = 2 * E + S
EPSILON = 1e-06
F32, BF16 = jnp.float32, jnp.bfloat16
NT = 25
SEMS = 60


MESH = pl.DeviceIdType.MESH


def halves_of(n):
    return ((0, (n + 1) // 2), ((n + 1) // 2, n // 2))


def pieces_of(n):
    return n // 8, n - 7 * (n // 8)


class Links:
    def __init__(self, send, recv):
        self.send, self.recv, self.used, self.waits = send, recv, 0, []
        self.x, self.y, self.zl = (lax.axis_index(a) for a in DP)
        self.zh, self.c = (lax.axis_index(a) for a in SEQ)

    def take(self, count=1):
        at = self.used
        self.used += count
        return at

    def at(self, x=None, y=None, zl=None, zh=None, c=None):
        return (
            self.x if x is None else x,
            self.y if y is None else y,
            self.zl if zl is None else zl,
            self.zh if zh is None else zh,
            self.c if c is None else c,
        )

    def copy(self, src, dst, target, sem):
        return pltpu.make_async_remote_copy(
            src_ref=src,
            dst_ref=dst,
            send_sem=self.send.at[sem],
            recv_sem=self.recv.at[sem],
            device_id=target,
            device_id_type=MESH,
        )

    def whole(self, region, sem):
        return self.copy(region, region, self.at(c=1 - self.c), sem)

    def arrived(self, region, sem):
        self.whole(region, sem).wait_recv()

    def later(self, region, sem, when=None):
        def wait():
            if when is None:
                self.whole(region, sem).wait_send()
            else:

                @pl.when(when)
                def _():
                    self.whole(region, sem).wait_send()

        self.waits.append(wait)

    def drain(self):
        for wait in self.waits:
            wait()


def mod4(v):
    return lax.rem(v + 8, 4)


def greet(k):
    sem = pltpu.get_barrier_semaphore()
    targets = [k.at(x=mod4(k.x + d)) for d in (1, 2, 3)]
    targets += [k.at(y=mod4(k.y + d)) for d in (1, 2, 3)]
    for dl in (0, 1):
        for dh in range(4):
            for dc in (0, 1):
                if dl or dh or dc:
                    targets.append(
                        k.at(zl=lax.rem(k.zl + dl, 2), zh=mod4(k.zh + dh), c=lax.rem(k.c + dc, 2))
                    )
    for target in targets:
        pl.semaphore_signal(sem, inc=1, device_id=target, device_id_type=MESH)
    return lambda: pl.semaphore_wait(sem, len(targets))


def tree_sum(parts):
    while len(parts) > 1:
        parts = [a + b for a, b in zip(parts[::2], parts[1::2])]
    return parts[0]


def small_sum(k, buf, value_ref, out_ref):
    sems = {}
    axes = (
        ("z", 8, 1, 2 * k.zh + k.zl, lambda i: k.at(zh=i // 2, zl=lax.rem(i, 2))),
        ("x", 4, 9, k.x, lambda i: k.at(x=i)),
        ("y", 4, 13, k.y, lambda i: k.at(y=i)),
    )

    def share(axis, value):
        name, size, first, me, target = axis
        buf[first + me] = value
        sem = sems[name] = k.take()
        box = buf.at[first + me]
        for d in range(1, size):
            k.copy(box, box, target(lax.rem(me + d, size)), sem).start()
        k.later(buf.at[first : first + size - 1], sem)

    def collected(axis):
        name, size, first, _, _ = axis
        k.arrived(buf.at[first : first + size - 1], sems[name])
        return tree_sum([buf[first + i] for i in range(size)])

    def pair():
        sems["p"] = k.take()
        k.copy(value_ref, buf.at[0], k.at(c=1 - k.c), sems["p"]).start()
        k.later(buf.at[0], sems["p"])

    def z():
        k.arrived(buf.at[0], sems["p"])
        share(axes[0], value_ref[...] + buf[0])

    def x():
        share(axes[1], collected(axes[0]))

    def y():
        share(axes[2], collected(axes[1]))

    def end():
        out_ref[...] = collected(axes[2])

    return [pair, z, x, y, end]


def sum_stages(k, grads, cuts, direct, paired, first_in, second_in, z_in, gathered):
    sems = {}
    me = (k.x, k.y)
    t_base, n_tiles = cuts[0], cuts[-1] - cuts[0]
    halves = halves_of(n_tiles)
    f32 = jnp.float32

    def to_axis(half, step, delta):
        along = (half + step) % 2
        return k.at(x=mod4(k.x + delta)) if along == 0 else k.at(y=mod4(k.y + delta))

    def view(half, step, delta, part=None):
        t0, n = halves[half]
        along = (half + step) % 2
        dest = mod4(me[along] + delta)
        if step == 0:
            sub = pl.ds(0, 4) if part is None else pl.ds(2 * part, 2)
            at = (dest, sub) if along == 0 else (sub, dest)
        else:
            at = (dest, k.y) if along == 0 else (k.x, dest)
        return paired.at[at[0], at[1], t0 : t0 + n]

    def pair_copy(i):
        lo, hi = cuts[i], cuts[i + 1]
        return k.copy(
            grads.at[:, :, 1 - k.c, lo:hi],
            paired.at[:, :, lo - t_base : hi - t_base],
            k.at(c=1 - k.c),
            sems["pair", i],
        )

    def pair_out(i):
        sems["pair", i] = k.take()
        op = pair_copy(i)
        op.start()
        k.waits.append(op.wait_send)

    def pair_in():
        for i in range(len(cuts) - 1):
            pair_copy(i).wait_recv()

        @pl.loop(0, 4)
        def _(i):
            paired[i] = paired[i] + grads[i, :, k.c, t_base : t_base + n_tiles]

        for half in (0, 1):
            spread(half, 0) if direct else outset(half)

    def spread(half, step):
        box = (first_in if step == 0 else second_in)[half]
        sem = sems[half, step] = k.take()
        for d in (2, 1, 3):
            k.copy(view(half, step, d), box.at[d - 1], to_axis(half, step, d), sem).start()
        k.later(box, sem)

    def collect_spread(half, step):
        box = (first_in if step == 0 else second_in)[half]
        k.arrived(box, sems[half, step])
        own = view(half, step, 0)
        near = box[0].astype(f32) + box[2].astype(f32)
        own[...] = ((own[...].astype(f32) + box[1].astype(f32)) + near).astype(jnp.bfloat16)

    def outset(half):
        one, two = first_in[half][:2], first_in[half][2:]
        base = sems[half, 0] = k.take(4)
        for direction, delta in ((0, 1), (1, -1)):
            k.copy(
                view(half, 0, 2, direction), one[direction], to_axis(half, 0, delta), base + direction
            ).start()
            k.later(one[direction], base + direction)
        for direction, delta in ((0, 1), (1, -1)):
            part = 1 - direction
            k.copy(
                view(half, 0, delta, part),
                two[direction].at[2 * part : 2 * part + 2],
                to_axis(half, 0, delta),
                base + 2 + direction,
            ).start()

    def relay():
        for half in (0, 1):
            one, two = first_in[half][:2], first_in[half][2:]
            base = sems[half, 0]
            for direction, delta in ((0, 1), (1, -1)):
                k.arrived(one[direction], base + direction)
                target = view(half, 0, delta, direction)
                target[...] = target[...] + one[direction][...]
                k.copy(
                    target,
                    two[direction].at[2 * direction : 2 * direction + 2],
                    to_axis(half, 0, delta),
                    base + 2 + direction,
                ).start()
                k.later(two[direction], base + 2 + direction)

    def collect(half):
        two = first_in[half][2:]
        for direction in (0, 1):
            k.arrived(two[direction], sems[half, 0] + 2 + direction)
        own = view(half, 0, 0)
        own[...] = (
            own[...].astype(f32) + (two[0][...].astype(f32) + two[1][...].astype(f32))
        ).astype(jnp.bfloat16)

    def turn():
        for half in (0, 1):
            collect_spread(half, 0) if direct else collect(half)
            spread(half, 1)

    spot = 2 * k.zh + k.zl
    holds = k.zl == k.c
    piece_step, piece_size = pieces_of(n_tiles)

    def z_out():
        for half in (0, 1):
            collect_spread(half, 1)
        sem = sems["z"] = k.take()
        for q in range(4):
            for e in range(2):
                piece = piece_step * (2 * q + e)
                source = paired.at[k.x, k.y, piece : piece + piece_size]
                mine = (k.zh == q) & (k.c == e) & holds
                op = k.copy(source, z_in.at[spot], k.at(zl=k.c, zh=q, c=e), sem)

                @pl.when(jnp.logical_not(mine))
                def _():
                    op.start()

                @pl.when(mine)
                def _():
                    z_in[spot] = source[...]

        k.later(z_in.at[0:7], sem, holds)
        k.later(z_in, sem, jnp.logical_not(holds))

    def z_sum():
        @pl.when(holds)
        def _():
            k.arrived(z_in.at[0:7], sems["z"])

        @pl.when(jnp.logical_not(holds))
        def _():
            k.arrived(z_in, sems["z"])

        p = 2 * k.zh + k.c
        gathered[p] = tree_sum([z_in[i].astype(f32) for i in range(8)]).astype(jnp.bfloat16)
        sem = sems["g"] = k.take()
        box = gathered.at[p]
        for d in range(1, 8):
            to = lax.rem(p + d, 8)
            k.copy(box, box, k.at(zh=to // 2, c=lax.rem(to, 2)), sem).start()
        k.later(gathered.at[0:7], sem)

    def gather():
        k.arrived(gathered.at[0:7], sems["g"])

    def whole_out():
        for half in (0, 1):
            collect_spread(half, 1)
        sem = sems["z"] = k.take()
        for q in range(4):
            op = k.copy(paired.at[k.x, k.y], z_in.at[spot], k.at(zl=k.c, zh=q), sem)

            @pl.when(jnp.logical_not(holds & (k.zh == q)))
            def _():
                op.start()

        @pl.when(holds)
        def _():
            z_in[spot] = paired[k.x, k.y]

        k.later(z_in.at[0:3], sem, holds)
        k.later(z_in.at[0:4], sem, jnp.logical_not(holds))

    def whole_sum():
        sems["g"] = k.take()

        @pl.when(holds)
        def _():
            k.arrived(z_in.at[0:7], sems["z"])
            gathered[0] = tree_sum([z_in[i].astype(f32) for i in range(8)]).astype(jnp.bfloat16)
            k.whole(gathered, sems["g"]).start()

        k.later(gathered, sems["g"], holds)

    def whole_in():
        @pl.when(jnp.logical_not(holds))
        def _():
            k.arrived(gathered, sems["g"])

    pairs = [functools.partial(pair_out, i) for i in range(len(cuts) - 1)]
    if direct:
        return pairs + [pair_in, turn, whole_out, whole_sum, whole_in]
    return pairs + [pair_in, relay, turn, z_out, z_sum, gather]


def write_shard(cuts, direct, gathered, grad_in_ref, grad_out_ref, scaling):
    t_base, n_tiles = cuts[0], cuts[-1] - cuts[0]
    piece_step = n_tiles if direct else pieces_of(n_tiles)[0]
    for at in range(n_tiles):
        p = min(at // piece_step, 7)
        values = gathered[p, at - piece_step * p].astype(jnp.float32) * scaling
        tile = t_base + at
        if tile < 8:
            column, half = tile // 2, tile % 2
            grad_out_ref[16 * half : 16 * half + 16, 128 * column : 128 * column + 128] = values
        else:
            grad_in_ref[:, 128 * (tile - 8) : 128 * (tile - 7)] = values


def sum_scratch(cuts, direct):
    n_tiles = cuts[-1] - cuts[0]

    def tiles(*lead):
        return pltpu.VMEM((*lead, 16, 128), jnp.bfloat16)

    shapes = [tiles(4, 4, n_tiles)]
    if direct:
        for lead in ((3, 4), (3,)):
            shapes += [tiles(*lead, n) for _, n in halves_of(n_tiles)]
        return shapes + [tiles(8, n_tiles), tiles(1, n_tiles)]
    for _, n in halves_of(n_tiles):
        shapes += [tiles(2, n)] * 2 + [tiles(4, n)] * 2
    shapes += [tiles(3, n) for _, n in halves_of(n_tiles)]
    return shapes + [tiles(8, pieces_of(n_tiles)[1])] * 2


def sum_refs(refs, direct):
    if direct:
        return refs[0], refs[1:3], refs[3:5], refs[5], refs[6]
    return refs[0], (refs[1:5], refs[5:9]), refs[9:11], refs[11], refs[12]


NN = (((1,), (0,)), ((), ()))
NT_DIMS = (((1,), (1,)), ((), ()))
TN = (((0,), (0,)), ((), ()))


def dot(a, b, dims=NN):
    return lax.dot_general(a, b, dims, preferred_element_type=F32)


def sigmoid(p):
    return 0.5 * jnp.tanh(0.5 * p) + 0.5


def cols(at, width=512):
    return slice(at, at + width)


def group_mask(unit):
    if unit == 0:
        return None
    row = lax.broadcasted_iota(jnp.int32, (BLOCK, BLOCK), 0)
    column = lax.broadcasted_iota(jnp.int32, (BLOCK, BLOCK), 1)
    return lax.rem(row, 16) == lax.rem(column, 16)


def positive_scores(unit, query, keyed):
    r = jnp.maximum(dot(query, keyed, NT_DIMS) * S ** (-0.5), 0.0)
    mask = group_mask(unit)
    return r if mask is None else jnp.where(mask, r, 0.0)


def length_of(unit):
    return BLOCK if unit == 0 else 16


def forward_group(m, unit, g, x):
    xf = x.astype(F32)
    scaling = lax.rsqrt(jnp.mean(xf * xf, axis=-1, keepdims=True) + EPSILON)
    hidden = (xf * scaling * m.gains[unit : unit + 1, :]).astype(BF16)
    m.hidden[unit, g] = hidden
    p = dot(hidden, m.w_in[unit, :, 2 * E :])
    m.proj[unit, g, :, 2 * E :] = p
    z = p * sigmoid(p)
    query = (z * m.scales[unit, 0:1, :]).astype(BF16)
    keyed = (z * m.scales[unit, 1:2, :]).astype(BF16)
    m.query[unit, g] = query
    m.keyed[unit, g] = keyed
    r = positive_scores(unit, query, keyed)
    weights = (r * r * (1.0 / length_of(unit))).astype(BF16)
    m.weights[unit, g] = weights
    for at in range(0, E, 512):
        p = dot(hidden, m.w_in[unit, :, cols(E + at)])
        m.proj[unit, g, :, cols(E + at)] = p
        m.value[unit, g, :, cols(at)] = (p * sigmoid(p)).astype(BF16)
        p = dot(hidden, m.w_in[unit, :, cols(at)])
        m.proj[unit, g, :, cols(at)] = p
        mixed = dot(weights, m.value[unit, g, :, cols(at)])
        m.mixed[unit, g, :, cols(at)] = mixed
        m.gated[unit, g, :, cols(at)] = (p * sigmoid(p) * mixed).astype(BF16)
    return (x.astype(F32) + dot(m.gated[unit, g], m.w_out[unit])).astype(BF16)


def backward_gate(m, unit, g, upstream):
    for at in range(0, E, 512):
        d_gated = dot(upstream, m.w_out[unit, cols(at), :], NT_DIMS).astype(BF16).astype(F32)
        p = m.proj[unit, g, :, cols(at)]
        sig = sigmoid(p)
        gate = p * sig
        m.d_mixed[g, :, cols(at)] = (d_gated * gate).astype(BF16)
        slope = sig + gate * (1.0 - sig)
        m.d_proj[g, :, cols(at)] = (d_gated * m.mixed[unit, g, :, cols(at)] * slope).astype(BF16)


def backward_attention(m, unit, g):
    d_weights = dot(m.d_mixed[g], m.value[unit, g], NT_DIMS).astype(BF16).astype(F32)
    query, keyed = m.query[unit, g], m.keyed[unit, g]
    r = positive_scores(unit, query, keyed)
    d_scores = (d_weights * r * (2.0 / length_of(unit) * S ** (-0.5))).astype(BF16)
    d_query = dot(d_scores, keyed).astype(BF16).astype(F32)
    d_keyed = dot(d_scores, query, TN).astype(BF16).astype(F32)
    p = m.proj[unit, g, :, 2 * E :]
    sig = sigmoid(p)
    z = p * sig
    d_z = d_query * m.scales[unit, 0:1, :] + d_keyed * m.scales[unit, 1:2, :]
    m.d_proj[g, :, 2 * E :] = (d_z * (sig + z * (1.0 - sig))).astype(BF16)
    m.small[unit, 4:5, :] += jnp.sum(d_query * z, axis=0, keepdims=True)
    m.small[unit, 5:6, :] += jnp.sum(d_keyed * z, axis=0, keepdims=True)
    weights = m.weights[unit, g]
    for at in range(0, E, 512):
        d_value = dot(weights, m.d_mixed[g, :, cols(at)], TN).astype(BF16).astype(F32)
        p = m.proj[unit, g, :, cols(E + at)]
        sig = sigmoid(p)
        m.d_proj[g, :, cols(E + at)] = (d_value * (sig + p * sig * (1.0 - sig))).astype(BF16)


def backward_input(m, unit, g, x, upstream):
    d_hidden = dot(m.d_proj[g], m.w_in[unit], NT_DIMS)
    xf = x.astype(F32)
    scaling = lax.rsqrt(jnp.mean(xf * xf, axis=-1, keepdims=True) + EPSILON)
    xs = xf * scaling
    d_gain = jnp.sum(d_hidden * xs, axis=0, keepdims=True)
    for i in range(4):
        m.small[unit, i : i + 1, :] += d_gain[:, 128 * i : 128 * i + 128]
    d_xs = d_hidden * m.gains[unit : unit + 1, :]
    d_x = scaling * (d_xs - xs * jnp.mean(d_xs * xs, axis=-1, keepdims=True))
    return (upstream.astype(F32) + d_x).astype(BF16)


def turned(m, unit):
    for g in (0, 1):
        m.hidden_t[unit, :, cols(BLOCK * g, BLOCK)] = m.hidden[unit, g].T
        m.gated_t[unit, :, cols(BLOCK * g, BLOCK)] = m.gated[unit, g].T


def weight_out_grad(m, unit, upstream):
    for i in range(4):
        rows = dot(m.gated_t[unit, cols(256 * i, 256), :], upstream).astype(BF16)
        parts = rows.reshape(4, 2, 2, 16, 512)
        for column in range(4):
            at = 2 * column
            m.grads[unit, i, :, :, at : at + 2] = parts[..., 128 * column : 128 * column + 128]


GATE = ((0, 512), (512, 512))
OTHERS = ((1024, 512), (1536, 512), (2048, 128))


def weight_in_grad(m, unit, columns):
    for at, width in columns:
        right = m.d_proj[:, :, cols(at, width)].reshape(2 * BLOCK, width)
        for i in (0, 1):
            part = dot(m.hidden_t[unit, cols(256 * i, 256), :], right).astype(BF16)
            part = part.reshape(2, 4, 2, 16, width)
            for j in range(width // 128):
                m.grads[unit, 2 * i : 2 * i + 2, :, :, 8 + at // 128 + j] = part[
                    ..., 128 * j : 128 * j + 128
                ]


class Memory:
    pass


SCRATCH = dict(
    w_in=((2, D, WIDE), BF16),
    w_out=((2, E, D), BF16),
    frames=((2, BLOCK, D), BF16),
    cot=((2, 8, 2, 16, D), BF16),
    first=((2, 8, 2, 16, D), BF16),
    first_pos=((2, 16, 16, D), BF16),
    cot_pos=((2, 16, 16, D), BF16),
    out_pos=((2, 16, 16, D), BF16),
    out=((2, 8, 2, 16, D), BF16),
    back_pos=((2, 16, 16, D), BF16),
    back=((2, 8, 2, 16, D), BF16),
    back_frames=((2, BLOCK, D), BF16),
    hidden=((2, 2, BLOCK, D), BF16),
    hidden_t=((2, D, 2 * BLOCK), BF16),
    proj=((2, 2, BLOCK, WIDE), F32),
    value=((2, 2, BLOCK, E), BF16),
    query=((2, 2, BLOCK, S), BF16),
    keyed=((2, 2, BLOCK, S), BF16),
    weights=((2, 2, BLOCK, BLOCK), BF16),
    mixed=((2, 2, BLOCK, E), F32),
    gated=((2, 2, BLOCK, E), BF16),
    gated_t=((2, E, 2 * BLOCK), BF16),
    d_mixed=((2, BLOCK, E), BF16),
    d_proj=((2, BLOCK, WIDE), BF16),
    grads=((2, 4, 4, 2, NT, 16, 128), BF16),
    small=((2, 8, 128), F32),
    scales=((2, 2, S), F32),
    gains=((2, D), F32),
)
GROUPS = (
    (1, (0, 8, 16), False),
    (1, (16, 25), False),
    (0, (0, 8, 16), False),
    (0, (16, 25), True),
)


def step_kernel(scaling, *refs):
    m = Memory()
    frames_hbm, cot_hbm, w_in_hbm, w_out_hbm, scales_hbm, gains_hbm = refs[:6]
    out_hbm, back_hbm, in_ref, wout_ref, small_ref = refs[6:11]
    refs = refs[11:]
    for name, ref in zip(SCRATCH, refs):
        setattr(m, name, ref)
    refs = refs[len(SCRATCH) :]
    sums = []
    for _, cuts, direct in GROUPS:
        count = len(sum_scratch(cuts, direct))
        sums.append(sum_refs(refs[:count], direct))
        refs = refs[count:]
    small_bufs = refs[0]
    local, send, recv = refs[1:4]
    k = Links(send, recv)
    p = 2 * k.zh + k.c

    def load(src, dst, sem):
        op = pltpu.make_async_copy(src, dst, local.at[sem])
        op.start()
        return op

    loads = dict(
        frames=load(frames_hbm, m.frames, 0),
        scales=load(scales_hbm, m.scales, 6),
        gains=load(gains_hbm, m.gains, 7),
        others_0=load(w_in_hbm.at[0, :, E:], m.w_in.at[0, :, E:], 1),
        gate_0=load(w_in_hbm.at[0, :, :E], m.w_in.at[0, :, :E], 8),
        out_0=load(w_out_hbm.at[0], m.w_out.at[0], 3),
    )
    met = greet(k)
    m.small[...] = jnp.zeros((2, 8, 128), F32)

    def peer(d):
        j = lax.rem(p + d, 8)
        return j, k.at(zh=j // 2, c=lax.rem(j, 2))

    def from_peer(d):
        j = lax.rem(p + 8 - d, 8)
        return j, k.at(zh=j // 2, c=lax.rem(j, 2))

    first_sems, cot_sems, out_sems, back_sems = (k.take(2) for _ in range(4))

    def first_copy(b, h, d, to):
        return k.copy(m.first.at[b, to[0], h], m.first_pos.at[h, 2 * p + b], to[1], first_sems + h)

    def cot_copy(h, d, to):
        box = m.cot_pos.at[h, pl.ds(2 * p, 2)]
        return k.copy(m.cot.at[:, to[0], h], box, to[1], cot_sems + h)

    def out_copy(h, d, to):
        box = m.out.at[:, p, h]
        return k.copy(m.out_pos.at[h, pl.ds(2 * to[0], 2)], box, to[1], out_sems + h)

    def back_copy(h, d, to):
        box = m.back.at[:, p, h]
        return k.copy(m.back_pos.at[h, pl.ds(2 * to[0], 2)], box, to[1], back_sems + h)

    def send(copy, h):
        for d in range(1, 8):
            copy(h, d, peer(d)).start()

    def receive(base, h):
        k.arrived(m.first_pos.at[0, 0:14], base + h)

    for name in ("frames", "scales", "gains", "others_0", "gate_0", "out_0"):
        loads[name].wait()
    loads = dict(
        cot=load(cot_hbm, m.cot, 2),
        in_1=load(w_in_hbm.at[1], m.w_in.at[1], 4),
        out_1=load(w_out_hbm.at[1], m.w_out.at[1], 5),
    )

    def exchange_first(b, h):
        for d in range(1, 8):
            first_copy(b, h, d, peer(d)).start()

    def block_forward(b):
        with jax.named_scope("f0"):
            m.first[b] = forward_group(m, 0, b, m.frames[b]).reshape(8, 2, 16, D)

    block_forward(0)
    with jax.named_scope("barrier"):
        met()
    for h in (0, 1):
        exchange_first(0, h)
    block_forward(1)
    for h in (0, 1):
        exchange_first(1, h)
        m.first_pos[h, pl.ds(2 * p, 2)] = m.first[:, p, h]
    loads["cot"].wait()
    for h in (0, 1):
        send(cot_copy, h)
        m.cot_pos[h, pl.ds(2 * p, 2)] = m.cot[:, p, h]
    with jax.named_scope("turn0"):
        turned(m, 0)
    loads["in_1"].wait()
    loads["out_1"].wait()

    @pl.loop(0, 2)
    def _(h):
        with jax.named_scope("w_first"):
            receive(first_sems, h)
        with jax.named_scope("f1"):
            x = m.first_pos[h].reshape(BLOCK, D)
            m.out_pos[h] = forward_group(m, 1, h, x).reshape(16, 16, D)

    m.out[:, p] = m.out_pos[:, pl.ds(2 * p, 2)].transpose(1, 0, 2, 3)
    with jax.named_scope("turn1"):
        turned(m, 1)

    groups = {}
    for name, (unit, cuts, direct), refs_of in zip(("a1", "b1", "a0", "b0"), GROUPS, sums):
        groups[name] = sum_stages(k, m.grads.at[unit], cuts, direct, *refs_of)
    groups["s"] = small_sum(k, small_bufs, m.small, small_ref)
    done = dict.fromkeys(groups, 0)

    def run(names):
        for name in names.split():
            with jax.named_scope(f"{name}_{done[name]}"):
                groups[name][done[name]]()
            done[name] += 1

    def unit_1_gate(h, wait=True):
        if wait:
            with jax.named_scope("w_cot"):
                receive(cot_sems, h)
        with jax.named_scope("gate1"):
            backward_gate(m, 1, h, m.cot_pos[h].reshape(BLOCK, D))

    def unit_1_rest(h):
        with jax.named_scope("rest1"):
            backward_attention(m, 1, h)
            x = m.first_pos[h].reshape(BLOCK, D)
            upstream = m.cot_pos[h].reshape(BLOCK, D)
            m.back_pos[h] = backward_input(m, 1, h, x, upstream).reshape(16, 16, D)
        send(back_copy, h)
        m.back[:, p, h] = m.back_pos[h, pl.ds(2 * p, 2)]

    def input_0(g):
        with jax.named_scope("input0"):
            m.back_frames[g] = backward_input(m, 0, g, m.frames[g], m.back[g].reshape(BLOCK, D))

    def write(at):
        unit, cuts, direct = GROUPS[at]
        write_shard(cuts, direct, sums[at][-1], in_ref.at[unit], wout_ref.at[unit], scaling)

    unit_1_gate(0)
    unit_1_rest(0)
    with jax.named_scope("w_cot"):
        receive(cot_sems, 1)
    with jax.named_scope("wgo1"):
        weight_out_grad(m, 1, m.cot_pos[...].reshape(2 * BLOCK, D))
    run("a1")
    unit_1_gate(1, False)
    with jax.named_scope("wgi1"):
        weight_in_grad(m, 1, GATE)
    run("a1")
    unit_1_rest(1)
    run("a1")
    with jax.named_scope("wg1b"):
        weight_in_grad(m, 1, OTHERS)
    run("b1 b1 a1")
    with jax.named_scope("w_back"):
        receive(back_sems, 0)
        receive(back_sems, 1)
    for h in (0, 1):
        send(out_copy, h)
    with jax.named_scope("wgo0"):
        weight_out_grad(m, 0, m.back[...].reshape(2 * BLOCK, D))
    run("a0")
    with jax.named_scope("gate0"):
        for g in (0, 1):
            backward_gate(m, 0, g, m.back[g].reshape(BLOCK, D))
    run("b1")
    with jax.named_scope("wgi0"):
        weight_in_grad(m, 0, GATE)
    run("a0 a1")
    with jax.named_scope("attn0"):
        for g in (0, 1):
            backward_attention(m, 0, g)
    run("b1 a0")
    with jax.named_scope("wg0b"):
        weight_in_grad(m, 0, OTHERS)
    run("b0")
    input_0(0)
    run("a1")
    input_0(1)
    store_back = load(m.back_frames, back_hbm, 0)
    run("s b0 a0 s b1 b0 a0 s a1 b1 b0 a0 s")
    with jax.named_scope("w_out"):
        receive(out_sems, 0)
        receive(out_sems, 1)
    store_out = load(m.out, out_hbm, 2)
    run("a0 s a1 b1")
    write(0)
    write(1)
    small_ref[...] = small_ref[...] * scaling
    run("b0 a0")
    write(2)
    run("b0")
    write(3)
    with jax.named_scope("drain"):
        k.drain()

        for base in (first_sems, cot_sems, out_sems, back_sems):
            for h in (0, 1):
                k.whole(m.first_pos.at[0, 0:14], base + h).wait_send()

        store_back.wait()
        store_out.wait()
    assert all(done[name] == len(stages) for name, stages in groups.items())
    assert k.used <= SEMS


def write_kernel(result, back, grad_in, grad_out, small, o_result, o_back, o_in, o_out, o_gains, o_scales):
    o_result[...] = result[...].reshape(o_result.shape)
    o_back[...] = back[...].reshape(o_back.shape)
    o_in[...] = grad_in[...]
    o_out[...] = grad_out[...]
    for unit in (0, 1):
        for i in range(4):
            o_gains[unit : unit + 1, 128 * i : 128 * i + 128] = small[unit, i : i + 1, :]
        o_scales[unit] = small[unit, 4:6, :]


def on_device(frames, cotangent, weight_in, qk_scales, weight_out, gains):
    tokens_all = frames.shape[0] * frames.shape[1] * lax.axis_size(DP) * lax.axis_size(SEQ)
    vmem = pl.BlockSpec(memory_space=pltpu.VMEM)
    hbm = pl.BlockSpec(memory_space=pl.ANY)
    scratch = [pltpu.VMEM(shape, dtype) for shape, dtype in SCRATCH.values()]
    for _, cuts, direct in GROUPS:
        scratch += sum_scratch(cuts, direct)
    scratch += [pltpu.VMEM((17, 2, 8, 128), F32)]
    dma = pltpu.SemaphoreType.DMA
    scratch += [dma((9,)), dma((SEMS,)), dma((SEMS,))]
    parts = pl.pallas_call(
        functools.partial(step_kernel, tokens_all ** (-0.5)),
        out_shape=(
            jax.ShapeDtypeStruct((2, 8, 2, 16, D), BF16),
            jax.ShapeDtypeStruct((2, BLOCK, D), BF16),
            jax.ShapeDtypeStruct((2, 16, WIDE), F32),
            jax.ShapeDtypeStruct((2, 32, D), F32),
            jax.ShapeDtypeStruct((2, 8, 128), F32),
        ),
        in_specs=[hbm] * 6,
        out_specs=(hbm, hbm, vmem, vmem, vmem),
        scratch_shapes=scratch,
        compiler_params=pltpu.CompilerParams(
            collective_id=0, has_side_effects=True, vmem_limit_bytes=67_043_328
        ),
    )(
        frames.reshape(2, BLOCK, D),
        cotangent.reshape(2, 8, 2, 16, D),
        weight_in,
        weight_out,
        qk_scales,
        gains,
    )
    return pl.pallas_call(
        write_kernel,
        out_shape=(
            jax.ShapeDtypeStruct(frames.shape, BF16),
            jax.ShapeDtypeStruct(frames.shape, BF16),
            jax.ShapeDtypeStruct((2, 16, WIDE), F32),
            jax.ShapeDtypeStruct((2, 32, D), F32),
            jax.ShapeDtypeStruct((2, D), F32),
            jax.ShapeDtypeStruct((2, 2, S), F32),
        ),
        in_specs=[vmem] * 5,
        out_specs=(vmem,) * 6,
    )(*parts)


def solution(mesh):
    split = Mesh(mesh.devices.reshape(4, 4, 2, 4, 2), DP + SEQ)
    placed = (P(DP, SEQ, None), P(DP, SEQ, None), P(), P(), P(), P())
    return jax.shard_map(
        on_device,
        mesh=split,
        in_specs=placed,
        out_specs=(
            P(DP, SEQ, None),
            P(DP, SEQ, None),
            P(None, DP, None),
            P(None, DP, None),
            P(),
            P(),
        ),
        check_vma=False,
    )
```

```python
import functools

import jax
import jax.numpy as jnp
from jax import lax
from jax.experimental import pallas as pl
from jax.experimental.pallas import tpu as pltpu
from jax.sharding import Mesh
from jax.sharding import PartitionSpec as P

DP = ("dp_0", "dp_1", "dp_2")
SEQ = ("seq_0", "seq_1")
D, E, S, BLOCK = 512, 1024, 128, 256
WIDE = 2 * E + S
EPSILON = 1e-06
F32, BF16 = jnp.float32, jnp.bfloat16
NT = 25
SEMS = 58


MESH = pl.DeviceIdType.MESH


def halves_of(n):
    return ((0, (n + 1) // 2), ((n + 1) // 2, n // 2))


def pieces_of(n):
    return n // 8, n - 7 * (n // 8)


class Links:
    def __init__(self, send, recv):
        self.send, self.recv, self.used, self.waits = send, recv, 0, []
        self.x, self.y, self.zl = (lax.axis_index(a) for a in DP)
        self.zh, self.c = (lax.axis_index(a) for a in SEQ)

    def take(self, count=1):
        at = self.used
        self.used += count
        return at

    def at(self, x=None, y=None, zl=None, zh=None, c=None):
        return (
            self.x if x is None else x,
            self.y if y is None else y,
            self.zl if zl is None else zl,
            self.zh if zh is None else zh,
            self.c if c is None else c,
        )

    def copy(self, src, dst, target, sem):
        return pltpu.make_async_remote_copy(
            src_ref=src,
            dst_ref=dst,
            send_sem=self.send.at[sem],
            recv_sem=self.recv.at[sem],
            device_id=target,
            device_id_type=MESH,
        )

    def whole(self, region, sem):
        return self.copy(region, region, self.at(c=1 - self.c), sem)

    def arrived(self, region, sem):
        self.whole(region, sem).wait_recv()

    def later(self, region, sem, when=None):
        def wait():
            if when is None:
                self.whole(region, sem).wait_send()
            else:

                @pl.when(when)
                def _():
                    self.whole(region, sem).wait_send()

        self.waits.append(wait)

    def drain(self):
        for wait in self.waits:
            wait()


def mod4(v):
    return lax.rem(v + 8, 4)


def greet(k):
    sem = pltpu.get_barrier_semaphore()
    targets = [k.at(x=mod4(k.x + d)) for d in (1, 2, 3)]
    targets += [k.at(y=mod4(k.y + d)) for d in (1, 2, 3)]
    for dl in (0, 1):
        for dh in range(4):
            for dc in (0, 1):
                if dl or dh or dc:
                    targets.append(
                        k.at(zl=lax.rem(k.zl + dl, 2), zh=mod4(k.zh + dh), c=lax.rem(k.c + dc, 2))
                    )
    for target in targets:
        pl.semaphore_signal(sem, inc=1, device_id=target, device_id_type=MESH)
    return lambda: pl.semaphore_wait(sem, len(targets))


def tree_sum(parts):
    while len(parts) > 1:
        parts = [a + b for a, b in zip(parts[::2], parts[1::2])]
    return parts[0]


def small_sum(k, buf, value_ref, out_ref):
    sems = {}
    axes = (
        ("z", 8, 1, 2 * k.zh + k.zl, lambda i: k.at(zh=i // 2, zl=lax.rem(i, 2))),
        ("x", 4, 9, k.x, lambda i: k.at(x=i)),
        ("y", 4, 13, k.y, lambda i: k.at(y=i)),
    )

    def share(axis, value):
        name, size, first, me, target = axis
        buf[first + me] = value
        sem = sems[name] = k.take()
        box = buf.at[first + me]
        for d in range(1, size):
            k.copy(box, box, target(lax.rem(me + d, size)), sem).start()
        k.later(buf.at[first : first + size - 1], sem)

    def collected(axis):
        name, size, first, _, _ = axis
        k.arrived(buf.at[first : first + size - 1], sems[name])
        return tree_sum([buf[first + i] for i in range(size)])

    def pair():
        sems["p"] = k.take()
        k.copy(value_ref, buf.at[0], k.at(c=1 - k.c), sems["p"]).start()
        k.later(buf.at[0], sems["p"])

    def z():
        k.arrived(buf.at[0], sems["p"])
        share(axes[0], value_ref[...] + buf[0])

    def x():
        share(axes[1], collected(axes[0]))

    def y():
        share(axes[2], collected(axes[1]))

    def end():
        out_ref[...] = collected(axes[2])

    return [pair, z, x, y, end]


def sum_stages(k, grads, cuts, direct, paired, first_in, second_in, z_in, gathered):
    sems = {}
    me = (k.x, k.y)
    t_base, n_tiles = cuts[0], cuts[-1] - cuts[0]
    halves = halves_of(n_tiles)
    f32 = jnp.float32

    def to_axis(half, step, delta):
        along = (half + step) % 2
        return k.at(x=mod4(k.x + delta)) if along == 0 else k.at(y=mod4(k.y + delta))

    def view(half, step, delta, part=None):
        t0, n = halves[half]
        along = (half + step) % 2
        dest = mod4(me[along] + delta)
        if step == 0:
            sub = pl.ds(0, 4) if part is None else pl.ds(2 * part, 2)
            at = (dest, sub) if along == 0 else (sub, dest)
        else:
            at = (dest, k.y) if along == 0 else (k.x, dest)
        return paired.at[at[0], at[1], t0 : t0 + n]

    def pair_copy(i):
        lo, hi = cuts[i], cuts[i + 1]
        return k.copy(
            grads.at[:, :, 1 - k.c, lo:hi],
            paired.at[:, :, lo - t_base : hi - t_base],
            k.at(c=1 - k.c),
            sems["pair", i],
        )

    def pair_out(i):
        sems["pair", i] = k.take()
        op = pair_copy(i)
        op.start()
        k.waits.append(op.wait_send)

    def pair_in():
        for i in range(len(cuts) - 1):
            pair_copy(i).wait_recv()

        @pl.loop(0, 4)
        def _(i):
            paired[i] = paired[i] + grads[i, :, k.c, t_base : t_base + n_tiles]

        for half in (0, 1):
            outset(half)

    def spread(half):
        box = second_in[half]
        sem = sems[half, 1] = k.take()
        for d in (2, 1, 3):
            k.copy(view(half, 1, d), box.at[d - 1], to_axis(half, 1, d), sem).start()
        k.later(box, sem)

    def collect_spread(half):
        box = second_in[half]
        k.arrived(box, sems[half, 1])
        own = view(half, 1, 0)
        near = box[0].astype(f32) + box[2].astype(f32)
        own[...] = ((own[...].astype(f32) + box[1].astype(f32)) + near).astype(jnp.bfloat16)

    ways = ((0, 1), (1, -1))

    def outset(half):
        one, two = first_in[half]
        base = sems[half, 0] = k.take(2)
        for way, delta in ways:
            target = to_axis(half, 0, delta)
            k.copy(view(half, 0, 2, way), one.at[way], target, base).start()
        for way, delta in ways:
            part = 1 - way
            box = two.at[way, 2 * part : 2 * part + 2]
            k.copy(view(half, 0, delta, part), box, to_axis(half, 0, delta), base + 1).start()
        k.later(one, base)

    def relay():
        for half in (0, 1):
            one, two = first_in[half]
            base = sems[half, 0]
            k.arrived(one, base)
            for way, delta in ways:
                target = view(half, 0, delta, way)
                target[...] = target[...] + one[way]
                box = two.at[way, 2 * way : 2 * way + 2]
                k.copy(target, box, to_axis(half, 0, delta), base + 1).start()
            k.later(two, base + 1)

    def collect(half):
        two = first_in[half][1]
        k.arrived(two, sems[half, 0] + 1)
        own = view(half, 0, 0)
        own[...] = (own[...].astype(f32) + (two[0].astype(f32) + two[1].astype(f32))).astype(
            jnp.bfloat16
        )

    def turn():
        for half in (0, 1):
            collect(half)
            spread(half)

    spot = 2 * k.zh + k.zl
    holds = k.zl == k.c
    piece_step, piece_size = pieces_of(n_tiles)

    def z_out():
        for half in (0, 1):
            collect_spread(half)
        sem = sems["z"] = k.take()
        for q in range(4):
            for e in range(2):
                piece = piece_step * (2 * q + e)
                source = paired.at[k.x, k.y, piece : piece + piece_size]
                mine = (k.zh == q) & (k.c == e) & holds
                op = k.copy(source, z_in.at[spot], k.at(zl=k.c, zh=q, c=e), sem)

                @pl.when(jnp.logical_not(mine))
                def _():
                    op.start()

                @pl.when(mine)
                def _():
                    z_in[spot] = source[...]

        k.later(z_in.at[0:7], sem, holds)
        k.later(z_in, sem, jnp.logical_not(holds))

    def z_sum():
        @pl.when(holds)
        def _():
            k.arrived(z_in.at[0:7], sems["z"])

        @pl.when(jnp.logical_not(holds))
        def _():
            k.arrived(z_in, sems["z"])

        p = 2 * k.zh + k.c
        gathered[p] = tree_sum([z_in[i].astype(f32) for i in range(8)]).astype(jnp.bfloat16)
        sem = sems["g"] = k.take()
        box = gathered.at[p]
        for d in range(1, 8):
            to = lax.rem(p + d, 8)
            k.copy(box, box, k.at(zh=to // 2, c=lax.rem(to, 2)), sem).start()
        k.later(gathered.at[0:7], sem)

    def gather():
        k.arrived(gathered.at[0:7], sems["g"])

    def whole_out():
        for half in (0, 1):
            collect_spread(half)
        sem = sems["z"] = k.take()
        for q in range(4):
            op = k.copy(paired.at[k.x, k.y], z_in.at[spot], k.at(zl=k.c, zh=q), sem)

            @pl.when(jnp.logical_not(holds & (k.zh == q)))
            def _():
                op.start()

        @pl.when(holds)
        def _():
            z_in[spot] = paired[k.x, k.y]

        k.later(z_in.at[0:3], sem, holds)
        k.later(z_in.at[0:4], sem, jnp.logical_not(holds))

    def whole_sum():
        sems["g"] = k.take()

        @pl.when(holds)
        def _():
            k.arrived(z_in.at[0:7], sems["z"])
            gathered[0] = tree_sum([z_in[i].astype(f32) for i in range(8)]).astype(jnp.bfloat16)
            k.whole(gathered, sems["g"]).start()

        k.later(gathered, sems["g"], holds)

    def whole_in():
        @pl.when(jnp.logical_not(holds))
        def _():
            k.arrived(gathered, sems["g"])

    pairs = [functools.partial(pair_out, i) for i in range(len(cuts) - 1)]
    if direct:
        return pairs + [pair_in, relay, turn, whole_out, whole_sum, whole_in]
    return pairs + [pair_in, relay, turn, z_out, z_sum, gather]


def write_shard(cuts, direct, gathered, grad_in_ref, grad_out_ref, scaling):
    t_base, n_tiles = cuts[0], cuts[-1] - cuts[0]
    piece_step = n_tiles if direct else pieces_of(n_tiles)[0]
    for at in range(n_tiles):
        p = min(at // piece_step, 7)
        values = gathered[p, at - piece_step * p].astype(jnp.float32) * scaling
        tile = t_base + at
        if tile < 8:
            column, half = tile // 2, tile % 2
            grad_out_ref[16 * half : 16 * half + 16, 128 * column : 128 * column + 128] = values
        else:
            grad_in_ref[:, 128 * (tile - 8) : 128 * (tile - 7)] = values


def sum_scratch(cuts, direct):
    n_tiles = cuts[-1] - cuts[0]

    def tiles(*lead):
        return pltpu.VMEM((*lead, 16, 128), jnp.bfloat16)

    shapes = [tiles(4, 4, n_tiles)]
    for _, n in halves_of(n_tiles):
        shapes += [tiles(2, 2, n), tiles(2, 4, n)]
    shapes += [tiles(3, n) for _, n in halves_of(n_tiles)]
    if direct:
        return shapes + [tiles(8, n_tiles), tiles(1, n_tiles)]
    return shapes + [tiles(8, pieces_of(n_tiles)[1])] * 2


def sum_refs(refs):
    return refs[0], (refs[1:3], refs[3:5]), refs[5:7], refs[7], refs[8]


NN = (((1,), (0,)), ((), ()))
NT_DIMS = (((1,), (1,)), ((), ()))
TN = (((0,), (0,)), ((), ()))


def dot(a, b, dims=NN):
    return lax.dot_general(a, b, dims, preferred_element_type=F32)


def sigmoid(p):
    return 0.5 * jnp.tanh(0.5 * p) + 0.5


def cols(at, width=512):
    return slice(at, at + width)


def group_mask(unit):
    if unit == 0:
        return None
    row = lax.broadcasted_iota(jnp.int32, (BLOCK, BLOCK), 0)
    column = lax.broadcasted_iota(jnp.int32, (BLOCK, BLOCK), 1)
    return lax.rem(row, 16) == lax.rem(column, 16)


def positive_scores(unit, query, keyed):
    r = jnp.maximum(dot(query, keyed, NT_DIMS) * S ** (-0.5), 0.0)
    mask = group_mask(unit)
    return r if mask is None else jnp.where(mask, r, 0.0)


def length_of(unit):
    return BLOCK if unit == 0 else 16


def forward_group(m, unit, g, x):
    xf = x.astype(F32)
    scaling = lax.rsqrt(jnp.mean(xf * xf, axis=-1, keepdims=True) + EPSILON)
    hidden = (xf * scaling * m.gains[unit : unit + 1, :]).astype(BF16)
    m.hidden[unit, g] = hidden
    p = dot(hidden, m.w_in[unit, :, 2 * E :])
    m.proj[unit, g, :, 2 * E :] = p
    z = p * sigmoid(p)
    query = (z * m.scales[unit, 0:1, :]).astype(BF16)
    keyed = (z * m.scales[unit, 1:2, :]).astype(BF16)
    m.query[unit, g] = query
    m.keyed[unit, g] = keyed
    r = positive_scores(unit, query, keyed)
    weights = (r * r * (1.0 / length_of(unit))).astype(BF16)
    m.weights[unit, g] = weights
    for at in range(0, E, 512):
        p = dot(hidden, m.w_in[unit, :, cols(E + at)])
        m.proj[unit, g, :, cols(E + at)] = p
        m.value[unit, g, :, cols(at)] = (p * sigmoid(p)).astype(BF16)
        p = dot(hidden, m.w_in[unit, :, cols(at)])
        m.proj[unit, g, :, cols(at)] = p
        mixed = dot(weights, m.value[unit, g, :, cols(at)])
        m.mixed[unit, g, :, cols(at)] = mixed
        m.gated[unit, g, :, cols(at)] = (p * sigmoid(p) * mixed).astype(BF16)
    return (x.astype(F32) + dot(m.gated[unit, g], m.w_out[unit])).astype(BF16)


def backward_gate(m, unit, g, upstream):
    for at in range(0, E, 512):
        d_gated = dot(upstream, m.w_out[unit, cols(at), :], NT_DIMS).astype(BF16).astype(F32)
        p = m.proj[unit, g, :, cols(at)]
        sig = sigmoid(p)
        gate = p * sig
        m.d_mixed[g, :, cols(at)] = (d_gated * gate).astype(BF16)
        slope = sig + gate * (1.0 - sig)
        m.d_proj[g, :, cols(at)] = (d_gated * m.mixed[unit, g, :, cols(at)] * slope).astype(BF16)


def backward_attention(m, unit, g):
    d_weights = dot(m.d_mixed[g], m.value[unit, g], NT_DIMS).astype(BF16).astype(F32)
    query, keyed = m.query[unit, g], m.keyed[unit, g]
    r = positive_scores(unit, query, keyed)
    d_scores = (d_weights * r * (2.0 / length_of(unit) * S ** (-0.5))).astype(BF16)
    d_query = dot(d_scores, keyed).astype(BF16).astype(F32)
    d_keyed = dot(d_scores, query, TN).astype(BF16).astype(F32)
    p = m.proj[unit, g, :, 2 * E :]
    sig = sigmoid(p)
    z = p * sig
    d_z = d_query * m.scales[unit, 0:1, :] + d_keyed * m.scales[unit, 1:2, :]
    m.d_proj[g, :, 2 * E :] = (d_z * (sig + z * (1.0 - sig))).astype(BF16)
    m.small[unit, 4:5, :] += jnp.sum(d_query * z, axis=0, keepdims=True)
    m.small[unit, 5:6, :] += jnp.sum(d_keyed * z, axis=0, keepdims=True)
    weights = m.weights[unit, g]
    for at in range(0, E, 512):
        d_value = dot(weights, m.d_mixed[g, :, cols(at)], TN).astype(BF16).astype(F32)
        p = m.proj[unit, g, :, cols(E + at)]
        sig = sigmoid(p)
        m.d_proj[g, :, cols(E + at)] = (d_value * (sig + p * sig * (1.0 - sig))).astype(BF16)


def backward_input(m, unit, g, x, upstream):
    d_hidden = dot(m.d_proj[g], m.w_in[unit], NT_DIMS)
    xf = x.astype(F32)
    scaling = lax.rsqrt(jnp.mean(xf * xf, axis=-1, keepdims=True) + EPSILON)
    xs = xf * scaling
    d_gain = jnp.sum(d_hidden * xs, axis=0, keepdims=True)
    for i in range(4):
        m.small[unit, i : i + 1, :] += d_gain[:, 128 * i : 128 * i + 128]
    d_xs = d_hidden * m.gains[unit : unit + 1, :]
    d_x = scaling * (d_xs - xs * jnp.mean(d_xs * xs, axis=-1, keepdims=True))
    return (upstream.astype(F32) + d_x).astype(BF16)


def turned(m, unit):
    for g in (0, 1):
        m.hidden_t[unit, :, cols(BLOCK * g, BLOCK)] = m.hidden[unit, g].T
        m.gated_t[unit, :, cols(BLOCK * g, BLOCK)] = m.gated[unit, g].T


def weight_out_grad(m, unit, upstream):
    for i in range(4):
        rows = dot(m.gated_t[unit, cols(256 * i, 256), :], upstream).astype(BF16)
        parts = rows.reshape(4, 2, 2, 16, 512)
        for column in range(4):
            at = 2 * column
            m.grads[unit, i, :, :, at : at + 2] = parts[..., 128 * column : 128 * column + 128]


GATE = ((0, 512), (512, 512))
OTHERS = ((1024, 512), (1536, 512), (2048, 128))


def weight_in_grad(m, unit, columns):
    for at, width in columns:
        right = m.d_proj[:, :, cols(at, width)].reshape(2 * BLOCK, width)
        for i in (0, 1):
            part = dot(m.hidden_t[unit, cols(256 * i, 256), :], right).astype(BF16)
            part = part.reshape(2, 4, 2, 16, width)
            for j in range(width // 128):
                m.grads[unit, 2 * i : 2 * i + 2, :, :, 8 + at // 128 + j] = part[
                    ..., 128 * j : 128 * j + 128
                ]


class Memory:
    pass


SCRATCH = dict(
    w_in=((2, D, WIDE), BF16),
    w_out=((2, E, D), BF16),
    frames=((2, BLOCK, D), BF16),
    cot=((2, 8, 2, 16, D), BF16),
    first=((2, 8, 2, 16, D), BF16),
    first_pos=((2, 16, 16, D), BF16),
    cot_pos=((2, 16, 16, D), BF16),
    out_pos=((2, 16, 16, D), BF16),
    out=((2, 8, 2, 16, D), BF16),
    back_pos=((2, 16, 16, D), BF16),
    back=((2, 8, 2, 16, D), BF16),
    back_frames=((2, BLOCK, D), BF16),
    hidden=((2, 2, BLOCK, D), BF16),
    hidden_t=((2, D, 2 * BLOCK), BF16),
    proj=((2, 2, BLOCK, WIDE), F32),
    value=((2, 2, BLOCK, E), BF16),
    query=((2, 2, BLOCK, S), BF16),
    keyed=((2, 2, BLOCK, S), BF16),
    weights=((2, 2, BLOCK, BLOCK), BF16),
    mixed=((2, 2, BLOCK, E), F32),
    gated=((2, 2, BLOCK, E), BF16),
    gated_t=((2, E, 2 * BLOCK), BF16),
    d_mixed=((2, BLOCK, E), BF16),
    d_proj=((2, BLOCK, WIDE), BF16),
    grads=((2, 4, 4, 2, NT, 16, 128), BF16),
    small=((2, 8, 128), F32),
    scales=((2, 2, S), F32),
    gains=((2, D), F32),
)
GROUPS = (
    (1, (0, 8, 16), False),
    (1, (16, 25), False),
    (0, (0, 8, 16), False),
    (0, (16, 25), True),
)


def step_kernel(scaling, *refs):
    m = Memory()
    frames_hbm, cot_hbm, w_in_hbm, w_out_hbm, scales_hbm, gains_hbm = refs[:6]
    out_hbm, back_hbm, in_ref, wout_ref, small_ref = refs[6:11]
    refs = refs[11:]
    for name, ref in zip(SCRATCH, refs):
        setattr(m, name, ref)
    refs = refs[len(SCRATCH) :]
    sums = []
    for _, cuts, direct in GROUPS:
        count = len(sum_scratch(cuts, direct))
        sums.append(sum_refs(refs[:count]))
        refs = refs[count:]
    small_bufs = refs[0]
    local, send, recv = refs[1:4]
    k = Links(send, recv)
    p = 2 * k.zh + k.c

    def load(src, dst, sem):
        op = pltpu.make_async_copy(src, dst, local.at[sem])
        op.start()
        return op

    loads = dict(
        frames=load(frames_hbm, m.frames, 0),
        scales=load(scales_hbm, m.scales, 6),
        gains=load(gains_hbm, m.gains, 7),
        others_0=load(w_in_hbm.at[0, :, E:], m.w_in.at[0, :, E:], 1),
        gate_0=load(w_in_hbm.at[0, :, :E], m.w_in.at[0, :, :E], 8),
        out_0=load(w_out_hbm.at[0], m.w_out.at[0], 3),
    )
    met = greet(k)
    m.small[...] = jnp.zeros((2, 8, 128), F32)

    def peer(d):
        j = lax.rem(p + d, 8)
        return j, k.at(zh=j // 2, c=lax.rem(j, 2))

    def from_peer(d):
        j = lax.rem(p + 8 - d, 8)
        return j, k.at(zh=j // 2, c=lax.rem(j, 2))

    first_sems, cot_sems, out_sems, back_sems = (k.take(2) for _ in range(4))

    def first_copy(b, h, d, to):
        return k.copy(m.first.at[b, to[0], h], m.first_pos.at[h, 2 * p + b], to[1], first_sems + h)

    def cot_copy(h, d, to):
        box = m.cot_pos.at[h, pl.ds(2 * p, 2)]
        return k.copy(m.cot.at[:, to[0], h], box, to[1], cot_sems + h)

    def out_copy(h, d, to):
        box = m.out.at[:, p, h]
        return k.copy(m.out_pos.at[h, pl.ds(2 * to[0], 2)], box, to[1], out_sems + h)

    def back_copy(h, d, to):
        box = m.back.at[:, p, h]
        return k.copy(m.back_pos.at[h, pl.ds(2 * to[0], 2)], box, to[1], back_sems + h)

    def send(copy, h):
        for d in range(1, 8):
            copy(h, d, peer(d)).start()

    def receive(base, h):
        k.arrived(m.first_pos.at[0, 0:14], base + h)

    for name in ("frames", "scales", "gains", "others_0", "gate_0", "out_0"):
        loads[name].wait()
    loads = dict(
        cot=load(cot_hbm, m.cot, 2),
        in_1=load(w_in_hbm.at[1], m.w_in.at[1], 4),
        out_1=load(w_out_hbm.at[1], m.w_out.at[1], 5),
    )

    def exchange_first(b, h):
        for d in range(1, 8):
            first_copy(b, h, d, peer(d)).start()

    def block_forward(b):
        with jax.named_scope("f0"):
            m.first[b] = forward_group(m, 0, b, m.frames[b]).reshape(8, 2, 16, D)

    block_forward(0)
    with jax.named_scope("barrier"):
        met()
    for h in (0, 1):
        exchange_first(0, h)
    block_forward(1)
    for h in (0, 1):
        exchange_first(1, h)
        m.first_pos[h, pl.ds(2 * p, 2)] = m.first[:, p, h]
    loads["cot"].wait()
    for h in (0, 1):
        send(cot_copy, h)
        m.cot_pos[h, pl.ds(2 * p, 2)] = m.cot[:, p, h]
    with jax.named_scope("turn0"):
        turned(m, 0)
    loads["in_1"].wait()
    loads["out_1"].wait()

    @pl.loop(0, 2)
    def _(h):
        with jax.named_scope("w_first"):
            receive(first_sems, h)
        with jax.named_scope("f1"):
            x = m.first_pos[h].reshape(BLOCK, D)
            m.out_pos[h] = forward_group(m, 1, h, x).reshape(16, 16, D)

    m.out[:, p] = m.out_pos[:, pl.ds(2 * p, 2)].transpose(1, 0, 2, 3)
    with jax.named_scope("turn1"):
        turned(m, 1)

    groups = {}
    for name, (unit, cuts, direct), refs_of in zip(("a1", "b1", "a0", "b0"), GROUPS, sums):
        groups[name] = sum_stages(k, m.grads.at[unit], cuts, direct, *refs_of)
    groups["s"] = small_sum(k, small_bufs, m.small, small_ref)
    done = dict.fromkeys(groups, 0)

    def run(names):
        for name in names.split():
            with jax.named_scope(f"{name}_{done[name]}"):
                groups[name][done[name]]()
            done[name] += 1

    def unit_1_gate(h, wait=True):
        if wait:
            with jax.named_scope("w_cot"):
                receive(cot_sems, h)
        with jax.named_scope("gate1"):
            backward_gate(m, 1, h, m.cot_pos[h].reshape(BLOCK, D))

    def unit_1_rest(h):
        with jax.named_scope("rest1"):
            backward_attention(m, 1, h)
            x = m.first_pos[h].reshape(BLOCK, D)
            upstream = m.cot_pos[h].reshape(BLOCK, D)
            m.back_pos[h] = backward_input(m, 1, h, x, upstream).reshape(16, 16, D)
        send(back_copy, h)
        m.back[:, p, h] = m.back_pos[h, pl.ds(2 * p, 2)]

    def attention_0(g):
        with jax.named_scope("attn0"):
            backward_attention(m, 0, g)

    def input_0(g):
        with jax.named_scope("input0"):
            m.back_frames[g] = backward_input(m, 0, g, m.frames[g], m.back[g].reshape(BLOCK, D))

    def write(at):
        unit, cuts, direct = GROUPS[at]
        write_shard(cuts, direct, sums[at][-1], in_ref.at[unit], wout_ref.at[unit], scaling)

    unit_1_gate(0)
    unit_1_rest(0)
    with jax.named_scope("w_cot"):
        receive(cot_sems, 1)
    with jax.named_scope("wgo1"):
        weight_out_grad(m, 1, m.cot_pos[...].reshape(2 * BLOCK, D))
    run("a1")
    unit_1_gate(1, False)
    with jax.named_scope("wgi1"):
        weight_in_grad(m, 1, GATE)
    run("a1")
    unit_1_rest(1)
    run("a1")
    with jax.named_scope("wg1b"):
        weight_in_grad(m, 1, OTHERS)
    run("b1 b1 a1")
    with jax.named_scope("w_back"):
        receive(back_sems, 0)
        receive(back_sems, 1)
    for h in (0, 1):
        send(out_copy, h)
    with jax.named_scope("wgo0"):
        weight_out_grad(m, 0, m.back[...].reshape(2 * BLOCK, D))
    run("a0 b1")
    with jax.named_scope("gate0"):
        for g in (0, 1):
            backward_gate(m, 0, g, m.back[g].reshape(BLOCK, D))
    with jax.named_scope("wgi0"):
        weight_in_grad(m, 0, GATE)
    run("a0 a1")
    attention_0(0)
    run("a0")
    attention_0(1)
    run("b1")
    with jax.named_scope("wg0b"):
        weight_in_grad(m, 0, OTHERS)
    run("b0 a1")
    input_0(0)
    run("a0")
    input_0(1)
    store_back = load(m.back_frames, back_hbm, 0)
    run("b0 s b1 s a0 b0 b0 a0 a1 b1 s b0 s")
    with jax.named_scope("w_out"):
        receive(out_sems, 0)
        receive(out_sems, 1)
    store_out = load(m.out, out_hbm, 2)
    run("a0 s a1 b1")
    write(0)
    write(1)
    small_ref[...] = small_ref[...] * scaling
    run("b0 a0")
    write(2)
    run("b0")
    write(3)
    with jax.named_scope("drain"):
        k.drain()

        for base in (first_sems, cot_sems, out_sems, back_sems):
            for h in (0, 1):
                k.whole(m.first_pos.at[0, 0:14], base + h).wait_send()

        store_back.wait()
        store_out.wait()
    assert all(done[name] == len(stages) for name, stages in groups.items())
    assert k.used <= SEMS


def write_kernel(result, back, grad_in, grad_out, small, o_result, o_back, o_in, o_out, o_gains, o_scales):
    o_result[...] = result[...].reshape(o_result.shape)
    o_back[...] = back[...].reshape(o_back.shape)
    o_in[...] = grad_in[...]
    o_out[...] = grad_out[...]
    for unit in (0, 1):
        for i in range(4):
            o_gains[unit : unit + 1, 128 * i : 128 * i + 128] = small[unit, i : i + 1, :]
        o_scales[unit] = small[unit, 4:6, :]


def on_device(frames, cotangent, weight_in, qk_scales, weight_out, gains):
    tokens_all = frames.shape[0] * frames.shape[1] * lax.axis_size(DP) * lax.axis_size(SEQ)
    vmem = pl.BlockSpec(memory_space=pltpu.VMEM)
    hbm = pl.BlockSpec(memory_space=pl.ANY)
    scratch = [pltpu.VMEM(shape, dtype) for shape, dtype in SCRATCH.values()]
    for _, cuts, direct in GROUPS:
        scratch += sum_scratch(cuts, direct)
    scratch += [pltpu.VMEM((17, 2, 8, 128), F32)]
    dma = pltpu.SemaphoreType.DMA
    scratch += [dma((9,)), dma((SEMS,)), dma((SEMS,))]
    parts = pl.pallas_call(
        functools.partial(step_kernel, tokens_all ** (-0.5)),
        out_shape=(
            jax.ShapeDtypeStruct((2, 8, 2, 16, D), BF16),
            jax.ShapeDtypeStruct((2, BLOCK, D), BF16),
            jax.ShapeDtypeStruct((2, 16, WIDE), F32),
            jax.ShapeDtypeStruct((2, 32, D), F32),
            jax.ShapeDtypeStruct((2, 8, 128), F32),
        ),
        in_specs=[hbm] * 6,
        out_specs=(hbm, hbm, vmem, vmem, vmem),
        scratch_shapes=scratch,
        compiler_params=pltpu.CompilerParams(
            collective_id=0, has_side_effects=True, vmem_limit_bytes=67_043_328
        ),
    )(
        frames.reshape(2, BLOCK, D),
        cotangent.reshape(2, 8, 2, 16, D),
        weight_in,
        weight_out,
        qk_scales,
        gains,
    )
    return pl.pallas_call(
        write_kernel,
        out_shape=(
            jax.ShapeDtypeStruct(frames.shape, BF16),
            jax.ShapeDtypeStruct(frames.shape, BF16),
            jax.ShapeDtypeStruct((2, 16, WIDE), F32),
            jax.ShapeDtypeStruct((2, 32, D), F32),
            jax.ShapeDtypeStruct((2, D), F32),
            jax.ShapeDtypeStruct((2, 2, S), F32),
        ),
        in_specs=[vmem] * 5,
        out_specs=(vmem,) * 6,
    )(*parts)


def solution(mesh):
    split = Mesh(mesh.devices.reshape(4, 4, 2, 4, 2), DP + SEQ)
    placed = (P(DP, SEQ, None), P(DP, SEQ, None), P(), P(), P(), P())
    return jax.shard_map(
        on_device,
        mesh=split,
        in_specs=placed,
        out_specs=(
            P(DP, SEQ, None),
            P(DP, SEQ, None),
            P(None, DP, None),
            P(None, DP, None),
            P(),
            P(),
        ),
        check_vma=False,
    )
```

```python
import functools

import jax
import jax.numpy as jnp
from jax import lax
from jax.experimental import pallas as pl
from jax.experimental.pallas import tpu as pltpu
from jax.sharding import Mesh
from jax.sharding import PartitionSpec as P

DP = ("dp_0", "dp_1", "dp_2")
SEQ = ("seq_0", "seq_1")
D, E, S, BLOCK = 512, 1024, 128, 256
WIDE = 2 * E + S
EPSILON = 1e-06
F32, BF16 = jnp.float32, jnp.bfloat16
NT = 25
SEMS = 58


MESH = pl.DeviceIdType.MESH


def halves_of(n):
    return ((0, (n + 1) // 2), ((n + 1) // 2, n // 2))


def pieces_of(n):
    return n // 8, n - 7 * (n // 8)


class Links:
    def __init__(self, send, recv):
        self.send, self.recv, self.used, self.waits = send, recv, 0, []
        self.x, self.y, self.zl = (lax.axis_index(a) for a in DP)
        self.zh, self.c = (lax.axis_index(a) for a in SEQ)

    def take(self, count=1):
        at = self.used
        self.used += count
        return at

    def at(self, x=None, y=None, zl=None, zh=None, c=None):
        return (
            self.x if x is None else x,
            self.y if y is None else y,
            self.zl if zl is None else zl,
            self.zh if zh is None else zh,
            self.c if c is None else c,
        )

    def copy(self, src, dst, target, sem):
        return pltpu.make_async_remote_copy(
            src_ref=src,
            dst_ref=dst,
            send_sem=self.send.at[sem],
            recv_sem=self.recv.at[sem],
            device_id=target,
            device_id_type=MESH,
        )

    def whole(self, region, sem):
        return self.copy(region, region, self.at(c=1 - self.c), sem)

    def arrived(self, region, sem):
        self.whole(region, sem).wait_recv()

    def later(self, region, sem, when=None):
        def wait():
            if when is None:
                self.whole(region, sem).wait_send()
            else:

                @pl.when(when)
                def _():
                    self.whole(region, sem).wait_send()

        self.waits.append(wait)

    def drain(self):
        for wait in self.waits:
            wait()


def mod4(v):
    return lax.rem(v + 8, 4)


def greet(k):
    sem = pltpu.get_barrier_semaphore()
    targets = [k.at(x=mod4(k.x + d)) for d in (1, 2, 3)]
    targets += [k.at(y=mod4(k.y + d)) for d in (1, 2, 3)]
    for dl in (0, 1):
        for dh in range(4):
            for dc in (0, 1):
                if dl or dh or dc:
                    targets.append(
                        k.at(zl=lax.rem(k.zl + dl, 2), zh=mod4(k.zh + dh), c=lax.rem(k.c + dc, 2))
                    )
    for target in targets:
        pl.semaphore_signal(sem, inc=1, device_id=target, device_id_type=MESH)
    return lambda: pl.semaphore_wait(sem, len(targets))


def tree_sum(parts):
    while len(parts) > 1:
        parts = [a + b for a, b in zip(parts[::2], parts[1::2])]
    return parts[0]


def small_sum(k, buf, value_ref, out_ref):
    sems = {}
    axes = (
        ("z", 8, 1, 2 * k.zh + k.zl, lambda i: k.at(zh=i // 2, zl=lax.rem(i, 2))),
        ("x", 4, 9, k.x, lambda i: k.at(x=i)),
        ("y", 4, 13, k.y, lambda i: k.at(y=i)),
    )

    def share(axis, value):
        name, size, first, me, target = axis
        buf[first + me] = value
        sem = sems[name] = k.take()
        box = buf.at[first + me]
        for d in range(1, size):
            k.copy(box, box, target(lax.rem(me + d, size)), sem).start()
        k.later(buf.at[first : first + size - 1], sem)

    def collected(axis):
        name, size, first, _, _ = axis
        k.arrived(buf.at[first : first + size - 1], sems[name])
        return tree_sum([buf[first + i] for i in range(size)])

    def pair():
        sems["p"] = k.take()
        k.copy(value_ref, buf.at[0], k.at(c=1 - k.c), sems["p"]).start()
        k.later(buf.at[0], sems["p"])

    def z():
        k.arrived(buf.at[0], sems["p"])
        share(axes[0], value_ref[...] + buf[0])

    def x():
        share(axes[1], collected(axes[0]))

    def y():
        share(axes[2], collected(axes[1]))

    def end():
        out_ref[...] = collected(axes[2])

    return [pair, z, x, y, end]


def sum_stages(k, grads, cuts, direct, paired, first_in, second_in, z_in, gathered):
    sems = {}
    me = (k.x, k.y)
    t_base, n_tiles = cuts[0], cuts[-1] - cuts[0]
    halves = halves_of(n_tiles)
    f32 = jnp.float32

    def to_axis(half, step, delta):
        along = (half + step) % 2
        return k.at(x=mod4(k.x + delta)) if along == 0 else k.at(y=mod4(k.y + delta))

    def view(half, step, delta, part=None):
        t0, n = halves[half]
        along = (half + step) % 2
        dest = mod4(me[along] + delta)
        if step == 0:
            sub = pl.ds(0, 4) if part is None else pl.ds(2 * part, 2)
            at = (dest, sub) if along == 0 else (sub, dest)
        else:
            at = (dest, k.y) if along == 0 else (k.x, dest)
        return paired.at[at[0], at[1], t0 : t0 + n]

    def pair_copy(i):
        lo, hi = cuts[i], cuts[i + 1]
        return k.copy(
            grads.at[:, :, 1 - k.c, lo:hi],
            paired.at[:, :, lo - t_base : hi - t_base],
            k.at(c=1 - k.c),
            sems["pair", i],
        )

    def pair_out(i):
        sems["pair", i] = k.take()
        op = pair_copy(i)
        op.start()
        k.waits.append(op.wait_send)

    def pair_in():
        for i in range(len(cuts) - 1):
            pair_copy(i).wait_recv()

        for half, (t0, n) in enumerate(halves):

            @pl.loop(0, 4)
            def _(i):
                own = grads[i, :, k.c, t_base + t0 : t_base + t0 + n]
                paired[i, :, t0 : t0 + n] = paired[i, :, t0 : t0 + n] + own

            outset(half)

    def spread(half):
        box = second_in[half]
        sem = sems[half, 1] = k.take()
        for d in (2, 1, 3):
            k.copy(view(half, 1, d), box.at[d - 1], to_axis(half, 1, d), sem).start()
        k.later(box, sem)

    def collect_spread(half):
        box = second_in[half]
        k.arrived(box, sems[half, 1])
        own = view(half, 1, 0)
        near = box[0].astype(f32) + box[2].astype(f32)
        own[...] = ((own[...].astype(f32) + box[1].astype(f32)) + near).astype(jnp.bfloat16)

    ways = ((0, 1), (1, -1))

    def outset(half):
        one, two = first_in[half]
        base = sems[half, 0] = k.take(2)
        for way, delta in ways:
            target = to_axis(half, 0, delta)
            k.copy(view(half, 0, 2, way), one.at[way], target, base).start()
        for way, delta in ways:
            part = 1 - way
            box = two.at[way, 2 * part : 2 * part + 2]
            k.copy(view(half, 0, delta, part), box, to_axis(half, 0, delta), base + 1).start()
        k.later(one, base)

    def relay():
        for half in (0, 1):
            one, two = first_in[half]
            base = sems[half, 0]
            k.arrived(one, base)
            for way, delta in ways:
                target = view(half, 0, delta, way)
                target[...] = target[...] + one[way]
                box = two.at[way, 2 * way : 2 * way + 2]
                k.copy(target, box, to_axis(half, 0, delta), base + 1).start()
            k.later(two, base + 1)

    def collect(half):
        two = first_in[half][1]
        k.arrived(two, sems[half, 0] + 1)
        own = view(half, 0, 0)
        own[...] = (own[...].astype(f32) + (two[0].astype(f32) + two[1].astype(f32))).astype(
            jnp.bfloat16
        )

    def turn():
        for half in (0, 1):
            collect(half)
            spread(half)

    spot = 2 * k.zh + k.zl
    holds = k.zl == k.c
    piece_step, piece_size = pieces_of(n_tiles)

    def z_out():
        for half in (0, 1):
            collect_spread(half)
        sem = sems["z"] = k.take()
        for q in range(4):
            for e in range(2):
                piece = piece_step * (2 * q + e)
                source = paired.at[k.x, k.y, piece : piece + piece_size]
                mine = (k.zh == q) & (k.c == e) & holds
                op = k.copy(source, z_in.at[spot], k.at(zl=k.c, zh=q, c=e), sem)

                @pl.when(jnp.logical_not(mine))
                def _():
                    op.start()

                @pl.when(mine)
                def _():
                    z_in[spot] = source[...]

        k.later(z_in.at[0:7], sem, holds)
        k.later(z_in, sem, jnp.logical_not(holds))

    def z_sum():
        @pl.when(holds)
        def _():
            k.arrived(z_in.at[0:7], sems["z"])

        @pl.when(jnp.logical_not(holds))
        def _():
            k.arrived(z_in, sems["z"])

        p = 2 * k.zh + k.c
        gathered[p] = tree_sum([z_in[i].astype(f32) for i in range(8)]).astype(jnp.bfloat16)
        sem = sems["g"] = k.take()
        box = gathered.at[p]
        for d in range(1, 8):
            to = lax.rem(p + d, 8)
            k.copy(box, box, k.at(zh=to // 2, c=lax.rem(to, 2)), sem).start()
        k.later(gathered.at[0:7], sem)

    def gather():
        k.arrived(gathered.at[0:7], sems["g"])

    def whole_out():
        for half in (0, 1):
            collect_spread(half)
        sem = sems["z"] = k.take()
        for q in range(4):
            op = k.copy(paired.at[k.x, k.y], z_in.at[spot], k.at(zl=k.c, zh=q), sem)

            @pl.when(jnp.logical_not(holds & (k.zh == q)))
            def _():
                op.start()

        @pl.when(holds)
        def _():
            z_in[spot] = paired[k.x, k.y]

        k.later(z_in.at[0:3], sem, holds)
        k.later(z_in.at[0:4], sem, jnp.logical_not(holds))

    def whole_sum():
        sems["g"] = k.take()

        @pl.when(holds)
        def _():
            k.arrived(z_in.at[0:7], sems["z"])
            gathered[0] = tree_sum([z_in[i].astype(f32) for i in range(8)]).astype(jnp.bfloat16)
            k.whole(gathered, sems["g"]).start()

        k.later(gathered, sems["g"], holds)

    def whole_in():
        @pl.when(jnp.logical_not(holds))
        def _():
            k.arrived(gathered, sems["g"])

    pairs = [functools.partial(pair_out, i) for i in range(len(cuts) - 1)]
    if direct:
        return pairs + [pair_in, relay, turn, whole_out, whole_sum, whole_in]
    return pairs + [pair_in, relay, turn, z_out, z_sum, gather]


def write_shard(cuts, direct, gathered, grad_in_ref, grad_out_ref, scaling):
    t_base, n_tiles = cuts[0], cuts[-1] - cuts[0]
    piece_step = n_tiles if direct else pieces_of(n_tiles)[0]
    for at in range(n_tiles):
        p = min(at // piece_step, 7)
        values = gathered[p, at - piece_step * p].astype(jnp.float32) * scaling
        tile = t_base + at
        if tile < 8:
            column, half = tile // 2, tile % 2
            grad_out_ref[16 * half : 16 * half + 16, 128 * column : 128 * column + 128] = values
        else:
            grad_in_ref[:, 128 * (tile - 8) : 128 * (tile - 7)] = values


def sum_scratch(cuts, direct):
    n_tiles = cuts[-1] - cuts[0]

    def tiles(*lead):
        return pltpu.VMEM((*lead, 16, 128), jnp.bfloat16)

    shapes = [tiles(4, 4, n_tiles)]
    for _, n in halves_of(n_tiles):
        shapes += [tiles(2, 2, n), tiles(2, 4, n)]
    shapes += [tiles(3, n) for _, n in halves_of(n_tiles)]
    if direct:
        return shapes + [tiles(8, n_tiles), tiles(1, n_tiles)]
    return shapes + [tiles(8, pieces_of(n_tiles)[1])] * 2


def sum_refs(refs):
    return refs[0], (refs[1:3], refs[3:5]), refs[5:7], refs[7], refs[8]


NN = (((1,), (0,)), ((), ()))
NT_DIMS = (((1,), (1,)), ((), ()))
TN = (((0,), (0,)), ((), ()))


def dot(a, b, dims=NN):
    return lax.dot_general(a, b, dims, preferred_element_type=F32)


def sigmoid(p):
    return 0.5 * jnp.tanh(0.5 * p) + 0.5


def cols(at, width=512):
    return slice(at, at + width)


def group_mask(unit):
    if unit == 0:
        return None
    row = lax.broadcasted_iota(jnp.int32, (BLOCK, BLOCK), 0)
    column = lax.broadcasted_iota(jnp.int32, (BLOCK, BLOCK), 1)
    return lax.rem(row, 16) == lax.rem(column, 16)


def positive_scores(unit, query, keyed):
    r = jnp.maximum(dot(query, keyed, NT_DIMS) * S ** (-0.5), 0.0)
    mask = group_mask(unit)
    return r if mask is None else jnp.where(mask, r, 0.0)


def length_of(unit):
    return BLOCK if unit == 0 else 16


def forward_group(m, unit, g, x):
    xf = x.astype(F32)
    scaling = lax.rsqrt(jnp.mean(xf * xf, axis=-1, keepdims=True) + EPSILON)
    hidden = (xf * scaling * m.gains[unit : unit + 1, :]).astype(BF16)
    m.hidden[unit, g] = hidden
    p = dot(hidden, m.w_in[unit, :, 2 * E :])
    m.proj[unit, g, :, 2 * E :] = p
    z = p * sigmoid(p)
    query = (z * m.scales[unit, 0:1, :]).astype(BF16)
    keyed = (z * m.scales[unit, 1:2, :]).astype(BF16)
    m.query[unit, g] = query
    m.keyed[unit, g] = keyed
    r = positive_scores(unit, query, keyed)
    weights = (r * r * (1.0 / length_of(unit))).astype(BF16)
    m.weights[unit, g] = weights
    for at in range(0, E, 512):
        p = dot(hidden, m.w_in[unit, :, cols(E + at)])
        m.proj[unit, g, :, cols(E + at)] = p
        m.value[unit, g, :, cols(at)] = (p * sigmoid(p)).astype(BF16)
        p = dot(hidden, m.w_in[unit, :, cols(at)])
        m.proj[unit, g, :, cols(at)] = p
        mixed = dot(weights, m.value[unit, g, :, cols(at)])
        m.mixed[unit, g, :, cols(at)] = mixed
        m.gated[unit, g, :, cols(at)] = (p * sigmoid(p) * mixed).astype(BF16)
    return (x.astype(F32) + dot(m.gated[unit, g], m.w_out[unit])).astype(BF16)


def backward_gate(m, unit, g, upstream):
    for at in range(0, E, 512):
        d_gated = dot(upstream, m.w_out[unit, cols(at), :], NT_DIMS).astype(BF16).astype(F32)
        p = m.proj[unit, g, :, cols(at)]
        sig = sigmoid(p)
        gate = p * sig
        m.d_mixed[g, :, cols(at)] = (d_gated * gate).astype(BF16)
        slope = sig + gate * (1.0 - sig)
        m.d_proj[g, :, cols(at)] = (d_gated * m.mixed[unit, g, :, cols(at)] * slope).astype(BF16)


def backward_attention(m, unit, g):
    d_weights = dot(m.d_mixed[g], m.value[unit, g], NT_DIMS).astype(BF16).astype(F32)
    query, keyed = m.query[unit, g], m.keyed[unit, g]
    r = positive_scores(unit, query, keyed)
    d_scores = (d_weights * r * (2.0 / length_of(unit) * S ** (-0.5))).astype(BF16)
    d_query = dot(d_scores, keyed).astype(BF16).astype(F32)
    d_keyed = dot(d_scores, query, TN).astype(BF16).astype(F32)
    p = m.proj[unit, g, :, 2 * E :]
    sig = sigmoid(p)
    z = p * sig
    d_z = d_query * m.scales[unit, 0:1, :] + d_keyed * m.scales[unit, 1:2, :]
    m.d_proj[g, :, 2 * E :] = (d_z * (sig + z * (1.0 - sig))).astype(BF16)
    m.small[unit, 4:5, :] += jnp.sum(d_query * z, axis=0, keepdims=True)
    m.small[unit, 5:6, :] += jnp.sum(d_keyed * z, axis=0, keepdims=True)
    weights = m.weights[unit, g]
    for at in range(0, E, 512):
        d_value = dot(weights, m.d_mixed[g, :, cols(at)], TN).astype(BF16).astype(F32)
        p = m.proj[unit, g, :, cols(E + at)]
        sig = sigmoid(p)
        m.d_proj[g, :, cols(E + at)] = (d_value * (sig + p * sig * (1.0 - sig))).astype(BF16)


def backward_input(m, unit, g, x, upstream):
    d_hidden = dot(m.d_proj[g], m.w_in[unit], NT_DIMS)
    xf = x.astype(F32)
    scaling = lax.rsqrt(jnp.mean(xf * xf, axis=-1, keepdims=True) + EPSILON)
    xs = xf * scaling
    d_gain = jnp.sum(d_hidden * xs, axis=0, keepdims=True)
    for i in range(4):
        m.small[unit, i : i + 1, :] += d_gain[:, 128 * i : 128 * i + 128]
    d_xs = d_hidden * m.gains[unit : unit + 1, :]
    d_x = scaling * (d_xs - xs * jnp.mean(d_xs * xs, axis=-1, keepdims=True))
    return (upstream.astype(F32) + d_x).astype(BF16)


def turned(m, unit):
    for g in (0, 1):
        m.hidden_t[unit, :, cols(BLOCK * g, BLOCK)] = m.hidden[unit, g].T
        m.gated_t[unit, :, cols(BLOCK * g, BLOCK)] = m.gated[unit, g].T


def weight_out_grad(m, unit, upstream):
    for i in range(4):
        rows = dot(m.gated_t[unit, cols(256 * i, 256), :], upstream).astype(BF16)
        parts = rows.reshape(4, 2, 2, 16, 512)
        for column in range(4):
            at = 2 * column
            m.grads[unit, i, :, :, at : at + 2] = parts[..., 128 * column : 128 * column + 128]


GATE = ((0, 512), (512, 512))
OTHERS = ((1024, 512), (1536, 512), (2048, 128))


def weight_in_grad(m, unit, columns):
    for at, width in columns:
        right = m.d_proj[:, :, cols(at, width)].reshape(2 * BLOCK, width)
        for i in (0, 1):
            part = dot(m.hidden_t[unit, cols(256 * i, 256), :], right).astype(BF16)
            part = part.reshape(2, 4, 2, 16, width)
            for j in range(width // 128):
                m.grads[unit, 2 * i : 2 * i + 2, :, :, 8 + at // 128 + j] = part[
                    ..., 128 * j : 128 * j + 128
                ]


class Memory:
    pass


SCRATCH = dict(
    w_in=((2, D, WIDE), BF16),
    w_out=((2, E, D), BF16),
    frames=((2, BLOCK, D), BF16),
    cot=((2, 8, 2, 16, D), BF16),
    first=((2, 8, 2, 16, D), BF16),
    first_pos=((2, 16, 16, D), BF16),
    cot_pos=((2, 16, 16, D), BF16),
    out_pos=((2, 16, 16, D), BF16),
    out=((2, 8, 2, 16, D), BF16),
    back_pos=((2, 16, 16, D), BF16),
    back=((2, 8, 2, 16, D), BF16),
    back_frames=((2, BLOCK, D), BF16),
    hidden=((2, 2, BLOCK, D), BF16),
    hidden_t=((2, D, 2 * BLOCK), BF16),
    proj=((2, 2, BLOCK, WIDE), F32),
    value=((2, 2, BLOCK, E), BF16),
    query=((2, 2, BLOCK, S), BF16),
    keyed=((2, 2, BLOCK, S), BF16),
    weights=((2, 2, BLOCK, BLOCK), BF16),
    mixed=((2, 2, BLOCK, E), F32),
    gated=((2, 2, BLOCK, E), BF16),
    gated_t=((2, E, 2 * BLOCK), BF16),
    d_mixed=((2, BLOCK, E), BF16),
    d_proj=((2, BLOCK, WIDE), BF16),
    grads=((2, 4, 4, 2, NT, 16, 128), BF16),
    small=((2, 8, 128), F32),
    scales=((2, 2, S), F32),
    gains=((2, D), F32),
)
GROUPS = (
    (1, (0, 8, 16), False),
    (1, (16, 25), False),
    (0, (0, 8, 16), False),
    (0, (16, 25), True),
)


def step_kernel(scaling, *refs):
    m = Memory()
    frames_hbm, cot_hbm, w_in_hbm, w_out_hbm, scales_hbm, gains_hbm = refs[:6]
    out_hbm, back_hbm, in_ref, wout_ref, small_ref = refs[6:11]
    refs = refs[11:]
    for name, ref in zip(SCRATCH, refs):
        setattr(m, name, ref)
    refs = refs[len(SCRATCH) :]
    sums = []
    for _, cuts, direct in GROUPS:
        count = len(sum_scratch(cuts, direct))
        sums.append(sum_refs(refs[:count]))
        refs = refs[count:]
    small_bufs = refs[0]
    local, send, recv = refs[1:4]
    k = Links(send, recv)
    p = 2 * k.zh + k.c

    def load(src, dst, sem):
        op = pltpu.make_async_copy(src, dst, local.at[sem])
        op.start()
        return op

    loads = dict(
        frames=load(frames_hbm, m.frames, 0),
        scales=load(scales_hbm, m.scales, 6),
        gains=load(gains_hbm, m.gains, 7),
        others_0=load(w_in_hbm.at[0, :, E:], m.w_in.at[0, :, E:], 1),
        gate_0=load(w_in_hbm.at[0, :, :E], m.w_in.at[0, :, :E], 8),
        out_0=load(w_out_hbm.at[0], m.w_out.at[0], 3),
    )
    met = greet(k)
    m.small[...] = jnp.zeros((2, 8, 128), F32)

    def peer(d):
        j = lax.rem(p + d, 8)
        return j, k.at(zh=j // 2, c=lax.rem(j, 2))

    def from_peer(d):
        j = lax.rem(p + 8 - d, 8)
        return j, k.at(zh=j // 2, c=lax.rem(j, 2))

    first_sems, cot_sems, out_sems, back_sems = (k.take(2) for _ in range(4))

    def first_copy(b, h, d, to):
        return k.copy(m.first.at[b, to[0], h], m.first_pos.at[h, 2 * p + b], to[1], first_sems + h)

    def cot_copy(h, d, to):
        box = m.cot_pos.at[h, pl.ds(2 * p, 2)]
        return k.copy(m.cot.at[:, to[0], h], box, to[1], cot_sems + h)

    def out_copy(h, d, to):
        box = m.out.at[:, p, h]
        return k.copy(m.out_pos.at[h, pl.ds(2 * to[0], 2)], box, to[1], out_sems + h)

    def back_copy(b, h, d, to):
        return k.copy(m.back_pos.at[h, 2 * to[0] + b], m.back.at[b, p, h], to[1], back_sems + b)

    def send(copy, h):
        for d in range(1, 8):
            copy(h, d, peer(d)).start()

    def receive(base, h):
        k.arrived(m.first_pos.at[0, 0:14], base + h)

    for name in ("frames", "scales", "gains", "others_0", "gate_0", "out_0"):
        loads[name].wait()
    loads = dict(
        cot=load(cot_hbm, m.cot, 2),
        in_1=load(w_in_hbm.at[1], m.w_in.at[1], 4),
        out_1=load(w_out_hbm.at[1], m.w_out.at[1], 5),
    )

    def exchange_first(b, h):
        for d in range(1, 8):
            first_copy(b, h, d, peer(d)).start()

    def block_forward(b):
        with jax.named_scope("f0"):
            m.first[b] = forward_group(m, 0, b, m.frames[b]).reshape(8, 2, 16, D)

    block_forward(0)
    with jax.named_scope("barrier"):
        met()
    for h in (0, 1):
        exchange_first(0, h)
    block_forward(1)
    for h in (0, 1):
        exchange_first(1, h)
        m.first_pos[h, pl.ds(2 * p, 2)] = m.first[:, p, h]
    loads["cot"].wait()
    for h in (0, 1):
        send(cot_copy, h)
        m.cot_pos[h, pl.ds(2 * p, 2)] = m.cot[:, p, h]
    with jax.named_scope("turn0"):
        turned(m, 0)
    loads["in_1"].wait()
    loads["out_1"].wait()

    @pl.loop(0, 2)
    def _(h):
        with jax.named_scope("w_first"):
            receive(first_sems, h)
        with jax.named_scope("f1"):
            x = m.first_pos[h].reshape(BLOCK, D)
            m.out_pos[h] = forward_group(m, 1, h, x).reshape(16, 16, D)

    m.out[:, p] = m.out_pos[:, pl.ds(2 * p, 2)].transpose(1, 0, 2, 3)
    with jax.named_scope("turn1"):
        turned(m, 1)

    groups = {}
    for name, (unit, cuts, direct), refs_of in zip(("a1", "b1", "a0", "b0"), GROUPS, sums):
        groups[name] = sum_stages(k, m.grads.at[unit], cuts, direct, *refs_of)
    groups["s"] = small_sum(k, small_bufs, m.small, small_ref)
    done = dict.fromkeys(groups, 0)

    def run(names):
        for name in names.split():
            with jax.named_scope(f"{name}_{done[name]}"):
                groups[name][done[name]]()
            done[name] += 1

    def unit_1_gate(h, wait=True):
        if wait:
            with jax.named_scope("w_cot"):
                receive(cot_sems, h)
        with jax.named_scope("gate1"):
            backward_gate(m, 1, h, m.cot_pos[h].reshape(BLOCK, D))

    def unit_1_rest(h):
        with jax.named_scope("rest1"):
            backward_attention(m, 1, h)
            x = m.first_pos[h].reshape(BLOCK, D)
            upstream = m.cot_pos[h].reshape(BLOCK, D)
            m.back_pos[h] = backward_input(m, 1, h, x, upstream).reshape(16, 16, D)
        for b in (0, 1):
            send(functools.partial(back_copy, b), h)
        m.back[:, p, h] = m.back_pos[h, pl.ds(2 * p, 2)]

    def gate_0(g, wait=True):
        if wait:
            with jax.named_scope("w_back"):
                receive(back_sems, g)
        with jax.named_scope("gate0"):
            backward_gate(m, 0, g, m.back[g].reshape(BLOCK, D))

    def attention_0(g):
        with jax.named_scope("attn0"):
            backward_attention(m, 0, g)

    def input_0(g):
        with jax.named_scope("input0"):
            m.back_frames[g] = backward_input(m, 0, g, m.frames[g], m.back[g].reshape(BLOCK, D))

    def write(at):
        unit, cuts, direct = GROUPS[at]
        write_shard(cuts, direct, sums[at][-1], in_ref.at[unit], wout_ref.at[unit], scaling)

    unit_1_gate(0)
    unit_1_rest(0)
    with jax.named_scope("w_cot"):
        receive(cot_sems, 1)
    with jax.named_scope("wgo1"):
        weight_out_grad(m, 1, m.cot_pos[...].reshape(2 * BLOCK, D))
    run("a1")
    unit_1_gate(1, False)
    with jax.named_scope("wgi1"):
        weight_in_grad(m, 1, GATE)
    run("a1")
    unit_1_rest(1)
    run("a1")
    with jax.named_scope("wg1b"):
        weight_in_grad(m, 1, OTHERS)
    run("b1 b1 a1")
    gate_0(0)
    with jax.named_scope("w_back1"):
        receive(back_sems, 1)
    for h in (0, 1):
        send(out_copy, h)
    with jax.named_scope("wgo0"):
        weight_out_grad(m, 0, m.back[...].reshape(2 * BLOCK, D))
    run("a0 b1")
    gate_0(1, False)
    with jax.named_scope("wgi0"):
        weight_in_grad(m, 0, GATE)
    run("a0 a1")
    attention_0(0)
    run("a0")
    attention_0(1)
    run("b1")
    with jax.named_scope("wg0b"):
        weight_in_grad(m, 0, OTHERS)
    run("b0 a1")
    input_0(0)
    run("a0")
    input_0(1)
    store_back = load(m.back_frames, back_hbm, 0)
    run("b0 s b1 s a0 b0 b0 a0 a1 b1 s b0 s")
    with jax.named_scope("w_out"):
        receive(out_sems, 0)
        receive(out_sems, 1)
    store_out = load(m.out, out_hbm, 2)
    run("a0 s a1 b1")
    write(0)
    write(1)
    small_ref[...] = small_ref[...] * scaling
    run("b0 a0")
    write(2)
    run("b0")
    write(3)
    with jax.named_scope("drain"):
        k.drain()

        for base in (first_sems, cot_sems, out_sems, back_sems):
            for h in (0, 1):
                k.whole(m.first_pos.at[0, 0:14], base + h).wait_send()

        store_back.wait()
        store_out.wait()
    assert all(done[name] == len(stages) for name, stages in groups.items())
    assert k.used <= SEMS


def write_kernel(result, back, grad_in, grad_out, small, o_result, o_back, o_in, o_out, o_gains, o_scales):
    o_result[...] = result[...].reshape(o_result.shape)
    o_back[...] = back[...].reshape(o_back.shape)
    o_in[...] = grad_in[...]
    o_out[...] = grad_out[...]
    for unit in (0, 1):
        for i in range(4):
            o_gains[unit : unit + 1, 128 * i : 128 * i + 128] = small[unit, i : i + 1, :]
        o_scales[unit] = small[unit, 4:6, :]


def on_device(frames, cotangent, weight_in, qk_scales, weight_out, gains):
    tokens_all = frames.shape[0] * frames.shape[1] * lax.axis_size(DP) * lax.axis_size(SEQ)
    vmem = pl.BlockSpec(memory_space=pltpu.VMEM)
    hbm = pl.BlockSpec(memory_space=pl.ANY)
    scratch = [pltpu.VMEM(shape, dtype) for shape, dtype in SCRATCH.values()]
    for _, cuts, direct in GROUPS:
        scratch += sum_scratch(cuts, direct)
    scratch += [pltpu.VMEM((17, 2, 8, 128), F32)]
    dma = pltpu.SemaphoreType.DMA
    scratch += [dma((9,)), dma((SEMS,)), dma((SEMS,))]
    parts = pl.pallas_call(
        functools.partial(step_kernel, tokens_all ** (-0.5)),
        out_shape=(
            jax.ShapeDtypeStruct((2, 8, 2, 16, D), BF16),
            jax.ShapeDtypeStruct((2, BLOCK, D), BF16),
            jax.ShapeDtypeStruct((2, 16, WIDE), F32),
            jax.ShapeDtypeStruct((2, 32, D), F32),
            jax.ShapeDtypeStruct((2, 8, 128), F32),
        ),
        in_specs=[hbm] * 6,
        out_specs=(hbm, hbm, vmem, vmem, vmem),
        scratch_shapes=scratch,
        compiler_params=pltpu.CompilerParams(
            collective_id=0, has_side_effects=True, vmem_limit_bytes=67_043_328
        ),
    )(
        frames.reshape(2, BLOCK, D),
        cotangent.reshape(2, 8, 2, 16, D),
        weight_in,
        weight_out,
        qk_scales,
        gains,
    )
    return pl.pallas_call(
        write_kernel,
        out_shape=(
            jax.ShapeDtypeStruct(frames.shape, BF16),
            jax.ShapeDtypeStruct(frames.shape, BF16),
            jax.ShapeDtypeStruct((2, 16, WIDE), F32),
            jax.ShapeDtypeStruct((2, 32, D), F32),
            jax.ShapeDtypeStruct((2, D), F32),
            jax.ShapeDtypeStruct((2, 2, S), F32),
        ),
        in_specs=[vmem] * 5,
        out_specs=(vmem,) * 6,
    )(*parts)


def solution(mesh):
    split = Mesh(mesh.devices.reshape(4, 4, 2, 4, 2), DP + SEQ)
    placed = (P(DP, SEQ, None), P(DP, SEQ, None), P(), P(), P(), P())
    return jax.shard_map(
        on_device,
        mesh=split,
        in_specs=placed,
        out_specs=(
            P(DP, SEQ, None),
            P(DP, SEQ, None),
            P(None, DP, None),
            P(None, DP, None),
            P(),
            P(),
        ),
        check_vma=False,
    )
```

```python
import functools

import jax
import jax.numpy as jnp
from jax import lax
from jax.experimental import pallas as pl
from jax.experimental.pallas import tpu as pltpu
from jax.sharding import Mesh
from jax.sharding import PartitionSpec as P

DP = ("dp_0", "dp_1", "dp_2")
SEQ = ("seq_0", "seq_1")
D, E, S, BLOCK = 512, 1024, 128, 256
WIDE = 2 * E + S
EPSILON = 1e-06
F32, BF16 = jnp.float32, jnp.bfloat16
NT = 25
SEMS = 58


MESH = pl.DeviceIdType.MESH


def halves_of(n):
    return ((0, (n + 1) // 2), ((n + 1) // 2, n // 2))


def pieces_of(n):
    return n // 8, n - 7 * (n // 8)


class Links:
    def __init__(self, send, recv):
        self.send, self.recv, self.used, self.waits = send, recv, 0, []
        self.x, self.y, self.zl = (lax.axis_index(a) for a in DP)
        self.zh, self.c = (lax.axis_index(a) for a in SEQ)

    def take(self, count=1):
        at = self.used
        self.used += count
        return at

    def at(self, x=None, y=None, zl=None, zh=None, c=None):
        return (
            self.x if x is None else x,
            self.y if y is None else y,
            self.zl if zl is None else zl,
            self.zh if zh is None else zh,
            self.c if c is None else c,
        )

    def copy(self, src, dst, target, sem):
        return pltpu.make_async_remote_copy(
            src_ref=src,
            dst_ref=dst,
            send_sem=self.send.at[sem],
            recv_sem=self.recv.at[sem],
            device_id=target,
            device_id_type=MESH,
        )

    def whole(self, region, sem):
        return self.copy(region, region, self.at(c=1 - self.c), sem)

    def arrived(self, region, sem):
        self.whole(region, sem).wait_recv()

    def later(self, region, sem, when=None):
        def wait():
            if when is None:
                self.whole(region, sem).wait_send()
            else:

                @pl.when(when)
                def _():
                    self.whole(region, sem).wait_send()

        self.waits.append(wait)

    def drain(self):
        for wait in self.waits:
            wait()


def mod4(v):
    return lax.rem(v + 8, 4)


def greet(k):
    sem = pltpu.get_barrier_semaphore()
    targets = [k.at(x=mod4(k.x + d)) for d in (1, 2, 3)]
    targets += [k.at(y=mod4(k.y + d)) for d in (1, 2, 3)]
    for dl in (0, 1):
        for dh in range(4):
            for dc in (0, 1):
                if dl or dh or dc:
                    targets.append(
                        k.at(zl=lax.rem(k.zl + dl, 2), zh=mod4(k.zh + dh), c=lax.rem(k.c + dc, 2))
                    )
    for target in targets:
        pl.semaphore_signal(sem, inc=1, device_id=target, device_id_type=MESH)
    return lambda: pl.semaphore_wait(sem, len(targets))


def tree_sum(parts):
    while len(parts) > 1:
        parts = [a + b for a, b in zip(parts[::2], parts[1::2])]
    return parts[0]


def small_sum(k, buf, value_ref, out_ref):
    sems = {}
    axes = (
        ("z", 8, 1, 2 * k.zh + k.zl, lambda i: k.at(zh=i // 2, zl=lax.rem(i, 2))),
        ("x", 4, 9, k.x, lambda i: k.at(x=i)),
        ("y", 4, 13, k.y, lambda i: k.at(y=i)),
    )

    def share(axis, value):
        name, size, first, me, target = axis
        buf[first + me] = value
        sem = sems[name] = k.take()
        box = buf.at[first + me]
        for d in range(1, size):
            k.copy(box, box, target(lax.rem(me + d, size)), sem).start()
        k.later(buf.at[first : first + size - 1], sem)

    def collected(axis):
        name, size, first, _, _ = axis
        k.arrived(buf.at[first : first + size - 1], sems[name])
        return tree_sum([buf[first + i] for i in range(size)])

    def pair():
        sems["p"] = k.take()
        k.copy(value_ref, buf.at[0], k.at(c=1 - k.c), sems["p"]).start()
        k.later(buf.at[0], sems["p"])

    def z():
        k.arrived(buf.at[0], sems["p"])
        share(axes[0], value_ref[...] + buf[0])

    def x():
        share(axes[1], collected(axes[0]))

    def y():
        share(axes[2], collected(axes[1]))

    def end():
        out_ref[...] = collected(axes[2])

    return [pair, z, x, y, end]


def sum_stages(k, grads, cuts, direct, paired, first_in, second_in, z_in, gathered):
    sems = {}
    me = (k.x, k.y)
    t_base, n_tiles = cuts[0], cuts[-1] - cuts[0]
    halves = halves_of(n_tiles)
    f32 = jnp.float32

    def to_axis(half, step, delta):
        along = (half + step) % 2
        return k.at(x=mod4(k.x + delta)) if along == 0 else k.at(y=mod4(k.y + delta))

    def view(half, step, delta, part=None):
        t0, n = halves[half]
        along = (half + step) % 2
        dest = mod4(me[along] + delta)
        if step == 0:
            sub = pl.ds(0, 4) if part is None else pl.ds(2 * part, 2)
            at = (dest, sub) if along == 0 else (sub, dest)
        else:
            at = (dest, k.y) if along == 0 else (k.x, dest)
        return paired.at[at[0], at[1], t0 : t0 + n]

    def pair_copy(i):
        lo, hi = cuts[i], cuts[i + 1]
        return k.copy(
            grads.at[:, :, 1 - k.c, lo:hi],
            paired.at[:, :, lo - t_base : hi - t_base],
            k.at(c=1 - k.c),
            sems["pair", i],
        )

    def pair_out(i):
        sems["pair", i] = k.take()
        op = pair_copy(i)
        op.start()
        k.waits.append(op.wait_send)

    def pair_in():
        for i in range(len(cuts) - 1):
            pair_copy(i).wait_recv()

        for half, (t0, n) in enumerate(halves):

            @pl.loop(0, 4)
            def _(i):
                own = grads[i, :, k.c, t_base + t0 : t_base + t0 + n]
                paired[i, :, t0 : t0 + n] = paired[i, :, t0 : t0 + n] + own

            outset(half)

    def spread(half):
        box = second_in[half]
        sem = sems[half, 1] = k.take()
        for d in (2, 1, 3):
            k.copy(view(half, 1, d), box.at[d - 1], to_axis(half, 1, d), sem).start()
        k.later(box, sem)

    def collect_spread(half):
        box = second_in[half]
        k.arrived(box, sems[half, 1])
        own = view(half, 1, 0)
        near = box[0].astype(f32) + box[2].astype(f32)
        own[...] = ((own[...].astype(f32) + box[1].astype(f32)) + near).astype(jnp.bfloat16)

    ways = ((0, 1), (1, -1))

    def outset(half):
        one, two = first_in[half]
        base = sems[half, 0] = k.take(2)
        for way, delta in ways:
            target = to_axis(half, 0, delta)
            k.copy(view(half, 0, 2, way), one.at[way], target, base).start()
        for way, delta in ways:
            part = 1 - way
            box = two.at[way, 2 * part : 2 * part + 2]
            k.copy(view(half, 0, delta, part), box, to_axis(half, 0, delta), base + 1).start()
        k.later(one, base)

    def relay():
        for half in (0, 1):
            one, two = first_in[half]
            base = sems[half, 0]
            k.arrived(one, base)
            for way, delta in ways:
                target = view(half, 0, delta, way)
                target[...] = target[...] + one[way]
                box = two.at[way, 2 * way : 2 * way + 2]
                k.copy(target, box, to_axis(half, 0, delta), base + 1).start()
            k.later(two, base + 1)

    def collect(half):
        two = first_in[half][1]
        k.arrived(two, sems[half, 0] + 1)
        own = view(half, 0, 0)
        own[...] = (own[...].astype(f32) + (two[0].astype(f32) + two[1].astype(f32))).astype(
            jnp.bfloat16
        )

    def turn():
        for half in (0, 1):
            collect(half)
            spread(half)

    spot = 2 * k.zh + k.zl
    holds = k.zl == k.c
    piece_step, piece_size = pieces_of(n_tiles)

    def z_out():
        for half in (0, 1):
            collect_spread(half)
        sem = sems["z"] = k.take()
        for q in range(4):
            for e in range(2):
                piece = piece_step * (2 * q + e)
                source = paired.at[k.x, k.y, piece : piece + piece_size]
                mine = (k.zh == q) & (k.c == e) & holds
                op = k.copy(source, z_in.at[spot], k.at(zl=k.c, zh=q, c=e), sem)

                @pl.when(jnp.logical_not(mine))
                def _():
                    op.start()

                @pl.when(mine)
                def _():
                    z_in[spot] = source[...]

        k.later(z_in.at[0:7], sem, holds)
        k.later(z_in, sem, jnp.logical_not(holds))

    def z_sum():
        @pl.when(holds)
        def _():
            k.arrived(z_in.at[0:7], sems["z"])

        @pl.when(jnp.logical_not(holds))
        def _():
            k.arrived(z_in, sems["z"])

        p = 2 * k.zh + k.c
        gathered[p] = tree_sum([z_in[i].astype(f32) for i in range(8)]).astype(jnp.bfloat16)
        sem = sems["g"] = k.take()
        box = gathered.at[p]
        for d in range(1, 8):
            to = lax.rem(p + d, 8)
            k.copy(box, box, k.at(zh=to // 2, c=lax.rem(to, 2)), sem).start()
        k.later(gathered.at[0:7], sem)

    def gather():
        k.arrived(gathered.at[0:7], sems["g"])

    def whole_out():
        for half in (0, 1):
            collect_spread(half)
        sem = sems["z"] = k.take()
        for q in range(4):
            op = k.copy(paired.at[k.x, k.y], z_in.at[spot], k.at(zl=k.c, zh=q), sem)

            @pl.when(jnp.logical_not(holds & (k.zh == q)))
            def _():
                op.start()

        @pl.when(holds)
        def _():
            z_in[spot] = paired[k.x, k.y]

        k.later(z_in.at[0:3], sem, holds)
        k.later(z_in.at[0:4], sem, jnp.logical_not(holds))

    def whole_sum():
        sems["g"] = k.take()

        @pl.when(holds)
        def _():
            k.arrived(z_in.at[0:7], sems["z"])
            gathered[0] = tree_sum([z_in[i].astype(f32) for i in range(8)]).astype(jnp.bfloat16)
            k.whole(gathered, sems["g"]).start()

        k.later(gathered, sems["g"], holds)

    def whole_in():
        @pl.when(jnp.logical_not(holds))
        def _():
            k.arrived(gathered, sems["g"])

    pairs = [functools.partial(pair_out, i) for i in range(len(cuts) - 1)]
    if direct:
        return pairs + [pair_in, relay, turn, whole_out, whole_sum, whole_in]
    return pairs + [pair_in, relay, turn, z_out, z_sum, gather]


def write_shard(cuts, direct, gathered, grad_in_ref, grad_out_ref, scaling):
    t_base, n_tiles = cuts[0], cuts[-1] - cuts[0]
    piece_step = n_tiles if direct else pieces_of(n_tiles)[0]
    for at in range(n_tiles):
        p = min(at // piece_step, 7)
        values = gathered[p, at - piece_step * p].astype(jnp.float32) * scaling
        tile = t_base + at
        if tile < 8:
            column, half = tile // 2, tile % 2
            grad_out_ref[16 * half : 16 * half + 16, 128 * column : 128 * column + 128] = values
        else:
            grad_in_ref[:, 128 * (tile - 8) : 128 * (tile - 7)] = values


def sum_scratch(cuts, direct):
    n_tiles = cuts[-1] - cuts[0]

    def tiles(*lead):
        return pltpu.VMEM((*lead, 16, 128), jnp.bfloat16)

    shapes = [tiles(4, 4, n_tiles)]
    for _, n in halves_of(n_tiles):
        shapes += [tiles(2, 2, n), tiles(2, 4, n)]
    shapes += [tiles(3, n) for _, n in halves_of(n_tiles)]
    if direct:
        return shapes + [tiles(8, n_tiles), tiles(1, n_tiles)]
    return shapes + [tiles(8, pieces_of(n_tiles)[1])] * 2


def sum_refs(refs):
    return refs[0], (refs[1:3], refs[3:5]), refs[5:7], refs[7], refs[8]


NN = (((1,), (0,)), ((), ()))
NT_DIMS = (((1,), (1,)), ((), ()))
TN = (((0,), (0,)), ((), ()))


def dot(a, b, dims=NN):
    return lax.dot_general(a, b, dims, preferred_element_type=F32)


def sigmoid(p):
    return 0.5 * jnp.tanh(0.5 * p) + 0.5


def cols(at, width=512):
    return slice(at, at + width)


def group_mask(unit):
    if unit == 0:
        return None
    row = lax.broadcasted_iota(jnp.int32, (BLOCK, BLOCK), 0)
    column = lax.broadcasted_iota(jnp.int32, (BLOCK, BLOCK), 1)
    return lax.rem(row, 16) == lax.rem(column, 16)


def positive_scores(unit, query, keyed):
    r = jnp.maximum(dot(query, keyed, NT_DIMS) * S ** (-0.5), 0.0)
    mask = group_mask(unit)
    return r if mask is None else jnp.where(mask, r, 0.0)


def length_of(unit):
    return BLOCK if unit == 0 else 16


def forward_group(m, unit, g, x):
    xf = x.astype(F32)
    scaling = lax.rsqrt(jnp.mean(xf * xf, axis=-1, keepdims=True) + EPSILON)
    hidden = (xf * scaling * m.gains[unit : unit + 1, :]).astype(BF16)
    m.hidden[unit, g] = hidden
    p = dot(hidden, m.w_in[unit, :, 2 * E :])
    m.proj[unit, g, :, 2 * E :] = p
    z = p * sigmoid(p)
    query = (z * m.scales[unit, 0:1, :]).astype(BF16)
    keyed = (z * m.scales[unit, 1:2, :]).astype(BF16)
    m.query[unit, g] = query
    m.keyed[unit, g] = keyed
    r = positive_scores(unit, query, keyed)
    weights = (r * r * (1.0 / length_of(unit))).astype(BF16)
    m.weights[unit, g] = weights
    for at in range(0, E, 512):
        p = dot(hidden, m.w_in[unit, :, cols(E + at)])
        m.proj[unit, g, :, cols(E + at)] = p
        m.value[unit, g, :, cols(at)] = (p * sigmoid(p)).astype(BF16)
        p = dot(hidden, m.w_in[unit, :, cols(at)])
        m.proj[unit, g, :, cols(at)] = p
        mixed = dot(weights, m.value[unit, g, :, cols(at)])
        m.mixed[unit, g, :, cols(at)] = mixed
        m.gated[unit, g, :, cols(at)] = (p * sigmoid(p) * mixed).astype(BF16)
    return (x.astype(F32) + dot(m.gated[unit, g], m.w_out[unit])).astype(BF16)


def backward_gate(m, unit, g, upstream):
    for at in range(0, E, 512):
        d_gated = dot(upstream, m.w_out[unit, cols(at), :], NT_DIMS).astype(BF16).astype(F32)
        p = m.proj[unit, g, :, cols(at)]
        sig = sigmoid(p)
        gate = p * sig
        m.d_mixed[g, :, cols(at)] = (d_gated * gate).astype(BF16)
        slope = sig + gate * (1.0 - sig)
        m.d_proj[g, :, cols(at)] = (d_gated * m.mixed[unit, g, :, cols(at)] * slope).astype(BF16)


def backward_attention(m, unit, g):
    d_weights = dot(m.d_mixed[g], m.value[unit, g], NT_DIMS).astype(BF16).astype(F32)
    query, keyed = m.query[unit, g], m.keyed[unit, g]
    r = positive_scores(unit, query, keyed)
    d_scores = (d_weights * r * (2.0 / length_of(unit) * S ** (-0.5))).astype(BF16)
    d_query = dot(d_scores, keyed).astype(BF16).astype(F32)
    d_keyed = dot(d_scores, query, TN).astype(BF16).astype(F32)
    p = m.proj[unit, g, :, 2 * E :]
    sig = sigmoid(p)
    z = p * sig
    d_z = d_query * m.scales[unit, 0:1, :] + d_keyed * m.scales[unit, 1:2, :]
    m.d_proj[g, :, 2 * E :] = (d_z * (sig + z * (1.0 - sig))).astype(BF16)
    m.small[unit, 4:5, :] += jnp.sum(d_query * z, axis=0, keepdims=True)
    m.small[unit, 5:6, :] += jnp.sum(d_keyed * z, axis=0, keepdims=True)
    weights = m.weights[unit, g]
    for at in range(0, E, 512):
        d_value = dot(weights, m.d_mixed[g, :, cols(at)], TN).astype(BF16).astype(F32)
        p = m.proj[unit, g, :, cols(E + at)]
        sig = sigmoid(p)
        m.d_proj[g, :, cols(E + at)] = (d_value * (sig + p * sig * (1.0 - sig))).astype(BF16)


def backward_input(m, unit, g, x, upstream):
    d_hidden = dot(m.d_proj[g], m.w_in[unit], NT_DIMS)
    xf = x.astype(F32)
    scaling = lax.rsqrt(jnp.mean(xf * xf, axis=-1, keepdims=True) + EPSILON)
    xs = xf * scaling
    d_gain = jnp.sum(d_hidden * xs, axis=0, keepdims=True)
    for i in range(4):
        m.small[unit, i : i + 1, :] += d_gain[:, 128 * i : 128 * i + 128]
    d_xs = d_hidden * m.gains[unit : unit + 1, :]
    d_x = scaling * (d_xs - xs * jnp.mean(d_xs * xs, axis=-1, keepdims=True))
    return (upstream.astype(F32) + d_x).astype(BF16)


def turned(m, unit):
    for g in (0, 1):
        m.hidden_t[unit, :, cols(BLOCK * g, BLOCK)] = m.hidden[unit, g].T
        m.gated_t[unit, :, cols(BLOCK * g, BLOCK)] = m.gated[unit, g].T


def weight_out_grad(m, unit, upstream):
    for i in range(4):
        rows = dot(m.gated_t[unit, cols(256 * i, 256), :], upstream).astype(BF16)
        parts = rows.reshape(4, 2, 2, 16, 512)
        for column in range(4):
            at = 2 * column
            m.grads[unit, i, :, :, at : at + 2] = parts[..., 128 * column : 128 * column + 128]


GATE = ((0, 512), (512, 512))
OTHERS = ((1024, 512), (1536, 512), (2048, 128))


def weight_in_grad(m, unit, columns):
    for at, width in columns:
        right = m.d_proj[:, :, cols(at, width)].reshape(2 * BLOCK, width)
        for i in (0, 1):
            part = dot(m.hidden_t[unit, cols(256 * i, 256), :], right).astype(BF16)
            part = part.reshape(2, 4, 2, 16, width)
            for j in range(width // 128):
                m.grads[unit, 2 * i : 2 * i + 2, :, :, 8 + at // 128 + j] = part[
                    ..., 128 * j : 128 * j + 128
                ]


class Memory:
    pass


SCRATCH = dict(
    w_in=((2, D, WIDE), BF16),
    w_out=((2, E, D), BF16),
    frames=((2, BLOCK, D), BF16),
    cot=((2, 8, 2, 16, D), BF16),
    first=((2, 8, 2, 16, D), BF16),
    first_pos=((2, 16, 16, D), BF16),
    cot_pos=((2, 16, 16, D), BF16),
    out_pos=((2, 16, 16, D), BF16),
    out=((2, 8, 2, 16, D), BF16),
    back_pos=((2, 16, 16, D), BF16),
    back=((2, 8, 2, 16, D), BF16),
    back_frames=((2, BLOCK, D), BF16),
    hidden=((2, 2, BLOCK, D), BF16),
    hidden_t=((2, D, 2 * BLOCK), BF16),
    proj=((2, 2, BLOCK, WIDE), F32),
    value=((2, 2, BLOCK, E), BF16),
    query=((2, 2, BLOCK, S), BF16),
    keyed=((2, 2, BLOCK, S), BF16),
    weights=((2, 2, BLOCK, BLOCK), BF16),
    mixed=((2, 2, BLOCK, E), F32),
    gated=((2, 2, BLOCK, E), BF16),
    gated_t=((2, E, 2 * BLOCK), BF16),
    d_mixed=((2, BLOCK, E), BF16),
    d_proj=((2, BLOCK, WIDE), BF16),
    grads=((2, 4, 4, 2, NT, 16, 128), BF16),
    small=((2, 8, 128), F32),
    scales=((2, 2, S), F32),
    gains=((2, D), F32),
)
GROUPS = (
    (1, (0, 8, 16), False),
    (1, (16, 25), False),
    (0, (0, 8, 16), False),
    (0, (16, 25), True),
)


def step_kernel(scaling, *refs):
    m = Memory()
    frames_hbm, cot_hbm, w_in_hbm, w_out_hbm, scales_hbm, gains_hbm = refs[:6]
    out_hbm, back_hbm, in_ref, wout_ref, small_ref = refs[6:11]
    refs = refs[11:]
    for name, ref in zip(SCRATCH, refs):
        setattr(m, name, ref)
    refs = refs[len(SCRATCH) :]
    sums = []
    for _, cuts, direct in GROUPS:
        count = len(sum_scratch(cuts, direct))
        sums.append(sum_refs(refs[:count]))
        refs = refs[count:]
    small_bufs = refs[0]
    local, send, recv = refs[1:4]
    k = Links(send, recv)
    p = 2 * k.zh + k.c

    def load(src, dst, sem):
        op = pltpu.make_async_copy(src, dst, local.at[sem])
        op.start()
        return op

    loads = dict(
        frames=load(frames_hbm, m.frames, 0),
        scales=load(scales_hbm, m.scales, 6),
        gains=load(gains_hbm, m.gains, 7),
        others_0=load(w_in_hbm.at[0, :, E:], m.w_in.at[0, :, E:], 1),
        gate_0=load(w_in_hbm.at[0, :, :E], m.w_in.at[0, :, :E], 8),
        out_0=load(w_out_hbm.at[0], m.w_out.at[0], 3),
    )
    met = greet(k)
    m.small[...] = jnp.zeros((2, 8, 128), F32)

    def peer(d):
        j = lax.rem(p + d, 8)
        return j, k.at(zh=j // 2, c=lax.rem(j, 2))

    def from_peer(d):
        j = lax.rem(p + 8 - d, 8)
        return j, k.at(zh=j // 2, c=lax.rem(j, 2))

    first_sems, cot_sems, out_sems, back_sems = (k.take(2) for _ in range(4))

    def first_copy(b, h, d, to):
        return k.copy(m.first.at[b, to[0], h], m.first_pos.at[h, 2 * p + b], to[1], first_sems + h)

    def cot_copy(h, d, to):
        box = m.cot_pos.at[h, pl.ds(2 * p, 2)]
        return k.copy(m.cot.at[:, to[0], h], box, to[1], cot_sems + h)

    def out_copy(h, d, to):
        box = m.out.at[:, p, h]
        return k.copy(m.out_pos.at[h, pl.ds(2 * to[0], 2)], box, to[1], out_sems + h)

    def back_copy(b, h, d, to):
        return k.copy(m.back_pos.at[h, 2 * to[0] + b], m.back.at[b, p, h], to[1], back_sems + b)

    def send(copy, h):
        for d in range(1, 8):
            copy(h, d, peer(d)).start()

    def receive(base, h):
        k.arrived(m.first_pos.at[0, 0:14], base + h)

    for name in ("frames", "scales", "gains", "others_0", "gate_0", "out_0"):
        loads[name].wait()
    loads = dict(
        cot=load(cot_hbm, m.cot, 2),
        in_1=load(w_in_hbm.at[1], m.w_in.at[1], 4),
        out_1=load(w_out_hbm.at[1], m.w_out.at[1], 5),
    )

    def exchange_first(b, h):
        for d in range(1, 8):
            first_copy(b, h, d, peer(d)).start()

    def block_forward(b):
        with jax.named_scope("f0"):
            m.first[b] = forward_group(m, 0, b, m.frames[b]).reshape(8, 2, 16, D)

    block_forward(0)
    with jax.named_scope("barrier"):
        met()
    for h in (0, 1):
        exchange_first(0, h)
    block_forward(1)
    for h in (0, 1):
        exchange_first(1, h)
        m.first_pos[h, pl.ds(2 * p, 2)] = m.first[:, p, h]
    loads["cot"].wait()
    for h in (0, 1):
        send(cot_copy, h)
        m.cot_pos[h, pl.ds(2 * p, 2)] = m.cot[:, p, h]
    with jax.named_scope("turn0"):
        turned(m, 0)
    loads["in_1"].wait()
    loads["out_1"].wait()

    @pl.loop(0, 2)
    def _(h):
        with jax.named_scope("w_first"):
            receive(first_sems, h)
        with jax.named_scope("f1"):
            x = m.first_pos[h].reshape(BLOCK, D)
            m.out_pos[h] = forward_group(m, 1, h, x).reshape(16, 16, D)

    m.out[:, p] = m.out_pos[:, pl.ds(2 * p, 2)].transpose(1, 0, 2, 3)
    with jax.named_scope("turn1"):
        turned(m, 1)

    groups = {}
    for name, (unit, cuts, direct), refs_of in zip(("a1", "b1", "a0", "b0"), GROUPS, sums):
        groups[name] = sum_stages(k, m.grads.at[unit], cuts, direct, *refs_of)
    groups["s"] = small_sum(k, small_bufs, m.small, small_ref)
    done = dict.fromkeys(groups, 0)

    def run(names):
        for name in names.split():
            with jax.named_scope(f"{name}_{done[name]}"):
                groups[name][done[name]]()
            done[name] += 1

    def unit_1_gate(h, wait=True):
        if wait:
            with jax.named_scope("w_cot"):
                receive(cot_sems, h)
        with jax.named_scope("gate1"):
            backward_gate(m, 1, h, m.cot_pos[h].reshape(BLOCK, D))

    def unit_1_rest(h):
        with jax.named_scope("rest1"):
            backward_attention(m, 1, h)
            x = m.first_pos[h].reshape(BLOCK, D)
            upstream = m.cot_pos[h].reshape(BLOCK, D)
            m.back_pos[h] = backward_input(m, 1, h, x, upstream).reshape(16, 16, D)
        for b in (0, 1):
            send(functools.partial(back_copy, b), h)
        m.back[:, p, h] = m.back_pos[h, pl.ds(2 * p, 2)]

    def gate_0(g, wait=True):
        if wait:
            with jax.named_scope("w_back"):
                receive(back_sems, g)
        with jax.named_scope("gate0"):
            backward_gate(m, 0, g, m.back[g].reshape(BLOCK, D))

    def attention_0(g):
        with jax.named_scope("attn0"):
            backward_attention(m, 0, g)

    def input_0(g):
        with jax.named_scope("input0"):
            m.back_frames[g] = backward_input(m, 0, g, m.frames[g], m.back[g].reshape(BLOCK, D))

    def write(at):
        unit, cuts, direct = GROUPS[at]
        write_shard(cuts, direct, sums[at][-1], in_ref.at[unit], wout_ref.at[unit], scaling)

    unit_1_gate(0)
    unit_1_rest(0)
    with jax.named_scope("w_cot"):
        receive(cot_sems, 1)
    with jax.named_scope("wgo1"):
        weight_out_grad(m, 1, m.cot_pos[...].reshape(2 * BLOCK, D))
    run("a1")
    unit_1_gate(1, False)
    with jax.named_scope("wgi1"):
        weight_in_grad(m, 1, GATE)
    run("a1")
    unit_1_rest(1)
    run("a1")
    with jax.named_scope("wg1b"):
        weight_in_grad(m, 1, OTHERS)
    run("b1 b1 a1")
    gate_0(0)
    with jax.named_scope("w_back1"):
        receive(back_sems, 1)
    for h in (0, 1):
        send(out_copy, h)
    with jax.named_scope("wgo0"):
        weight_out_grad(m, 0, m.back[...].reshape(2 * BLOCK, D))
    run("a0 b1")
    gate_0(1, False)
    with jax.named_scope("wgi0"):
        weight_in_grad(m, 0, GATE)
    run("a0 a1")
    attention_0(0)
    run("a0")
    attention_0(1)
    run("b1")
    with jax.named_scope("wg0b"):
        weight_in_grad(m, 0, OTHERS)
    run("b0 a1")
    input_0(0)
    run("a0")
    input_0(1)
    store_back = load(m.back_frames, back_hbm, 0)
    run("b0 s b1 s a0 b0 b0 a0 a1 b1 s b0 s")
    with jax.named_scope("w_out"):
        receive(out_sems, 0)
        receive(out_sems, 1)
    store_out = load(m.out, out_hbm, 2)
    run("a0 s a1 b1")
    write(0)
    write(1)
    small_ref[...] = small_ref[...] * scaling
    run("b0 a0")
    write(2)
    run("b0")
    write(3)
    with jax.named_scope("drain"):
        k.drain()

        for base in (first_sems, cot_sems, out_sems, back_sems):
            for h in (0, 1):
                k.whole(m.first_pos.at[0, 0:14], base + h).wait_send()

        store_back.wait()
        store_out.wait()
    assert all(done[name] == len(stages) for name, stages in groups.items())
    assert k.used <= SEMS


def write_kernel(*refs):
    arrived, outputs, held = refs[:5], refs[5:11], refs[11:18]
    come, gone = refs[18:]
    incoming = [pltpu.make_async_copy(arrived[i], held[i], come.at[i]) for i in range(5)]
    for i in (4, 3, 2, 1, 0):
        incoming[i].start()
    outgoing = [pltpu.make_async_copy(held[i], outputs[i], gone.at[i]) for i in range(4)]
    small, gains, scales = held[4:]
    outgoing += [
        pltpu.make_async_copy(gains, outputs[4], gone.at[4]),
        pltpu.make_async_copy(scales, outputs[5], gone.at[5]),
    ]
    incoming[4].wait()
    for unit in (0, 1):
        for i in range(4):
            gains[unit : unit + 1, 128 * i : 128 * i + 128] = small[unit, i : i + 1, :]
        scales[unit] = small[unit, 4:6, :]
    outgoing[4].start()
    outgoing[5].start()
    for i in (3, 2, 1, 0):
        incoming[i].wait()
        outgoing[i].start()
    for op in outgoing:
        op.wait()


def on_device(frames, cotangent, weight_in, qk_scales, weight_out, gains):
    tokens_all = frames.shape[0] * frames.shape[1] * lax.axis_size(DP) * lax.axis_size(SEQ)
    vmem = pl.BlockSpec(memory_space=pltpu.VMEM)
    hbm = pl.BlockSpec(memory_space=pl.ANY)
    scratch = [pltpu.VMEM(shape, dtype) for shape, dtype in SCRATCH.values()]
    for _, cuts, direct in GROUPS:
        scratch += sum_scratch(cuts, direct)
    scratch += [pltpu.VMEM((17, 2, 8, 128), F32)]
    dma = pltpu.SemaphoreType.DMA
    scratch += [dma((9,)), dma((SEMS,)), dma((SEMS,))]
    parts = pl.pallas_call(
        functools.partial(step_kernel, tokens_all ** (-0.5)),
        out_shape=(
            jax.ShapeDtypeStruct((2, 8, 2, 16, D), BF16),
            jax.ShapeDtypeStruct((2, BLOCK, D), BF16),
            jax.ShapeDtypeStruct((2, 16, WIDE), F32),
            jax.ShapeDtypeStruct((2, 32, D), F32),
            jax.ShapeDtypeStruct((2, 8, 128), F32),
        ),
        in_specs=[hbm] * 6,
        out_specs=(hbm, hbm, vmem, vmem, vmem),
        scratch_shapes=scratch,
        compiler_params=pltpu.CompilerParams(
            collective_id=0, has_side_effects=True, vmem_limit_bytes=67_043_328
        ),
    )(
        frames.reshape(2, BLOCK, D),
        cotangent.reshape(2, 8, 2, 16, D),
        weight_in,
        weight_out,
        qk_scales,
        gains,
    )
    shapes = [(part.shape, part.dtype) for part in parts]
    small_shapes = [((2, D), F32), ((2, 2, S), F32)]
    result, back, grad_in, grad_out, gains_sum, scales_sum = pl.pallas_call(
        write_kernel,
        out_shape=tuple(jax.ShapeDtypeStruct(*one) for one in shapes[:4] + small_shapes),
        in_specs=[hbm] * 5,
        out_specs=(hbm,) * 6,
        scratch_shapes=[pltpu.VMEM(*one) for one in shapes + small_shapes] + [dma((5,)), dma((6,))],
    )(*parts)
    return (
        result.reshape(frames.shape),
        back.reshape(frames.shape),
        grad_in,
        grad_out,
        gains_sum,
        scales_sum,
    )


def solution(mesh):
    split = Mesh(mesh.devices.reshape(4, 4, 2, 4, 2), DP + SEQ)
    placed = (P(DP, SEQ, None), P(DP, SEQ, None), P(), P(), P(), P())
    return jax.shard_map(
        on_device,
        mesh=split,
        in_specs=placed,
        out_specs=(
            P(DP, SEQ, None),
            P(DP, SEQ, None),
            P(None, DP, None),
            P(None, DP, None),
            P(),
            P(),
        ),
        check_vma=False,
    )
```
